32 devices in a mesh: dp: 16 (over z, x, core), mp: 2 (over y).
Axes of the slice: x: 2, y: 2, z: 4, core: 2. Of those that a mesh axis runs over, the one named last changes fastest.
Arguments:
- node_feats: bfloat16 [256, 32768], P('mp', 'dp'), may hold values from -6 to 6
- proj_weight: bfloat16 [256, 256], P('mp'), may hold values from -0.375 to 0.375
- att_src: float32 [256], P('mp'), may hold values from -32 to 32
- att_dst: float32 [256], P('mp'), may hold values from -32 to 32
- out_bias: float32 [256], P('mp'), may hold values from -3 to 3
- tile_rows: int32 [512], P('dp'), may hold values from 0 to 255, as said below
- tile_cols: int32 [512], P('dp'), may hold values from 0 to 255, as said below
- tile_masks: int32 [512, 4, 128], P('dp'), may hold values from -2147483648 to 2147483646
Outputs:
- node_out: bfloat16 [256, 32768], P('mp', 'dp')
The draws below stay inside these ranges and needn't reach their ends.
Inputs may be any that keep to these rules, and one draw needn't show every extreme that they name: `tile_rows`: block b holds nodes 128 b to 128 b + 127 and belongs to index b // 16 of dp. Among the 32 tiles of one index of dp, no owner's blocks are named more than 4 times; on every index one owner's blocks are named exactly 4 times. `tile_cols`: the same bound holds for source blocks: among the 32 tiles of one index of dp, no owner's blocks are named more than 4 times, and one owner's exactly 4 times on every index.
All inputs are finite; a program needn't handle non-finite values.
Results may differ from the reference program's by a relative error of at most 0.0034.
Values may be sent and summed in bfloat16 or wider, within the bound.
No kernel may reach another device: no remote copies, remote signals or barrier semaphores. Data moves between devices by JAX's collectives and lax.ppermute only.
A program may use at most 64 MiB of HBM per device.

```python
import jax
import jax.numpy as jnp
from jax import lax

FIN = 256
HEADS = 8
HD = 32
TILE = 128
TILES_DEV = 32
NODES = 32768
BLK_DEV = 16
NBLK = 256
TILES = 512
CAP = 4
N_DP = 16


def tile_blocks(key, salt):
    base_key = jax.random.fold_in(key, salt)
    hub_owner = jax.random.randint(jax.random.fold_in(base_key, 7), (), 0, N_DP)

    def device_tiles(device):
        device_key = jax.random.fold_in(base_key, device)
        key_rest, key_shift, key_local, key_order = jax.random.split(device_key, 4)
        rest_slots = CAP + jax.random.permutation(key_rest, N_DP * CAP - CAP)[:TILES_DEV - CAP]
        position = jnp.concatenate([jnp.arange(CAP, dtype=jnp.int32), rest_slots.astype(jnp.int32)])
        shifts = jnp.concatenate([jnp.zeros((1,), jnp.int32), 1 + jax.random.permutation(key_shift, N_DP - 1).astype(jnp.int32)])
        owners = (hub_owner + shifts[position // CAP]) % N_DP
        local_block = jax.random.randint(key_local, (TILES_DEV,), 0, BLK_DEV)
        blocks = owners * BLK_DEV + local_block
        return blocks[jax.random.permutation(key_order, TILES_DEV)]
    return jax.vmap(device_tiles)(jnp.arange(N_DP)).reshape(-1).astype(jnp.int32)


def draw_tile_rows(key, part):
    return tile_blocks(key, 101)


def draw_tile_cols(key, part):
    return tile_blocks(key, 202)


def attention_vector(key):
    key_base = jax.random.fold_in(key, 0)
    vector = 0.25 * jnp.clip(jax.random.normal(key_base, (HEADS, HD), jnp.float32), -4.0, 4.0)
    return vector.reshape(-1)


def draw_att_src(key, part):
    return attention_vector(jax.random.fold_in(key, 11))


def draw_att_dst(key, part):
    return attention_vector(jax.random.fold_in(key, 23))


def plant(entries, key, smallest, top_value):
    index_at = [jax.random.randint(jax.random.fold_in(key, axis), (), 0, length) for axis, length in enumerate(entries.shape)]
    widest = entries.shape.index(max(entries.shape))
    neighbour = index_at[:widest] + [(index_at[widest] + 1) % entries.shape[widest]] + index_at[widest + 1:]
    return entries.at[tuple(index_at)].set(smallest).at[tuple(neighbour)].set(top_value)


def levels(rng, shape, pieces, low, top_value):
    loudness, own = 1.0, jax.random.fold_in(rng, 6)
    for dim, parts in pieces:
        draws = jnp.exp(jax.random.uniform(jax.random.fold_in(own, dim), (parts,), jnp.float32, low / len(pieces), top_value / len(pieces)))
        loudness = loudness * jnp.repeat(draws, shape[dim] // parts).reshape([-1 if axis == dim else 1 for axis in range(len(shape))])
    return loudness


def bell_draw(stream_key, extent, width, limit, shards=(), held_as=jnp.bfloat16):
    values = width * jax.random.normal(stream_key, extent, jnp.float32)
    if shards:
        values = values * levels(stream_key, extent, shards, -0.22, 0.18)
    return jnp.clip(values, -limit, limit).astype(held_as)


def setup_inputs(seed: int = 0) -> dict:
    streams_of = jax.random.split(jax.random.key(seed), 9)
    return {
        "node_feats": bell_draw(streams_of[0], (FIN, NODES), 1.0, 6.0, ((0, 2), (1, 16))),
        "proj_weight": bell_draw(streams_of[1], (HEADS * HD, FIN), FIN ** -0.5, 0.375, ((0, 2),)),
        "att_src": draw_att_src(jax.random.fold_in(streams_of[8], 71), 0),
        "att_dst": draw_att_dst(jax.random.fold_in(streams_of[8], 71), 0),
        "out_bias": bell_draw(streams_of[4], (HEADS * HD,), 0.5, 3.0, ((0, 2),), jnp.float32),
        "tile_rows": draw_tile_rows(jax.random.fold_in(streams_of[8], 71), 0),
        "tile_cols": draw_tile_cols(jax.random.fold_in(streams_of[8], 71), 0),
        "tile_masks": plant(jax.random.randint(streams_of[7], (TILES, TILE // 32, TILE), -2147483648, 2147483647), jax.random.fold_in(streams_of[7], 1), -2147483648, 2147483646).astype(jnp.int32),
    }


far_below = -1.0e30


def leaky_relu(scores):
    return jnp.where(scores > 0, scores, 0.2 * scores)


def unpack_bits(packed):
    offsets = jnp.arange(32, dtype=jnp.int32)
    spread = jnp.bitwise_and(jnp.right_shift(packed[..., :, None, :], offsets[:, None]), 1)
    return spread.reshape(packed.shape[:-2] + (packed.shape[-2] * 32, packed.shape[-1])).astype(jnp.int32)


def edge_scores(edge_mask, source, target):
    raw_scores = leaky_relu(target[:, :, None, :] + source[:, :, :, None])
    return jnp.where(edge_mask[:, None] == 1, raw_scores, far_below)


def reference(node_feats, proj_weight, att_src, att_dst, out_bias, tile_rows, tile_cols, tile_masks):
    projected = jnp.dot(proj_weight, node_feats, preferred_element_type=jnp.float32)
    features = projected.astype(jnp.bfloat16)
    by_head = projected.reshape(HEADS, HD, NODES)
    source = jnp.einsum("hd,hdn->hn", att_src.reshape(HEADS, HD), by_head, precision=lax.Precision.HIGHEST)
    target = jnp.einsum("hd,hdn->hn", att_dst.reshape(HEADS, HD), by_head, precision=lax.Precision.HIGHEST)
    source_blocks = source.reshape(HEADS, NBLK, TILE).transpose(1, 0, 2)
    target_blocks = target.reshape(HEADS, NBLK, TILE).transpose(1, 0, 2)
    feat_blocks = features.reshape(HEADS, HD, NBLK, TILE).transpose(2, 0, 1, 3)
    group_rows = tile_rows.reshape(-1, TILES_DEV)
    group_cols = tile_cols.reshape(-1, TILES_DEV)
    group_masks = tile_masks.reshape(-1, TILES_DEV, TILE // 32, TILE)

    def tile_scores(inputs):
        row_ids, col_ids, packed = inputs
        edge_mask = unpack_bits(packed)
        scores = edge_scores(edge_mask, source_blocks[col_ids], target_blocks[row_ids])
        tile_peaks = jnp.max(scores, axis=2)
        weights = jnp.where(edge_mask[:, None] == 1, jnp.exp(scores - tile_peaks[:, :, None, :]), 0.0)
        return tile_peaks, weights

    def first_pass(inputs):
        tile_peaks, weights = tile_scores(inputs)
        return tile_peaks, jnp.sum(weights, axis=2)

    tile_peaks, masses = lax.map(first_pass, (group_rows, group_cols, group_masks))
    tile_peaks = tile_peaks.reshape(TILES, HEADS, TILE)
    masses = masses.reshape(TILES, HEADS, TILE)
    self_scores = leaky_relu(source_blocks + target_blocks)
    row_peak = self_scores.at[tile_rows].max(tile_peaks)
    self_weight = jnp.exp(self_scores - row_peak)
    denominator = self_weight.at[tile_rows].add(jnp.exp(tile_peaks - row_peak[tile_rows]) * masses)

    def second_pass(summed, inputs):
        row_ids, col_ids, packed = inputs
        peaks_here, weights = tile_scores(inputs)
        rounded = lax.optimization_barrier(weights.astype(jnp.bfloat16)).astype(jnp.float32)
        partial_values = jnp.einsum("ghdc,ghcr->ghdr", feat_blocks[col_ids].astype(jnp.float32), rounded)
        rescale = jnp.exp(peaks_here - row_peak[row_ids])
        return summed.at[row_ids].add(rescale[:, :, None, :] * partial_values), None

    start_sum = self_weight[:, :, None, :] * feat_blocks.astype(jnp.float32)
    summed, ignored = lax.scan(second_pass, start_sum, (group_rows, group_cols, group_masks))
    gathered = summed / denominator[:, :, None, :]
    flat_out = gathered.transpose(1, 2, 0, 3).reshape(HEADS * HD, NODES)
    return jax.nn.elu(flat_out + node_feats.astype(jnp.float32) + out_bias[:, None]).astype(jnp.bfloat16)
```

```python
import functools

import jax
import jax.numpy as jnp
from jax import lax
from jax.experimental import pallas as pl
from jax.experimental.pallas import tpu as pltpu
from jax.sharding import PartitionSpec as P

HD = 32
LOG2E = 1.4426950408889634
FAR = -1e30
F32 = jnp.float32
BF16 = jnp.bfloat16


VMEM = pl.BlockSpec(memory_space=pltpu.VMEM)
SMEM = pl.BlockSpec(memory_space=pltpu.SMEM)


def pad8(count):
    return -(-count // 8) * 8


def leaky(scores):
    return jnp.maximum(scores, 0.2 * scores)


def head_sums(rows):
    return jnp.sum(rows.reshape(rows.shape[0] // HD, HD, rows.shape[1]), axis=1)


def stack_rows(pieces, total):
    have = sum(p.shape[0] for p in pieces)
    if have < total:
        pieces = pieces + [jnp.zeros((total - have, pieces[0].shape[1]), F32)]
    return jnp.concatenate(pieces, axis=0)


def ring_order(chips):
    columns = max(1, chips // 4)
    rows = chips // columns
    if columns == 1:
        return list(range(chips))
    order = [row * columns for row in range(rows)]
    for row in reversed(range(rows)):
        inner = list(range(1, columns))
        order += [row * columns + col for col in (inner if (rows - 1 - row) % 2 == 0 else inner[::-1])]
    return order


def project_kernel(parts, mp_ref, w_ref, att_ref, *refs):
    x_refs, (pay_ref, sc_ref) = refs[:parts], refs[parts:]
    me = mp_ref[0]
    depth = w_ref.shape[1] // parts
    total = None
    for k in range(parts):
        at = pl.multiple_of((me ^ k) * depth, depth) if parts > 1 else 0
        term = jnp.dot(w_ref[:, pl.ds(at, depth)], x_refs[k][...], preferred_element_type=F32)
        total = term if total is None else total + term
    rounded = total.astype(BF16)
    a_src, a_dst = att_ref[:, 0:1], att_ref[:, 1:2]
    source = head_sums(total * a_src)
    target = head_sums(total * a_dst)
    rest = source - head_sums(rounded.astype(F32) * a_src)
    rest_hi = rest.astype(BF16).astype(F32)
    extra = stack_rows([rest_hi, rest - rest_hi], pay_ref.shape[1] - rounded.shape[0]).astype(BF16)
    scores = stack_rows([target, leaky(source + target)], sc_ref.shape[1])
    dims, tile = rounded.shape[0], pay_ref.shape[2]
    for b in range(pay_ref.shape[0]):
        at = slice(b * tile, (b + 1) * tile)
        pay_ref[b, :dims, :] = rounded[:, at]
        pay_ref[b, dims:, :] = extra[:, at]
        sc_ref[b] = scores[:, at]


def pack_kernel(blocks, rows_ref, cols_ref, masks_ref, out_ref, count):
    devices, slots = out_ref.shape[0], out_ref.shape[1] - 1
    words = out_ref.shape[2:]
    lane = lax.broadcasted_iota(jnp.int32, words, 1)
    first = lax.broadcasted_iota(jnp.int32, words, 0) == 0
    for d in range(devices):
        count[d] = 0
        out_ref[d, slots] = jnp.zeros(words, jnp.int32)

    def body(t, carry):
        row, col = rows_ref[t], cols_ref[t]
        owner, parity = row // blocks, (col // blocks) % 2
        other = (owner + parity) % 2
        goal = owner - owner % 2 + parity
        at = count[goal]
        count[goal] = at + 1
        out_ref[goal, at] = masks_ref[t]
        code = 1 + other * blocks + row % blocks + 2 * blocks * col
        out_ref[goal, slots] = jnp.where(first & (lane == at), code, out_ref[goal, slots])
        return carry

    lax.fori_loop(0, rows_ref.shape[0], body, 0)


def list_kernel(blocks, half, chips, starts, slots, ids_ref, place_ref, list_ref, count_ref):
    groups = len(starts)
    total = ids_ref.shape[0]
    for g in range(groups):
        count_ref[g] = 0
    mine = place_ref[chips]

    def body(n, carry):
        code = ids_ref[n] - 1

        @pl.when(code >= 0)
        def _():
            row, col = code % (2 * blocks), code // (2 * blocks)
            back = mine - place_ref[col // (2 * blocks)]
            back = jnp.where(back < 0, back + chips, back)
            j = col % blocks
            part, at = j // half, j % half
            step = jnp.minimum(back, chips - back)
            way = jnp.where(back > step, 2, 0)
            buf = jnp.where(
                back == 0, part, 2 + 4 * (step - 1) + jnp.where(2 * back == chips, 0, way) + part
            )
            group = jnp.int32(0)
            base = jnp.int32(0)
            for s in starts[1:]:
                group = group + jnp.where(buf >= s, 1, 0)
                base = jnp.where(buf >= s, s, base)
            slot = n + n // slots
            entry = ((slot * (2 * blocks) + row) * 64 + buf - base) * half + at
            n_here = count_ref[group]
            list_ref[group * total + n_here] = entry
            count_ref[group] = n_here + 1

        return carry

    lax.fori_loop(0, total, body, 0)


def tile_step(entry, blocks, half, dims, masks_ref, tscore, att, buf, state):
    heads = dims // HD
    at = entry % half
    entry = entry // half
    which = entry % 64
    entry = entry // 64
    row = entry % (2 * blocks)
    slot = entry // (2 * blocks)
    packed = masks_ref[slot]
    tile = packed.shape[1]
    bit = lax.broadcasted_iota(jnp.int32, (32, tile), 0)
    block = [
        jnp.where(
            (jnp.broadcast_to(packed[w : w + 1], (32, tile)) >> bit) & 1 == 1, 0.0, FAR
        )
        for w in range(packed.shape[0])
    ]
    block = jnp.concatenate(block, axis=0)
    feats = buf[which, at, :dims, :]
    extra = buf[which, at, dims:, :].astype(F32)
    source = head_sums(feats.astype(F32) * att) + extra[:heads] + extra[heads : 2 * heads]
    columns = jnp.transpose(stack_rows([source], pad8(heads)))
    for h in range(heads):
        col = jnp.broadcast_to(columns[:, h : h + 1], (tile, tile))
        top = jnp.max(col + block, axis=0, keepdims=True)
        target = tscore[row, h : h + 1, :]
        old = state[row, dims + h : dims + h + 1, :]
        new = jnp.maximum(old, leaky(target + top))
        alpha = jnp.exp2(old - new)
        raw = jnp.maximum(col + (target - new), 0.2 * col + (0.2 * target - new))
        weight = jnp.exp2(raw + block)
        mass = jnp.sum(weight, axis=0, keepdims=True)
        at_l = dims + heads + h
        state[row, dims + h : dims + h + 1, :] = new
        state[row, at_l : at_l + 1, :] = state[row, at_l : at_l + 1, :] * alpha + mass
        rows = slice(h * HD, (h + 1) * HD)
        state[row, rows, :] = state[row, rows, :] * alpha + jnp.dot(
            feats[rows], weight.astype(BF16), preferred_element_type=F32
        )


def stage_kernel(group, total, first, last, buffers, list_ref, count_ref, masks_ref, own_sc, other_sc, att_ref, *refs):
    pays, refs = refs[:buffers], refs[buffers:]
    if not first:
        state_in, refs = refs[0], refs[1:]
    if last:
        (own_out, other_out, state, tscore, buf) = refs
    else:
        (state, tscore, buf) = refs
    blocks, dims = own_sc.shape[0], att_ref.shape[0]
    half = buf.shape[1]
    heads = dims // HD
    for k in range(buffers):
        buf[k] = pays[k][...]
    tscore[:blocks] = own_sc[...]
    tscore[blocks:] = other_sc[...]
    if first:
        tile = state.shape[2]
        rest = state.shape[1] - dims - 2 * heads
        for b in range(blocks):
            state[b, :dims] = pays[b // half][b % half, :dims].astype(F32)
            state[b, dims : dims + heads] = own_sc[b, heads : 2 * heads]
            state[b, dims + heads : dims + 2 * heads] = jnp.ones((heads, tile), F32)
            state[blocks + b, :dims] = jnp.zeros((dims, tile), F32)
            state[blocks + b, dims : dims + heads] = jnp.full((heads, tile), FAR, F32)
            state[blocks + b, dims + heads :] = jnp.zeros((heads + rest, tile), F32)
            if rest:
                state[b, dims + 2 * heads :] = jnp.zeros((rest, tile), F32)
    else:
        state[...] = state_in[...]
    att = att_ref[:, 0:1]

    def body(i, carry):
        tile_step(list_ref[group * total + i], blocks, half, dims, masks_ref, tscore, att, buf, state)
        return carry

    lax.fori_loop(0, count_ref[group], body, 0)
    if last:
        own_out[...] = state[:blocks]
        other_out[...] = state[blocks:]


def merge_kernel(own_ref, other_ref, x_ref, bias_ref, out_ref):
    blocks, dims, tile = own_ref.shape[0], x_ref.shape[0], own_ref.shape[2]
    heads = dims // HD
    bias = bias_ref[...]
    for b in range(blocks):
        m1, m2 = own_ref[b, dims : dims + heads], other_ref[b, dims : dims + heads]
        l1 = own_ref[b, dims + heads : dims + 2 * heads]
        l2 = other_ref[b, dims + heads : dims + 2 * heads]
        best = jnp.maximum(m1, m2)
        c1, c2 = jnp.exp2(m1 - best), jnp.exp2(m2 - best)
        scale = 1.0 / (l1 * c1 + l2 * c2)
        c1, c2 = (c1 * scale)[:, None, :], (c2 * scale)[:, None, :]
        mixed = own_ref[b, :dims].reshape(heads, HD, tile) * c1
        mixed = mixed + other_ref[b, :dims].reshape(heads, HD, tile) * c2
        at = slice(b * tile, (b + 1) * tile)
        v = mixed.reshape(dims, tile) + x_ref[:, at].astype(F32) + bias
        out_ref[:, at] = jnp.where(v > 0, v, jnp.exp(jnp.minimum(v, 0.0)) - 1.0).astype(BF16)


def local(node_feats, proj_weight, att_src, att_dst, out_bias, tile_rows, tile_cols, tile_masks):
    nodes = node_feats.shape[1]
    dims = proj_weight.shape[0]
    heads = dims // HD
    words, tile = tile_masks.shape[1:]
    blocks = nodes // tile
    tiles = tile_rows.shape[0]
    n_dp, n_mp = lax.axis_size("dp"), lax.axis_size("mp")
    chips = n_dp // 2
    slots = 2 * max(2, 2 * tiles // n_dp)
    half = blocks // 2
    pay_rows = dims + pad8(2 * heads)
    sc_rows = pad8(2 * heads)
    st_rows = dims + pad8(2 * heads)
    order = ring_order(chips)
    place = [order.index(c) for c in range(chips)]
    me_dp, me_mp = lax.axis_index("dp"), lax.axis_index("mp")

    def hop(step):
        pairs = []
        for p, c in enumerate(order):
            to = order[(p + step) % chips]
            pairs += [(2 * c, 2 * to), (2 * c + 1, 2 * to + 1)]
        return sorted(pairs)

    right, left = hop(1), hop(-1)
    swap = [(i, i ^ 1) for i in range(n_dp)]

    att = jnp.stack([att_src, att_dst], axis=1) * LOG2E
    mine = jnp.full((1,), me_mp, jnp.int32)
    if n_mp == 2:
        flip = [(0, 1), (1, 0)]
        halves = [node_feats[:, k * (nodes // 2) : (k + 1) * (nodes // 2)] for k in range(2)]
        inputs = [[x, lax.ppermute(x, "mp", flip)] for x in halves]
    else:
        whole = lax.all_gather(node_feats, "mp", axis=0, tiled=True)
        inputs = [[whole[:, k * (nodes // 2) : (k + 1) * (nodes // 2)]] for k in range(2)]

    packed = pl.pallas_call(
        functools.partial(pack_kernel, blocks),
        out_shape=jax.ShapeDtypeStruct((n_dp, slots + 1, words, tile), jnp.int32),
        in_specs=[SMEM, SMEM, VMEM],
        out_specs=VMEM,
        scratch_shapes=[pltpu.SMEM((n_dp,), jnp.int32)],
        name="pack",
    )(tile_rows, tile_cols, tile_masks)
    got = lax.all_to_all(packed, "dp", split_axis=0, concat_axis=0, tiled=True)

    pays, scs = [], []
    for xs in inputs:
        pay, sc = pl.pallas_call(
            functools.partial(project_kernel, len(xs)),
            out_shape=(
                jax.ShapeDtypeStruct((half, pay_rows, tile), BF16),
                jax.ShapeDtypeStruct((half, sc_rows, tile), F32),
            ),
            in_specs=[SMEM, VMEM, VMEM] + [VMEM] * len(xs),
            out_specs=(VMEM, VMEM),
            name="project",
        )(mine, proj_weight, att, *xs)
        pays.append(pay)
        scs.append(sc)
    own_sc = jnp.concatenate(scs, axis=0)
    other_sc = lax.ppermute(own_sc, "dp", swap)

    bufs = list(pays)
    going = {("r", 0): pays[0], ("r", 1): pays[1], ("l", 0): pays[0], ("l", 1): pays[1]}
    steps = (chips - 1) // 2
    stages = [2]
    for k in range(1, steps + 1):
        for part in range(2):
            going["r", part] = lax.ppermute(going["r", part], "dp", right)
            going["l", part] = lax.ppermute(going["l", part], "dp", left)
        bufs += [going["r", 0], going["r", 1], going["l", 0], going["l", 1]]
        stages.append(len(bufs))
    if chips % 2 == 0:
        bufs += [lax.ppermute(going["r", 0], "dp", right), lax.ppermute(going["l", 1], "dp", left)]
        stages.append(len(bufs))
    starts = (0, stages[-3], stages[-2])
    ends = (stages[-3], stages[-2], stages[-1])

    ids = got[:, slots, 0, :slots].reshape(n_dp * slots)
    table = jnp.array(place, jnp.int32)
    table = jnp.concatenate([table, table[me_dp // 2][None]])
    total = n_dp * slots
    lists, counts = pl.pallas_call(
        functools.partial(list_kernel, blocks, half, chips, starts, slots),
        out_shape=(
            jax.ShapeDtypeStruct((len(starts) * total,), jnp.int32),
            jax.ShapeDtypeStruct((len(starts),), jnp.int32),
        ),
        in_specs=[SMEM, SMEM],
        out_specs=(SMEM, SMEM),
        name="lists",
    )(ids, table)

    masks = got.reshape(n_dp * (slots + 1), words, tile)
    state_shape = jax.ShapeDtypeStruct((2 * blocks, st_rows, tile), F32)
    half_shape = jax.ShapeDtypeStruct((blocks, st_rows, tile), F32)
    state = None
    for g in range(3):
        mine_bufs = bufs[starts[g] : ends[g]]
        first, last = g == 0, g == 2
        scratch = [
            pltpu.VMEM((2 * blocks, sc_rows, tile), F32),
            pltpu.VMEM((len(mine_bufs), half, pay_rows, tile), BF16),
        ]
        if last:
            scratch = [pltpu.VMEM(state_shape.shape, F32)] + scratch
        extra = [] if first else [state]
        state = pl.pallas_call(
            functools.partial(stage_kernel, g, total, first, last, len(mine_bufs)),
            out_shape=(half_shape, half_shape) if last else state_shape,
            in_specs=[SMEM, SMEM] + [VMEM] * (4 + len(mine_bufs) + len(extra)),
            out_specs=(VMEM, VMEM) if last else VMEM,
            scratch_shapes=scratch,
            name=f"stage{g}",
        )(lists, counts, masks, own_sc, other_sc, att, *mine_bufs, *extra)
    own, other = state
    back = lax.ppermute(other, "dp", swap)
    return pl.pallas_call(
        merge_kernel,
        out_shape=jax.ShapeDtypeStruct((dims, nodes), BF16),
        in_specs=[VMEM] * 4,
        out_specs=VMEM,
        name="merge",
    )(own, back, node_feats, out_bias[:, None])


def solution(mesh):
    return jax.shard_map(
        local,
        mesh=mesh,
        in_specs=(
            P("mp", "dp"),
            P("mp", None),
            P("mp"),
            P("mp"),
            P("mp"),
            P("dp"),
            P("dp"),
            P("dp", None, None),
        ),
        out_specs=P("mp", "dp"),
        check_vma=False,
    )
```

```python
import functools

import jax
import jax.numpy as jnp
from jax import lax
from jax.experimental import pallas as pl
from jax.experimental.pallas import tpu as pltpu
from jax.sharding import PartitionSpec as P


HD = 32
LOG2E = 1.4426950408889634
FAR = -1e30
F32 = jnp.float32
BF16 = jnp.bfloat16


GROUP = 2
LIMIT = 16 * 1024 * 1024

VMEM = pl.BlockSpec(memory_space=pltpu.VMEM)
SMEM = pl.BlockSpec(memory_space=pltpu.SMEM)


def split(value, size):
    if size & (size - 1) == 0:
        return value >> (size.bit_length() - 1), value & (size - 1)
    return lax.div(value, jnp.int32(size)), lax.rem(value, jnp.int32(size))


def pad8(count):
    return -(-count // 8) * 8


def leaky(scores):
    return jnp.maximum(scores, 0.2 * scores)


def head_sums(rows):
    return jnp.sum(rows.reshape(rows.shape[0] // HD, HD, rows.shape[1]), axis=1)


def stack_rows(pieces, total):
    have = sum(p.shape[0] for p in pieces)
    if have < total:
        pieces = pieces + [jnp.zeros((total - have, pieces[0].shape[1]), F32)]
    return jnp.concatenate(pieces, axis=0)


def ring_order(chips):
    columns = max(1, chips // 4)
    rows = chips // columns
    if columns == 1:
        return list(range(chips))
    order = [row * columns for row in range(rows)]
    for row in reversed(range(rows)):
        inner = list(range(1, columns))
        order += [row * columns + col for col in (inner if (rows - 1 - row) % 2 == 0 else inner[::-1])]
    return order


def project_kernel(parts, mp_ref, w_ref, att_ref, *refs):
    x_refs, (pay_ref, sc_ref) = refs[:parts], refs[parts:]
    me = mp_ref[0]
    depth = w_ref.shape[1] // parts
    total = None
    for k in range(parts):
        at = pl.multiple_of((me ^ k) * depth, depth) if parts > 1 else 0
        term = jnp.dot(w_ref[:, pl.ds(at, depth)], x_refs[k][...], preferred_element_type=F32)
        total = term if total is None else total + term
    rounded = total.astype(BF16)
    a_src, a_dst = att_ref[:, 0:1], att_ref[:, 1:2]
    source = head_sums(total * a_src)
    target = head_sums(total * a_dst)
    rest = source - head_sums(rounded.astype(F32) * a_src)
    rest_hi = rest.astype(BF16).astype(F32)
    extra = stack_rows([rest_hi, rest - rest_hi], pay_ref.shape[1] - rounded.shape[0]).astype(BF16)
    scores = stack_rows([target, leaky(source + target)], sc_ref.shape[1])
    dims, tile = rounded.shape[0], pay_ref.shape[2]
    for b in range(pay_ref.shape[0]):
        at = slice(b * tile, (b + 1) * tile)
        pay_ref[b, :dims, :] = rounded[:, at]
        pay_ref[b, dims:, :] = extra[:, at]
        sc_ref[b] = scores[:, at]


def pack_kernel(blocks, chips, groups, rows_ref, cols_ref, place_ref, masks_ref, out_ref, count):
    devices, slots = out_ref.shape[0], out_ref.shape[1] - 1
    words = out_ref.shape[2:]
    half = blocks // 2
    lane = lax.broadcasted_iota(jnp.int32, words, 1)
    for d in range(devices):
        count[d] = 0
        out_ref[d, slots] = jnp.zeros(words, jnp.int32)

    def body(t, carry):
        row, col = rows_ref[t], cols_ref[t]
        owner, row_at = split(row, blocks)
        holder, col_at = split(col, blocks)
        parity = holder & 1
        other = (owner ^ parity) & 1
        goal = (owner & -2) + parity
        at = count[goal]
        count[goal] = at + 1
        out_ref[goal, at] = masks_ref[t]
        back = place_ref[owner >> 1] - place_ref[holder >> 1]
        back = jnp.where(back < 0, back + chips, back)
        step = jnp.minimum(back, chips - back)
        part, j = split(col_at, half)
        far = 2 * back == chips
        buf = part + jnp.where((back > step) & ~far, 2, 0)
        group = step + jnp.where(far & (other == 0), 1, 0)
        code = (((row_at + other * blocks) * 4 + buf) * half + j) * groups + group
        here = out_ref[goal, slots]
        here = jnp.where(lane == at, code, jnp.where(lane == slots, at + 1, here))
        out_ref[goal, slots] = here
        return carry

    lax.fori_loop(0, rows_ref.shape[0], body, 0)


def list_kernel(devices, slots, groups, ids_ref, list_ref, count_ref):
    total = list_ref.shape[0] // groups
    for g in range(groups):
        count_ref[g] = 0

    for d in range(devices):
        def body(n, carry, d=d):
            code, group = split(ids_ref[d * (slots + 1) + n], groups)
            at = count_ref[group]
            list_ref[group * total + at] = (code * (devices * (slots + 1)) + d * (slots + 1) + n) * 2 + 1
            count_ref[group] = at + 1
            return carry

        lax.fori_loop(0, ids_ref[d * (slots + 1) + slots], body, 0)
    for g in range(groups):
        at = count_ref[g]
        for k in range(GROUP - 1):
            list_ref[g * total + at + k] = 0
        count_ref[g] = lax.div(at + GROUP - 1, jnp.int32(GROUP))


def tile_bundle(entries, masks_total, half, dims, masks_ref, tscore, att, buf, state):
    heads = dims // HD
    tile = masks_ref.shape[2]
    up = 31 - lax.broadcasted_iota(jnp.int32, (32, tile), 0)
    work = []
    for entry in entries:
        valid = -(entry & 1)
        code, slot = split(entry >> 1, masks_total)
        code, at = split(code, half)
        row, which = split(code, 4)
        packed = masks_ref[slot] & valid
        block = [
            jnp.where((jnp.broadcast_to(packed[w : w + 1], (32, tile)) << up) < 0, 0.0, FAR)
            for w in range(packed.shape[0])
        ]
        block = jnp.concatenate(block, axis=0)
        feats = buf[which, at, :dims, :]
        extra = buf[which, at, dims:, :].astype(F32)
        source = head_sums(feats.astype(F32) * att) + extra[:heads] + extra[heads : 2 * heads]
        columns = jnp.transpose(stack_rows([source], pad8(heads)))
        tops = [
            jnp.max(jnp.broadcast_to(columns[:, h : h + 1], (tile, tile)) + block, axis=0, keepdims=True)
            for h in range(heads)
        ]
        work.append((row, feats, block, columns, jnp.concatenate(tops, axis=0)))
    moved = []
    for row, _, _, _, tops in work:
        target = tscore[row, :heads, :]
        old = state[row, dims : dims + heads, :]
        new = jnp.maximum(old, leaky(target + tops))
        state[row, dims : dims + heads, :] = new
        moved.append((jnp.exp2(old - new), target - new, 0.2 * target - new))
    sums = []
    for (row, feats, block, columns, _), (alpha, up1, up2) in zip(work, moved):
        masses, values = [], []
        for h in range(heads):
            col = jnp.broadcast_to(columns[:, h : h + 1], (tile, tile))
            low = jnp.broadcast_to(0.2 * columns[:, h : h + 1], (tile, tile))
            raw = jnp.maximum(col + up1[h : h + 1], low + up2[h : h + 1])
            weight = jnp.exp2(raw + block)
            masses.append(jnp.sum(weight, axis=0, keepdims=True))
            values.append(
                jnp.dot(
                    feats[h * HD : (h + 1) * HD], weight.astype(BF16), preferred_element_type=F32
                )
            )
        sums.append((jnp.concatenate(masses, axis=0), values))
    for (row, _, _, _, _), (alpha, _, _), (mass, values) in zip(work, moved, sums):
        at = slice(dims + heads, dims + 2 * heads)
        state[row, at, :] = state[row, at, :] * alpha + mass
        for h in range(heads):
            at = slice(h * HD, (h + 1) * HD)
            state[row, at, :] = state[row, at, :] * alpha[h : h + 1] + values[h]


def stage_kernel(group, groups, first, hand, list_ref, count_ref, masks_ref, own_sc, other_sc, att_ref, *refs):
    if hand:
        *refs, other_out, tscore, buf = refs
        refs = [*refs, tscore, buf]
    if first:
        *pays, state, tscore, buf = refs
    else:
        *pays, _, state, tscore, buf = refs
    total = list_ref.shape[0] // groups
    blocks, dims = own_sc.shape[0], att_ref.shape[0]
    half = buf.shape[1]
    heads = dims // HD
    for k, pay in enumerate(pays):
        buf[k] = pay[...]
    tscore[:blocks] = own_sc[...]
    tscore[blocks:] = other_sc[...]
    if first:
        tile = state.shape[2]
        rest = state.shape[1] - dims - 2 * heads
        for b in range(blocks):
            state[b, :dims] = pays[b // half][b % half, :dims].astype(F32)
            state[b, dims : dims + heads] = own_sc[b, heads : 2 * heads]
            state[b, dims + heads : dims + 2 * heads] = jnp.ones((heads, tile), F32)
            state[blocks + b, :dims] = jnp.zeros((dims, tile), F32)
            state[blocks + b, dims : dims + heads] = jnp.full((heads, tile), FAR, F32)
            state[blocks + b, dims + heads :] = jnp.zeros((heads + rest, tile), F32)
            if rest:
                state[b, dims + 2 * heads :] = jnp.zeros((rest, tile), F32)
    att = att_ref[:, 0:1]

    def body(i, carry):
        at = group * total + i * GROUP
        entries = [list_ref[at + k] for k in range(GROUP)]
        tile_bundle(entries, masks_ref.shape[0], half, dims, masks_ref, tscore, att, buf, state)
        return carry

    lax.fori_loop(0, count_ref[group], body, 0)
    if hand:
        other_out[...] = state[blocks:]


def merge_kernel(state_ref, other_ref, x_ref, bias_ref, out_ref):
    blocks, dims, tile = other_ref.shape[0], x_ref.shape[0], other_ref.shape[2]
    heads = dims // HD
    bias = bias_ref[...]
    for b in range(blocks):
        m1, m2 = state_ref[b, dims : dims + heads], other_ref[b, dims : dims + heads]
        l1 = state_ref[b, dims + heads : dims + 2 * heads]
        l2 = other_ref[b, dims + heads : dims + 2 * heads]
        best = jnp.maximum(m1, m2)
        c1, c2 = jnp.exp2(m1 - best), jnp.exp2(m2 - best)
        scale = 1.0 / (l1 * c1 + l2 * c2)
        c1, c2 = (c1 * scale)[:, None, :], (c2 * scale)[:, None, :]
        mixed = state_ref[b, :dims].reshape(heads, HD, tile) * c1
        mixed = mixed + other_ref[b, :dims].reshape(heads, HD, tile) * c2
        at = slice(b * tile, (b + 1) * tile)
        v = mixed.reshape(dims, tile) + x_ref[:, at].astype(F32) + bias
        out_ref[:, at] = jnp.where(v > 0, v, jnp.exp(jnp.minimum(v, 0.0)) - 1.0).astype(BF16)


def call(kernel, outs, args, in_specs=None, out_specs=VMEM, scratch=(), aliases=None, flops=1000000):
    return pl.pallas_call(
        kernel,
        out_shape=outs,
        in_specs=in_specs or [VMEM] * len(args),
        out_specs=out_specs,
        scratch_shapes=list(scratch),
        input_output_aliases=aliases or {},
        compiler_params=pltpu.CompilerParams(vmem_limit_bytes=LIMIT),
        cost_estimate=pl.CostEstimate(flops=flops, bytes_accessed=0, transcendentals=0),
    )(*args)


def near(x):
    return pltpu.with_memory_space_constraint(x, pltpu.VMEM)


def local(node_feats, proj_weight, att_src, att_dst, out_bias, tile_rows, tile_cols, tile_masks):
    nodes = node_feats.shape[1]
    dims = proj_weight.shape[0]
    heads = dims // HD
    words, tile = tile_masks.shape[1:]
    blocks = nodes // tile
    tiles = tile_rows.shape[0]
    n_dp, n_mp = lax.axis_size("dp"), lax.axis_size("mp")
    chips = n_dp // 2
    slots = 2 * max(2, 2 * tiles // n_dp)
    half = blocks // 2
    extra = pad8(2 * heads)
    order = ring_order(chips)
    place = [order.index(c) for c in range(chips)]
    me_mp = lax.axis_index("mp")
    steps = chips // 2
    groups = 8
    while groups < steps + 2:
        groups *= 2

    def hop(step):
        pairs = []
        for p, c in enumerate(order):
            to = order[(p + step) % chips]
            pairs += [(2 * c, 2 * to), (2 * c + 1, 2 * to + 1)]
        return sorted(pairs)

    right, left = hop(1), hop(-1)
    swap = [(i, i ^ 1) for i in range(n_dp)]

    mine = jnp.full((1,), me_mp, jnp.int32)
    if n_mp == 2:
        flip = [(0, 1), (1, 0)]
        halves = [node_feats[:, k * (nodes // 2) : (k + 1) * (nodes // 2)] for k in range(2)]
        inputs = [[x, lax.ppermute(x, "mp", flip)] for x in halves]
    else:
        whole = lax.all_gather(node_feats, "mp", axis=0, tiled=True)
        inputs = [[whole[:, k * (nodes // 2) : (k + 1) * (nodes // 2)]] for k in range(2)]
    att = jnp.stack([att_src, att_dst], axis=1) * LOG2E

    packed = call(
        functools.partial(pack_kernel, blocks, chips, groups),
        pltpu.VMEM((n_dp, slots + 1, words, tile), jnp.int32),
        (tile_rows, tile_cols, jnp.array(place, jnp.int32), tile_masks),
        in_specs=[SMEM, SMEM, SMEM, VMEM],
        scratch=[pltpu.SMEM((n_dp,), jnp.int32)],
    )
    got = lax.all_to_all(packed, "dp", split_axis=0, concat_axis=0, tiled=True)

    pays, scs = [], []
    for xs in inputs:
        pay, sc = call(
            functools.partial(project_kernel, len(xs)),
            (pltpu.VMEM((half, dims + extra, tile), BF16), pltpu.VMEM((half, extra, tile), F32)),
            (mine, proj_weight, att, *[near(x) for x in xs]),
            in_specs=[SMEM] + [VMEM] * (2 + len(xs)),
            out_specs=(VMEM, VMEM),
        )
        pays.append(pay)
        scs.append(sc)
    own_sc = jnp.concatenate(scs, axis=0)
    other_sc = lax.ppermute(own_sc, "dp", swap)

    arrivals = [list(pays)]
    going = {w + p: pays["AB".index(p)] for w in "rl" for p in "AB"}
    for k in range(1, steps + 1):
        far = 2 * k == chips
        for way in ("rA", "lB") if far else ("rA", "lA", "rB", "lB"):
            pairs = right if way[0] == "r" else left
            going[way] = lax.ppermute(going[way], "dp", pairs)
        names = ("rA", "lB") if far else ("rA", "rB", "lA", "lB")
        arrivals.append([going[w] for w in names])

    ids = got[:, slots, 0, : slots + 1].reshape(n_dp * (slots + 1))
    total = n_dp * slots + GROUP
    lists, counts = call(
        functools.partial(list_kernel, n_dp, slots, groups),
        (
            jax.ShapeDtypeStruct((groups * total,), jnp.int32),
            jax.ShapeDtypeStruct((groups,), jnp.int32),
        ),
        (ids,),
        in_specs=[SMEM],
        out_specs=(SMEM, SMEM),
    )

    masks = near(got.reshape(n_dp * (slots + 1), words, tile))
    near_sc = (near(own_sc), near(other_sc))
    state_shape = pltpu.VMEM((2 * blocks, dims + extra, tile), F32)

    half_shape = pltpu.VMEM((blocks, dims + extra, tile), F32)

    def stage(g, bufs, state, hand=False):
        args = [lists, counts, masks, *near_sc, att, *[near(b) for b in bufs]]
        if state is not None:
            args.append(near(state))
        return call(
            functools.partial(stage_kernel, g, groups, state is None, hand),
            (state_shape, half_shape) if hand else state_shape,
            args,
            out_specs=(VMEM, VMEM) if hand else VMEM,
            in_specs=[SMEM, SMEM] + [VMEM] * (len(args) - 2),
            scratch=[
                pltpu.VMEM((2 * blocks, extra, tile), F32),
                pltpu.VMEM((len(bufs), half, dims + extra, tile), BF16),
            ],
            aliases={} if state is None else {len(args) - 1: 0},
            flops=8000000000,
        )

    state = None
    for g, bufs in enumerate(arrivals):
        state = stage(g, bufs, state, g == steps)
    state, other = state
    back = lax.ppermute(other, "dp", swap)
    state = stage(steps + 1, arrivals[-1], state)
    return call(
        merge_kernel,
        jax.ShapeDtypeStruct((dims, nodes), BF16),
        (near(state), near(back), node_feats, out_bias[:, None]),
    )


def solution(mesh):
    return jax.shard_map(
        local,
        mesh=mesh,
        in_specs=(
            P("mp", "dp"),
            P("mp", None),
            P("mp"),
            P("mp"),
            P("mp"),
            P("dp"),
            P("dp"),
            P("dp", None, None),
        ),
        out_specs=P("mp", "dp"),
        check_vma=False,
    )
```

```python
import functools

import jax
import jax.numpy as jnp
from jax import lax
from jax.experimental import pallas as pl
from jax.experimental.pallas import tpu as pltpu
from jax.sharding import PartitionSpec as P


HD = 32
LOG2E = 1.4426950408889634
FAR = -1e30
F32 = jnp.float32
BF16 = jnp.bfloat16


WIDE = 1
LIMIT = 16 * 1024 * 1024

VMEM = pl.BlockSpec(memory_space=pltpu.VMEM)
SMEM = pl.BlockSpec(memory_space=pltpu.SMEM)


def split(value, size):
    if size & (size - 1) == 0:
        return value >> (size.bit_length() - 1), value & (size - 1)
    return lax.div(value, jnp.int32(size)), lax.rem(value, jnp.int32(size))


def pad8(count):
    return -(-count // 8) * 8


def leaky(scores):
    return jnp.maximum(scores, 0.2 * scores)


def head_sums(rows):
    return jnp.sum(rows.reshape(rows.shape[0] // HD, HD, rows.shape[1]), axis=1)


def stack_rows(pieces, total):
    have = sum(p.shape[0] for p in pieces)
    if have < total:
        pieces = pieces + [jnp.zeros((total - have, pieces[0].shape[1]), F32)]
    return jnp.concatenate(pieces, axis=0)


def ring_order(chips):
    columns = max(1, chips // 4)
    rows = chips // columns
    if columns == 1:
        return list(range(chips))
    order = [row * columns for row in range(rows)]
    for row in reversed(range(rows)):
        inner = list(range(1, columns))
        order += [row * columns + col for col in (inner if (rows - 1 - row) % 2 == 0 else inner[::-1])]
    return order


def column(row_ref):
    return jnp.transpose(jnp.broadcast_to(row_ref[...], (8, row_ref.shape[1])))[:, 0:1]


def project_kernel(parts, base, mp_ref, w_ref, src_ref, dst_ref, *refs):
    x_refs, (pay_ref, sc_ref) = refs[:parts], refs[-2:]
    me = mp_ref[0]
    depth = w_ref.shape[1] // parts
    total = None
    for k in range(parts):
        at = pl.multiple_of((me ^ k) * depth, depth) if parts > 1 else 0
        term = jnp.dot(w_ref[:, pl.ds(at, depth)], x_refs[k][...], preferred_element_type=F32)
        total = term if total is None else total + term
    rounded = total.astype(BF16)
    a_src, a_dst = column(src_ref) * LOG2E, column(dst_ref) * LOG2E
    source = head_sums(total * a_src)
    target = head_sums(total * a_dst)
    rest = source - head_sums(rounded.astype(F32) * a_src)
    rest_hi = rest.astype(BF16).astype(F32)
    extra = stack_rows([rest_hi, rest - rest_hi], pay_ref.shape[1] - rounded.shape[0]).astype(BF16)
    scores = stack_rows([target, leaky(source + target)], sc_ref.shape[1])
    dims, tile = rounded.shape[0], pay_ref.shape[2]
    for b in range(pay_ref.shape[0]):
        at = slice(b * tile, (b + 1) * tile)
        pay_ref[b, :dims, :] = rounded[:, at]
        pay_ref[b, dims:, :] = extra[:, at]
        sc_ref[base + b] = scores[:, at]


def open_kernel(halves, *refs):
    count = (len(refs) - halves) // 2
    sources, outs, sems = refs[:count], refs[count:-1], refs[-1]
    size = outs[0].shape[1]
    sources = [sources[0].at[:, k * size : (k + 1) * size] for k in range(halves)] + list(sources[1:])
    copies = [pltpu.make_async_copy(v, w, sems.at[k]) for k, (v, w) in enumerate(zip(sources, outs))]
    for copy in copies:
        copy.start()
    for copy in copies:
        copy.wait()


def pack_kernel(blocks, place, groups, rows_in, cols_in, masks_in, out_ref, rows_ref, cols_ref, masks_ref, count, place_ref, sems):
    ins, tos = (rows_in, cols_in, masks_in), (rows_ref, cols_ref, masks_ref)
    copies = [pltpu.make_async_copy(v, w, sems.at[k]) for k, (v, w) in enumerate(zip(ins, tos))]
    for copy in copies:
        copy.start()
    devices, slots = out_ref.shape[0], out_ref.shape[1] - 1
    words = out_ref.shape[2:]
    half = blocks // 2
    chips = len(place)
    lane = lax.broadcasted_iota(jnp.int32, words, 1)
    for c in range(chips):
        place_ref[c] = place[c]
    for d in range(devices):
        count[d] = 0
        out_ref[d, slots] = jnp.zeros(words, jnp.int32)
    for copy in copies:
        copy.wait()

    def body(t, carry):
        row, col = rows_ref[t], cols_ref[t]
        owner, row_at = split(row, blocks)
        holder, col_at = split(col, blocks)
        at = count[owner]
        count[owner] = at + 1
        out_ref[owner, at] = masks_ref[t]
        back = place_ref[owner >> 1] - place_ref[holder >> 1]
        back = jnp.where(back < 0, back + chips, back)
        step = jnp.minimum(back, chips - back)
        part, j = split(col_at, half)
        last = 2 * back == chips
        spot = col_at + jnp.where(back > step, blocks, 0) + jnp.where(step == 1, blocks, 0)
        before = step == chips // 2 - 1
        spot = jnp.where(before, j + jnp.where(back > step, half, 0), jnp.where(last, j, spot))
        group = jnp.where(step > 0, step - 1, 0) + jnp.where(before | last, part, 0) + jnp.where(last, 1, 0)
        code = ((row_at * (4 * blocks) + spot) * 2 + (holder & 1)) * groups + group
        here = out_ref[owner, slots]
        here = jnp.where(lane == at, code, jnp.where(lane == slots, at + 1, here))
        out_ref[owner, slots] = here
        return carry

    lax.fori_loop(0, rows_ref.shape[0], body, 0)


def list_kernel(devices, slots, groups, blocks, final, core_ref, own_ids, other_ids, own_masks, other_masks, list_ref, count_ref, masks_ref):
    total = list_ref.shape[0] // groups
    width = devices * (slots + 1)
    core = core_ref[0]
    for g in range(groups):
        count_ref[g] = 0
    for side, (ids, masks) in enumerate(((own_ids, own_masks), (other_ids, other_masks))):
        masks_ref[side * width : (side + 1) * width] = masks[...]
        for d in range(devices):
            base = d * (slots + 1)

            def body(n, carry, side=side, ids=ids, base=base):
                code, group = split(ids[base + n], groups)

                @pl.when((code & 1) == core)
                def _():
                    code_here = (code >> 1) + side * (4 * blocks * blocks)
                    to = group if side else group + jnp.where(group == final, 1, 0)
                    at = count_ref[to]
                    list_ref[to * total + at] = (code_here * (2 * width) + side * width + base + n) * 2 + 1
                    count_ref[to] = at + 1

                return carry

            lax.fori_loop(0, ids[base + slots], body, 0)
    for g in range(groups):
        at = count_ref[g]
        for k in range(3 * WIDE):
            list_ref[g * total + at + k] = 0
        count_ref[g] = lax.div(at + 2 * WIDE - 1, 2 * WIDE)


def prepare(entry, fields, heads, dims, masks_ref, att, buf, edges, tops):
    _, spot, slot = fields
    tile = masks_ref.shape[2]
    up = 31 - lax.broadcasted_iota(jnp.int32, (32, tile), 0)
    packed = masks_ref[slot] & -(entry & 1)
    block = [
        jnp.where((jnp.broadcast_to(packed[w : w + 1], (32, tile)) << up) < 0, 0.0, FAR)
        for w in range(packed.shape[0])
    ]
    block = jnp.concatenate(block, axis=0)
    feats = buf[spot, :dims, :]
    extra = buf[spot, dims:, :].astype(F32)
    source = head_sums(feats.astype(F32) * att) + extra[:heads] + extra[heads : 2 * heads]
    columns = jnp.transpose(stack_rows([source], pad8(heads)))
    for h in range(heads):
        edge = jnp.broadcast_to(columns[:, h : h + 1], (tile, tile)) + block
        edges[h] = edge
        tops[h : h + 1, :] = jnp.max(edge, axis=0, keepdims=True)


def absorb(fields, heads, dims, tscore, buf, edges, tops, state):
    row, spot, _ = fields
    tile = state.shape[2]
    ones = jnp.ones((16, tile), BF16)
    target = tscore[row, :heads, :]
    old = state[row, dims : dims + heads, :]
    new = jnp.maximum(old, leaky(target + tops[:heads, :]))
    state[row, dims : dims + heads, :] = new
    alpha, up1, up2 = jnp.exp2(old - new), target - new, 0.2 * target - new
    values = []
    for h in range(heads):
        edge = edges[h]
        raw = jnp.maximum(edge + up1[h : h + 1], 0.2 * edge + up2[h : h + 1])
        weight = jnp.exp2(raw).astype(BF16)
        left = jnp.concatenate([buf[spot, h * HD : (h + 1) * HD, :], ones], axis=0)
        values.append(jnp.dot(left, weight, preferred_element_type=F32))
    at = slice(dims + heads, dims + 2 * heads)
    mass = jnp.concatenate([v[HD : HD + 1] for v in values], axis=0)
    state[row, at, :] = state[row, at, :] * alpha + mass
    for h in range(heads):
        at = slice(h * HD, (h + 1) * HD)
        state[row, at, :] = state[row, at, :] * alpha[h : h + 1] + values[h][:HD]


def stage_kernel(group, groups, first, count, list_ref, count_ref, masks_ref, own_sc, other_sc, src_ref, *refs):
    pays, (tscore, buf, edges0, edges1, tops0, tops1) = refs[:count], refs[-6:]
    outs = refs[count if first else count + 1 : -6]
    state = outs[0]
    total = list_ref.shape[0] // groups
    blocks, dims = own_sc.shape[0], src_ref.shape[1]
    heads = dims // HD
    base = 0
    for pay in pays:
        buf[base : base + pay.shape[0]] = pay[...]
        base += pay.shape[0]
    tscore[:blocks] = own_sc[...]
    tscore[blocks:] = other_sc[...]
    if first:
        tile = state.shape[2]
        rest = state.shape[1] - dims - 2 * heads
        for b in range(blocks):
            state[b, :dims] = buf[b, :dims].astype(F32)
            state[b, dims : dims + heads] = own_sc[b, heads : 2 * heads]
            state[b, dims + heads : dims + 2 * heads] = jnp.ones((heads, tile), F32)
            state[blocks + b, :dims] = jnp.zeros((dims, tile), F32)
            state[blocks + b, dims : dims + heads] = jnp.full((heads, tile), 0.1 * FAR, F32)
            state[blocks + b, dims + heads :] = jnp.zeros((heads + rest, tile), F32)
            if rest:
                state[b, dims + 2 * heads :] = jnp.zeros((rest, tile), F32)
    att = column(src_ref) * LOG2E
    spaces = ((edges0, tops0), (edges1, tops1))

    def fields(entry):
        code, slot = split(entry >> 1, masks_ref.shape[0])
        row, spot = split(code, 4 * blocks)
        return row, spot, slot

    def ready(n, side):
        for k in range(WIDE):
            entry = list_ref[group * total + n * WIDE + k]
            space = [v.at[k] for v in spaces[side]]
            prepare(entry, fields(entry), heads, dims, masks_ref, att, buf, *space)

    def take(n, side):
        for k in range(WIDE):
            entry = list_ref[group * total + n * WIDE + k]
            space = [v.at[k] for v in spaces[side]]
            absorb(fields(entry), heads, dims, tscore, buf, *space, state)

    def body(i, carry):
        ready(2 * i + 1, 1)
        take(2 * i, 0)
        ready(2 * i + 2, 0)
        take(2 * i + 1, 1)
        return carry

    ready(0, 0)
    lax.fori_loop(0, count_ref[group], body, 0)
    if len(outs) > 1:
        outs[1][...] = state[blocks:]


def merge_kernel(state_ref, other_ref, x_ref, bias_ref, out_ref):
    blocks, dims, tile = other_ref.shape[0], x_ref.shape[0], other_ref.shape[2]
    heads = dims // HD
    bias = column(bias_ref)
    for b in range(blocks):
        m1, m2 = state_ref[b, dims : dims + heads], other_ref[b, dims : dims + heads]
        l1 = state_ref[b, dims + heads : dims + 2 * heads]
        l2 = other_ref[b, dims + heads : dims + 2 * heads]
        best = jnp.maximum(m1, m2)
        c1, c2 = jnp.exp2(m1 - best), jnp.exp2(m2 - best)
        scale = 1.0 / (l1 * c1 + l2 * c2)
        c1, c2 = (c1 * scale)[:, None, :], (c2 * scale)[:, None, :]
        mixed = state_ref[b, :dims].reshape(heads, HD, tile) * c1
        mixed = mixed + other_ref[b, :dims].reshape(heads, HD, tile) * c2
        at = slice(b * tile, (b + 1) * tile)
        v = mixed.reshape(dims, tile) + x_ref[:, at].astype(F32) + bias
        out_ref[:, at] = jnp.where(v > 0, v, jnp.exp(jnp.minimum(v, 0.0)) - 1.0).astype(BF16)


def call(kernel, outs, args, in_specs=None, out_specs=VMEM, scratch=(), aliases=None, flops=1000000):
    return pl.pallas_call(
        kernel,
        out_shape=outs,
        in_specs=in_specs or [VMEM] * len(args),
        out_specs=out_specs,
        scratch_shapes=list(scratch),
        input_output_aliases=aliases or {},
        compiler_params=pltpu.CompilerParams(vmem_limit_bytes=LIMIT),
        cost_estimate=pl.CostEstimate(flops=flops, bytes_accessed=0, transcendentals=0),
    )(*args)


def near(x):
    return pltpu.with_memory_space_constraint(x, pltpu.VMEM)


def far(x):
    return pltpu.with_memory_space_constraint(x, pltpu.HBM)


def local(node_feats, proj_weight, att_src, att_dst, out_bias, tile_rows, tile_cols, tile_masks):
    nodes = node_feats.shape[1]
    dims = proj_weight.shape[0]
    heads = dims // HD
    words, tile = tile_masks.shape[1:]
    blocks = nodes // tile
    tiles = tile_rows.shape[0]
    n_dp, n_mp = lax.axis_size("dp"), lax.axis_size("mp")
    chips = n_dp // 2
    slots = max(2, 2 * tiles // n_dp)
    half = blocks // 2
    extra = pad8(2 * heads)
    order = ring_order(chips)
    place = [order.index(c) for c in range(chips)]
    me_mp = lax.axis_index("mp")
    steps = chips // 2
    groups = 8
    while groups < steps + 3:
        groups *= 2

    def hop(step):
        pairs = []
        for p, c in enumerate(order):
            to = order[(p + step) % chips]
            pairs += [(2 * c, 2 * to), (2 * c + 1, 2 * to + 1)]
        return sorted(pairs)

    right, left = hop(1), hop(-1)
    swap = [(i, i ^ 1) for i in range(n_dp)]

    mine = jnp.full((1,), me_mp, jnp.int32)
    core = jnp.full((1,), lax.axis_index("dp") & 1, jnp.int32)
    parts = 2 if n_mp == 2 else 1
    moved = [node_feats, proj_weight, att_src.reshape(1, dims), att_dst.reshape(1, dims)]
    shapes = [(node_feats.shape[0], nodes // parts)] * parts + [v.shape for v in moved[1:]]
    kinds = [BF16] * (parts + 1) + [F32] * 2
    anywhere = pl.BlockSpec(memory_space=pl.ANY)
    *cuts, weight, a_src, a_dst = call(
        functools.partial(open_kernel, parts),
        [pltpu.VMEM(v, k) for v, k in zip(shapes, kinds)],
        [far(v) for v in moved],
        in_specs=[anywhere] * len(moved),
        out_specs=[VMEM] * len(shapes),
        scratch=[pltpu.SemaphoreType.DMA((len(shapes),))],
    )
    if n_mp == 2:
        flip = [(0, 1), (1, 0)]
        inputs = [[x, lax.ppermute(x, "mp", flip)] for x in cuts]
    else:
        whole = lax.all_gather(node_feats, "mp", axis=0, tiled=True)
        inputs = [[whole[:, k * (nodes // 2) : (k + 1) * (nodes // 2)]] for k in range(2)]
    att = (a_src, a_dst)

    packed = call(
        functools.partial(pack_kernel, blocks, place, groups),
        pltpu.HBM((n_dp, slots + 1, words, tile), jnp.int32),
        [far(v) for v in (tile_rows, tile_cols, tile_masks)],
        in_specs=[anywhere] * 3,
        scratch=[
            pltpu.SMEM(tile_rows.shape, jnp.int32),
            pltpu.SMEM(tile_cols.shape, jnp.int32),
            pltpu.VMEM(tile_masks.shape, jnp.int32),
            pltpu.SMEM((n_dp,), jnp.int32),
            pltpu.SMEM((chips,), jnp.int32),
            pltpu.SemaphoreType.DMA((3,)),
        ],
    )
    got = lax.all_to_all(packed, "dp", split_axis=0, concat_axis=0, tiled=True)
    got = got.reshape(n_dp * (slots + 1), words, tile)
    got_other = lax.ppermute(got, "dp", swap)

    pays, own_sc = [], None
    for k, xs in enumerate(inputs):
        args = [mine] + [near(v) for v in (weight, *att, *xs)]
        if own_sc is not None:
            args.append(near(own_sc))
        pay, own_sc = call(
            functools.partial(project_kernel, len(xs), k * half),
            (
                pltpu.VMEM((half, dims + extra, tile), BF16),
                pltpu.VMEM((blocks, extra, tile), F32),
            ),
            args,
            in_specs=[SMEM] + [VMEM] * (len(args) - 1),
            out_specs=(VMEM, VMEM),
            aliases={len(args) - 1: 1} if k else None,
        )
        pays.append(pay)
    other_sc = lax.ppermute(own_sc, "dp", swap)

    arrivals = []
    going = {w + p: pays["AB".index(p)] for w in "rl" for p in "AB"}
    for k in range(1, steps):
        for way in ("rA", "lA", "rB", "lB"):
            going[way] = lax.ppermute(going[way], "dp", right if way[0] == "r" else left)
        if k < steps - 1:
            arrivals.append([going[w] for w in ("rA", "rB", "lA", "lB")])
        else:
            arrivals += [[going[w] for w in ways] for ways in (("rA", "lA"), ("rB", "lB"))]
    arrivals[0] = pays + arrivals[0]
    for p in "AB":
        both = []
        for w, pairs, cut in (("r", right, slice(0, half // 2)), ("l", left, slice(half // 2, half))):
            both.append(lax.ppermute(going[w + p][cut], "dp", pairs))
        arrivals.append(both)

    width = n_dp * (slots + 1)
    total = 2 * n_dp * slots + 4 * WIDE
    ids = [v.reshape(n_dp, slots + 1, words, tile)[:, slots, 0, : slots + 1] for v in (got, got_other)]
    lists, counts, masks = call(
        functools.partial(list_kernel, n_dp, slots, groups, blocks, steps + 1),
        (
            jax.ShapeDtypeStruct((groups * total,), jnp.int32),
            jax.ShapeDtypeStruct((groups,), jnp.int32),
            pltpu.VMEM((2 * width, words, tile), jnp.int32),
        ),
        (core, *[v.reshape(width) for v in ids], near(got), near(got_other)),
        in_specs=[SMEM] * 3 + [VMEM] * 2,
        out_specs=(SMEM, SMEM, VMEM),
    )

    shared = [masks, own_sc, other_sc, att[0]]
    state_shape = pltpu.VMEM((2 * blocks, dims + extra, tile), F32)
    half_shape = pltpu.VMEM((blocks, dims + extra, tile), F32)

    def stage(g, bufs, state, hand=False):
        args = [lists, counts] + [near(v) for v in shared + bufs]
        outs, aliases = [state_shape], {}
        if state is not None:
            args.append(near(state))
            aliases[len(args) - 1] = 0
        if hand:
            outs.append(half_shape)
            for k, v in enumerate(shared + bufs):
                aliases[2 + k] = len(outs)
                outs.append(pltpu.VMEM(v.shape, v.dtype))
        return call(
            functools.partial(stage_kernel, g, groups, state is None, len(bufs)),
            outs,
            args,
            in_specs=[SMEM, SMEM] + [VMEM] * (len(args) - 2),
            out_specs=[VMEM] * len(outs),
            scratch=[
                pltpu.VMEM((2 * blocks, extra, tile), F32),
                pltpu.VMEM((sum(v.shape[0] for v in bufs), dims + extra, tile), BF16),
                *[pltpu.VMEM((WIDE, heads, tile, tile), F32)] * 2,
                *[pltpu.VMEM((WIDE, pad8(heads), tile), F32)] * 2,
            ],
            aliases=aliases,
            flops=8000000000,
        )

    state = None
    for g, bufs in enumerate(arrivals[:-1]):
        (state,) = stage(g, bufs, state)
    state, other, *rest = stage(steps + 1, arrivals[-1], state, True)
    back = lax.ppermute(other, "dp", swap)
    shared = rest[: len(shared)]
    (state,) = stage(steps + 2, rest[len(shared) :], state)
    return call(
        merge_kernel,
        jax.ShapeDtypeStruct((dims, nodes), BF16),
        (near(state), near(back), node_feats, out_bias.reshape(1, dims)),
    )


def solution(mesh):
    return jax.shard_map(
        local,
        mesh=mesh,
        in_specs=(
            P("mp", "dp"),
            P("mp", None),
            P("mp"),
            P("mp"),
            P("mp"),
            P("dp"),
            P("dp"),
            P("dp", None, None),
        ),
        out_specs=P("mp", "dp"),
        check_vma=False,
    )
```

```python
import functools
import math

import jax
import jax.numpy as jnp
from jax import lax
from jax.experimental import pallas as pl
from jax.experimental.pallas import tpu as pltpu
from jax.sharding import PartitionSpec as P


HD = 32
LOG2E = 1.4426950408889634
FAR = -1e30
F32 = jnp.float32
BF16 = jnp.bfloat16


WIDE = 2
LIMIT = 16 * 1024 * 1024

VMEM = pl.BlockSpec(memory_space=pltpu.VMEM)
SMEM = pl.BlockSpec(memory_space=pltpu.SMEM)


def split(value, size):
    if size & (size - 1) == 0:
        return value >> (size.bit_length() - 1), value & (size - 1)
    return lax.div(value, jnp.int32(size)), lax.rem(value, jnp.int32(size))


def pad8(count):
    return -(-count // 8) * 8


def leaky(scores):
    return jnp.maximum(scores, 0.2 * scores)


def head_sums(rows):
    return jnp.sum(rows.reshape(rows.shape[0] // HD, HD, rows.shape[1]), axis=1)


def stack_rows(pieces, total):
    have = sum(p.shape[0] for p in pieces)
    if have < total:
        pieces = pieces + [jnp.zeros((total - have, pieces[0].shape[1]), F32)]
    return jnp.concatenate(pieces, axis=0)


def ring_order(chips):
    columns = max(1, chips // 4)
    rows = chips // columns
    if columns == 1:
        return list(range(chips))
    order = [row * columns for row in range(rows)]
    for row in reversed(range(rows)):
        inner = list(range(1, columns))
        order += [row * columns + col for col in (inner if (rows - 1 - row) % 2 == 0 else inner[::-1])]
    return order


def column(row_ref):
    return jnp.transpose(jnp.broadcast_to(row_ref[...], (8, row_ref.shape[1])))[:, 0:1]


def project_kernel(parts, base, mp_ref, w_ref, src_ref, dst_ref, *refs):
    x_refs, (pay_ref, sc_ref) = refs[:parts], refs[-2:]
    me = mp_ref[0]
    depth = w_ref.shape[1] // parts
    total = None
    for k in range(parts):
        at = pl.multiple_of((me ^ k) * depth, depth) if parts > 1 else 0
        term = jnp.dot(w_ref[:, pl.ds(at, depth)], x_refs[k][...], preferred_element_type=F32)
        total = term if total is None else total + term
    rounded = total.astype(BF16)
    a_src, a_dst = column(src_ref) * LOG2E, column(dst_ref) * LOG2E
    source = head_sums(total * a_src)
    target = head_sums(total * a_dst)
    rest = source - head_sums(rounded.astype(F32) * a_src)
    rest_hi = rest.astype(BF16).astype(F32)
    extra = stack_rows([rest_hi, rest - rest_hi], pay_ref.shape[1] - rounded.shape[0]).astype(BF16)
    scores = stack_rows([target, leaky(source + target)], sc_ref.shape[1])
    dims, tile = rounded.shape[0], pay_ref.shape[2]
    for b in range(pay_ref.shape[0]):
        at = slice(b * tile, (b + 1) * tile)
        pay_ref[b, :dims, :] = rounded[:, at]
        pay_ref[b, dims:, :] = extra[:, at]
        sc_ref[base + b] = scores[:, at]


def open_kernel(halves, *refs):
    count = (len(refs) - halves) // 2
    sources, outs, sems = refs[:count], refs[count:-1], refs[-1]
    size = outs[0].shape[1]
    sources = [sources[0].at[:, k * size : (k + 1) * size] for k in range(halves)] + list(sources[1:])
    copies = [pltpu.make_async_copy(v, w, sems.at[k]) for k, (v, w) in enumerate(zip(sources, outs))]
    for copy in copies:
        copy.start()
    for copy in copies:
        copy.wait()


def pack_kernel(blocks, place, groups, rows_ref, cols_ref, masks_ref, out_ref, count, place_ref, codes):
    devices, slots = out_ref.shape[0], out_ref.shape[1] - 1
    words = out_ref.shape[2:]
    half = blocks // 2
    chips = len(place)
    width = slots + 2
    for c in range(chips):
        place_ref[c] = place[c]
    for d in range(devices):
        count[2 * d] = 0
        count[2 * d + 1] = 0
        for n in range(slots):
            codes[d * width + n] = 0

    def body(t, carry):
        row, col = rows_ref[t], cols_ref[t]
        owner, row_at = split(row, blocks)
        holder, col_at = split(col, blocks)
        odd = holder & 1
        have = count[2 * owner + odd]
        count[2 * owner + odd] = have + 1
        at = jnp.where(odd == 1, slots - 1 - have, have)
        out_ref[owner, at] = masks_ref[t]
        back = place_ref[owner >> 1] - place_ref[holder >> 1]
        back = jnp.where(back < 0, back + chips, back)
        step = jnp.minimum(back, chips - back)
        part, j = split(col_at, half)
        last = 2 * back == chips
        before = step == chips // 2 - 1
        spot = col_at + jnp.where(back > step, blocks, 0) + jnp.where(step == 1, blocks, 0)
        spot = jnp.where(before, j + jnp.where(back > step, half, 0), jnp.where(last, j, spot))
        group = jnp.where(step > 0, step - 1, 0) + jnp.where(before | last, part, 0) + jnp.where(last, 1, 0)
        codes[owner * width + at] = (row_at * (4 * blocks) + spot) * groups + group
        return carry

    lax.fori_loop(0, rows_ref.shape[0], body, 0)
    lane = lax.broadcasted_iota(jnp.int32, words, 1)
    for d in range(devices):
        here = jnp.zeros(words, jnp.int32)
        for n in range(slots):
            here = jnp.where(lane == n, codes[d * width + n], here)
        for n in range(2):
            here = jnp.where(lane == slots + n, count[2 * d + n], here)
        out_ref[d, slots] = here


def list_kernel(devices, slots, groups, blocks, final, core_ref, own_ids, other_ids, own_masks, other_masks, list_ref, count_ref, masks_ref):
    total = list_ref.shape[0] // groups
    width = devices * (slots + 1)
    core = core_ref[0]
    for g in range(groups):
        count_ref[g] = 0
    for side, (ids, masks) in enumerate(((own_ids, own_masks), (other_ids, other_masks))):
        masks_ref[side * width : (side + 1) * width] = masks[...]
        turn = 0 if side else 1

        def holder(d, carry, side=side, ids=ids, turn=turn):
            at_ids, at_slots = d * (slots + 2), d * (slots + 1) + side * width
            number = ids[at_ids + slots + core]
            base = jnp.where(core == 1, slots - number, 0)

            def body(n, carry):
                code, group = split(ids[at_ids + n], groups)
                to = group + jnp.where(group == final, turn, 0)
                at = count_ref[to]
                code = code + side * (4 * blocks * blocks)
                list_ref[to * total + at] = (code * (2 * width) + at_slots + n) * 2 + 1
                count_ref[to] = at + 1
                return carry

            return lax.fori_loop(base, base + number, body, carry)

        lax.fori_loop(0, devices, holder, 0)
    for g in range(groups):
        at = count_ref[g]
        for k in range(3 * WIDE):
            list_ref[g * total + at + k] = 0
        count_ref[g] = lax.div(at + WIDE - 1, WIDE)


def prepare(entry, fields, heads, dims, masks_ref, att, buf, edges, tops):
    _, spot, slot = fields
    tile = masks_ref.shape[2]
    up = 31 - lax.broadcasted_iota(jnp.int32, (32, tile), 0)
    packed = masks_ref[slot] & -(entry & 1)
    block = [
        jnp.where((jnp.broadcast_to(packed[w : w + 1], (32, tile)) << up) < 0, 0.0, FAR)
        for w in range(packed.shape[0])
    ]
    block = jnp.concatenate(block, axis=0)
    feats = buf[spot, :dims, :]
    extra = buf[spot, dims:, :].astype(F32)
    source = head_sums(feats.astype(F32) * att) + extra[:heads] + extra[heads : 2 * heads]
    columns = jnp.transpose(stack_rows([source], pad8(heads)))
    for h in range(heads):
        edge = jnp.broadcast_to(columns[:, h : h + 1], (tile, tile)) + block
        edges[h] = edge
        tops[h : h + 1, :] = jnp.max(edge, axis=0, keepdims=True)


def absorb(fields, heads, dims, tscore, buf, edges, tops, state):
    row, spot, _ = fields
    tile = state.shape[2]
    ones = jnp.ones((16, tile), BF16)
    target = tscore[row, :heads, :]
    old = state[row, dims : dims + heads, :]
    new = jnp.maximum(old, leaky(target + tops[:heads, :]))
    state[row, dims : dims + heads, :] = new
    alpha, up1, up2 = jnp.exp2(old - new), target - new, 0.2 * target - new
    values = []
    for h in range(heads):
        edge = edges[h]
        raw = jnp.maximum(edge + up1[h : h + 1], 0.2 * edge + up2[h : h + 1])
        weight = jnp.exp2(raw).astype(BF16)
        left = jnp.concatenate([buf[spot, h * HD : (h + 1) * HD, :], ones], axis=0)
        values.append(jnp.dot(left, weight, preferred_element_type=F32))
    at = slice(dims + heads, dims + 2 * heads)
    mass = jnp.concatenate([v[HD : HD + 1] for v in values], axis=0)
    state[row, at, :] = state[row, at, :] * alpha + mass
    for h in range(heads):
        at = slice(h * HD, (h + 1) * HD)
        state[row, at, :] = state[row, at, :] * alpha[h : h + 1] + values[h][:HD]


def stage_kernel(group, groups, first, short, count, list_ref, count_ref, masks_ref, own_sc, other_sc, src_ref, *refs):
    pays, (tscore, buf, edges0, edges1, tops0, tops1) = refs[:count], refs[-6:]
    outs = refs[count if first else count + 1 : -6]
    state = outs[0]
    total = list_ref.shape[0] // groups
    blocks, dims = own_sc.shape[0], src_ref.shape[1]
    heads = dims // HD
    base = 0
    for pay in pays:
        buf[base : base + pay.shape[0]] = pay[...]
        base += pay.shape[0]
    tscore[:blocks] = own_sc[...]
    tscore[blocks:] = other_sc[...]
    if first:
        tile = state.shape[2]
        rest = state.shape[1] - dims - 2 * heads
        for b in range(blocks):
            state[b, :dims] = buf[b, :dims].astype(F32)
            state[b, dims : dims + heads] = own_sc[b, heads : 2 * heads]
            state[b, dims + heads : dims + 2 * heads] = jnp.ones((heads, tile), F32)
            state[blocks + b, :dims] = jnp.zeros((dims, tile), F32)
            state[blocks + b, dims : dims + heads] = jnp.full((heads, tile), 0.1 * FAR, F32)
            state[blocks + b, dims + heads :] = jnp.zeros((heads + rest, tile), F32)
            if rest:
                state[b, dims + 2 * heads :] = jnp.zeros((rest, tile), F32)
    att = column(src_ref) * LOG2E
    spaces = ((edges0, tops0), (edges1, tops1))

    def fields(entry):
        code, slot = split(entry >> 1, masks_ref.shape[0])
        row, spot = split(code, 4 * blocks)
        return row, spot, slot

    def ready(n, side):
        for k in range(WIDE):
            entry = list_ref[group * total + n * WIDE + k]
            space = [v.at[k] for v in spaces[side]]
            prepare(entry, fields(entry), heads, dims, masks_ref, att, buf, *space)

    def take(n, side):
        for k in range(WIDE):
            entry = list_ref[group * total + n * WIDE + k]
            space = [v.at[k] for v in spaces[side]]
            absorb(fields(entry), heads, dims, tscore, buf, *space, state)

    number = count_ref[group]

    def body(i, carry):
        ready(2 * i + 1, 1)
        take(2 * i, 0)

        @pl.when(2 * i + 1 < number)
        def _():
            ready(2 * i + 2, 0)
            take(2 * i + 1, 1)

        return carry

    def plain(i, carry):
        ready(i, 0)
        take(i, 0)
        return carry

    if short:
        lax.fori_loop(0, number, plain, 0)
    else:

        @pl.when(number > 0)
        def _():
            ready(0, 0)
            lax.fori_loop(0, (number + 1) >> 1, body, 0)

    if len(outs) > 1:
        outs[1][...] = state[blocks:]


def merge_kernel(state_ref, other_ref, x_ref, bias_ref, whole_ref, out_ref, sems):
    blocks, dims, tile = other_ref.shape[0], x_ref.shape[0], other_ref.shape[2]
    heads = dims // HD
    bias = column(bias_ref)
    share, copies = blocks // sems.shape[0], []
    for b in range(blocks):
        m1, m2 = state_ref[b, dims : dims + heads], other_ref[b, dims : dims + heads]
        l1 = state_ref[b, dims + heads : dims + 2 * heads]
        l2 = other_ref[b, dims + heads : dims + 2 * heads]
        best = jnp.maximum(m1, m2)
        c1, c2 = jnp.exp2(m1 - best), jnp.exp2(m2 - best)
        scale = 1.0 / (l1 * c1 + l2 * c2)
        c1, c2 = (c1 * scale)[:, None, :], (c2 * scale)[:, None, :]
        mixed = state_ref[b, :dims].reshape(heads, HD, tile) * c1
        mixed = mixed + other_ref[b, :dims].reshape(heads, HD, tile) * c2
        at = slice(b * tile, (b + 1) * tile)
        v = mixed.reshape(dims, tile) + x_ref[:, at].astype(F32) + bias
        out_ref[:, at] = jnp.where(v > 0, v, jnp.exp(jnp.minimum(v, 0.0)) - 1.0).astype(BF16)
        if (b + 1) % share == 0:
            at = slice((b + 1 - share) * tile, (b + 1) * tile)
            copies.append(pltpu.make_async_copy(out_ref.at[:, at], whole_ref.at[:, at], sems.at[b // share]))
            copies[-1].start()
    for copy in copies:
        copy.wait()


def call(kernel, outs, args, in_specs=None, out_specs=VMEM, scratch=(), aliases=None, flops=1000000):
    return pl.pallas_call(
        kernel,
        out_shape=outs,
        in_specs=in_specs or [VMEM] * len(args),
        out_specs=out_specs,
        scratch_shapes=list(scratch),
        input_output_aliases=aliases or {},
        compiler_params=pltpu.CompilerParams(vmem_limit_bytes=LIMIT),
        cost_estimate=pl.CostEstimate(flops=flops, bytes_accessed=0, transcendentals=0),
    )(*args)


def near(x):
    return pltpu.with_memory_space_constraint(x, pltpu.VMEM)


def held(x):
    return pltpu.with_memory_space_constraint(x, pltpu.SMEM)


def far(x):
    return pltpu.with_memory_space_constraint(x, pltpu.HBM)


def local(node_feats, proj_weight, att_src, att_dst, out_bias, tile_rows, tile_cols, tile_masks):
    nodes = node_feats.shape[1]
    dims = proj_weight.shape[0]
    heads = dims // HD
    words, tile = tile_masks.shape[1:]
    blocks = nodes // tile
    tiles = tile_rows.shape[0]
    n_dp, n_mp = lax.axis_size("dp"), lax.axis_size("mp")
    chips = n_dp // 2
    slots = max(2, 2 * tiles // n_dp)
    half = blocks // 2
    extra = pad8(2 * heads)
    order = ring_order(chips)
    place = [order.index(c) for c in range(chips)]
    me_mp = lax.axis_index("mp")
    steps = chips // 2
    groups = 8
    while groups < steps + 3:
        groups *= 2

    def hop(step):
        pairs = []
        for p, c in enumerate(order):
            to = order[(p + step) % chips]
            pairs += [(2 * c, 2 * to), (2 * c + 1, 2 * to + 1)]
        return sorted(pairs)

    right, left = hop(1), hop(-1)
    swap = [(i, i ^ 1) for i in range(n_dp)]

    mine = jnp.full((1,), me_mp, jnp.int32)
    core = jnp.full((1,), lax.axis_index("dp") & 1, jnp.int32)
    parts = 2 if n_mp == 2 else 1
    moved = [node_feats, proj_weight, att_src.reshape(1, dims), att_dst.reshape(1, dims)]
    moved += [tile_masks, tile_rows, tile_cols]
    shapes = [((node_feats.shape[0], nodes // parts), BF16)] * parts + [(v.shape, v.dtype) for v in moved[1:]]
    spaces = [pltpu.VMEM] * (len(shapes) - 2) + [pltpu.SMEM] * 2
    anywhere = pl.BlockSpec(memory_space=pl.ANY)
    *cuts, weight, a_src, a_dst, near_masks, near_rows, near_cols = call(
        functools.partial(open_kernel, parts),
        [space(*v) for space, v in zip(spaces, shapes)],
        [far(v) for v in moved],
        in_specs=[anywhere] * len(moved),
        out_specs=[pl.BlockSpec(memory_space=v) for v in spaces],
        scratch=[pltpu.SemaphoreType.DMA((len(shapes),))],
    )
    if n_mp == 2:
        flip = [(0, 1), (1, 0)]
        inputs = [[x, lax.ppermute(x, "mp", flip)] for x in cuts]
    else:
        whole = lax.all_gather(node_feats, "mp", axis=0, tiled=True)
        inputs = [[whole[:, k * (nodes // 2) : (k + 1) * (nodes // 2)]] for k in range(2)]
    att = (a_src, a_dst)

    packed = call(
        functools.partial(pack_kernel, blocks, place, groups),
        pltpu.HBM((n_dp, slots + 1, words, tile), jnp.int32),
        [held(near_rows), held(near_cols), near(near_masks)],
        in_specs=[SMEM, SMEM, VMEM],
        scratch=[
            pltpu.SMEM((2 * n_dp,), jnp.int32),
            pltpu.SMEM((chips,), jnp.int32),
            pltpu.SMEM((n_dp * (slots + 2),), jnp.int32),
        ],
    )
    got = lax.all_to_all(packed, "dp", split_axis=0, concat_axis=0, tiled=True)
    got = got.reshape(n_dp * (slots + 1), words, tile)
    got_other = lax.ppermute(got, "dp", swap)

    pays, own_sc = [], None
    for k, xs in enumerate(inputs):
        args = [mine] + [near(v) for v in (weight, *att, *xs)]
        if own_sc is not None:
            args.append(near(own_sc))
        pay, own_sc = call(
            functools.partial(project_kernel, len(xs), k * half),
            (
                pltpu.VMEM((half, dims + extra, tile), BF16),
                pltpu.VMEM((blocks, extra, tile), F32),
            ),
            args,
            in_specs=[SMEM] + [VMEM] * (len(args) - 1),
            out_specs=(VMEM, VMEM),
            aliases={len(args) - 1: 1} if k else None,
        )
        pays.append(pay)
    other_sc = lax.ppermute(own_sc, "dp", swap)

    arrivals = []
    going = {w + p: pays["AB".index(p)] for w in "rl" for p in "AB"}
    for k in range(1, steps):
        for way in ("rA", "lA", "rB", "lB"):
            going[way] = lax.ppermute(going[way], "dp", right if way[0] == "r" else left)
        if k < steps - 1:
            arrivals.append([going[w] for w in ("rA", "rB", "lA", "lB")])
        else:
            arrivals += [[going[w] for w in ways] for ways in (("rA", "lA"), ("rB", "lB"))]
    arrivals[0] = pays + arrivals[0]
    for p in "AB":
        both = []
        for w, pairs, cut in (("r", right, slice(0, half // 2)), ("l", left, slice(half // 2, half))):
            both.append(lax.ppermute(going[w + p][cut], "dp", pairs))
        arrivals.append(both)

    width = n_dp * (slots + 1)
    total = 2 * n_dp * slots + 4 * WIDE
    ids = [v.reshape(n_dp, slots + 1, words, tile)[:, slots, 0, : slots + 2] for v in (got, got_other)]
    lists, counts, masks = call(
        functools.partial(list_kernel, n_dp, slots, groups, blocks, steps + 1),
        (
            pltpu.SMEM((groups * total,), jnp.int32),
            pltpu.SMEM((groups,), jnp.int32),
            pltpu.VMEM((2 * width, words, tile), jnp.int32),
        ),
        (core, *[v.reshape(n_dp * (slots + 2)) for v in ids], near(got), near(got_other)),
        in_specs=[SMEM] * 3 + [VMEM] * 2,
        out_specs=(SMEM, SMEM, VMEM),
    )

    shared = [masks, own_sc, other_sc, att[0]]
    state_shape = pltpu.VMEM((2 * blocks, dims + extra, tile), F32)
    half_shape = pltpu.VMEM((blocks, dims + extra, tile), F32)

    def stage(g, bufs, state, hand=False):
        args = [held(lists), held(counts)] + [near(v) for v in shared + bufs]
        outs, aliases = [state_shape], {}
        if state is not None:
            args.append(near(state))
            aliases[len(args) - 1] = 0
        if hand:
            outs.append(half_shape)
            for k, v in enumerate(shared + bufs):
                aliases[2 + k] = len(outs)
                outs.append(pltpu.VMEM(v.shape, v.dtype))
        return call(
            functools.partial(stage_kernel, g, groups, state is None, g >= steps, len(bufs)),
            outs,
            args,
            in_specs=[SMEM, SMEM] + [VMEM] * (len(args) - 2),
            out_specs=[VMEM] * len(outs),
            scratch=[
                pltpu.VMEM((2 * blocks, extra, tile), F32),
                pltpu.VMEM((sum(v.shape[0] for v in bufs), dims + extra, tile), BF16),
                *[pltpu.VMEM((WIDE, heads, tile, tile), F32)] * 2,
                *[pltpu.VMEM((WIDE, pad8(heads), tile), F32)] * 2,
            ],
            aliases=aliases,
            flops=8000000000,
        )

    state = None
    for g, bufs in enumerate(arrivals[:-1]):
        (state,) = stage(g, bufs, state)
    state, other, *rest = stage(steps + 1, arrivals[-1], state, True)
    back = lax.ppermute(other, "dp", swap)
    shared = rest[: len(shared)]
    (state,) = stage(steps + 2, rest[len(shared) :], state)
    return call(
        merge_kernel,
        jax.ShapeDtypeStruct((dims, nodes), BF16),
        (near(state), near(back), node_feats, out_bias.reshape(1, dims)),
        out_specs=anywhere,
        scratch=[pltpu.VMEM((dims, nodes), BF16), pltpu.SemaphoreType.DMA((math.gcd(blocks, 4),))],
    )


def solution(mesh):
    return jax.shard_map(
        local,
        mesh=mesh,
        in_specs=(
            P("mp", "dp"),
            P("mp", None),
            P("mp"),
            P("mp"),
            P("mp"),
            P("dp"),
            P("dp"),
            P("dp", None, None),
        ),
        out_specs=P("mp", "dp"),
        check_vma=False,
    )
```

```python
import functools
import math

import jax
import jax.numpy as jnp
from jax import lax
from jax.experimental import pallas as pl
from jax.experimental.pallas import tpu as pltpu
from jax.sharding import PartitionSpec as P


HD = 32
LOG2E = 1.4426950408889634
FAR = -1e30
F32 = jnp.float32
BF16 = jnp.bfloat16


WIDE = 2
LIMIT = 16 * 1024 * 1024

VMEM = pl.BlockSpec(memory_space=pltpu.VMEM)
SMEM = pl.BlockSpec(memory_space=pltpu.SMEM)


def split(value, size):
    if size & (size - 1) == 0:
        return value >> (size.bit_length() - 1), value & (size - 1)
    return lax.div(value, jnp.int32(size)), lax.rem(value, jnp.int32(size))


def pad8(count):
    return -(-count // 8) * 8


def leaky(scores):
    return jnp.maximum(scores, 0.2 * scores)


def head_sums(rows):
    return jnp.sum(rows.reshape(rows.shape[0] // HD, HD, rows.shape[1]), axis=1)


def stack_rows(pieces, total):
    have = sum(p.shape[0] for p in pieces)
    if have < total:
        pieces = pieces + [jnp.zeros((total - have, pieces[0].shape[1]), F32)]
    return jnp.concatenate(pieces, axis=0)


def ring_order(chips):
    columns = max(1, chips // 4)
    rows = chips // columns
    if columns == 1:
        return list(range(chips))
    order = [row * columns for row in range(rows)]
    for row in reversed(range(rows)):
        inner = list(range(1, columns))
        order += [row * columns + col for col in (inner if (rows - 1 - row) % 2 == 0 else inner[::-1])]
    return order


def column(row_ref):
    return jnp.transpose(jnp.broadcast_to(row_ref[...], (8, row_ref.shape[1])))[:, 0:1]


def project_kernel(parts, base, mp_ref, w_ref, src_ref, dst_ref, *refs):
    x_refs, (pay_ref, sc_ref) = refs[:parts], refs[-2:]
    me = mp_ref[0]
    depth = w_ref.shape[1] // parts
    total = None
    for k in range(parts):
        at = pl.multiple_of((me ^ k) * depth, depth) if parts > 1 else 0
        term = jnp.dot(w_ref[:, pl.ds(at, depth)], x_refs[k][...], preferred_element_type=F32)
        total = term if total is None else total + term
    rounded = total.astype(BF16)
    a_src, a_dst = column(src_ref) * LOG2E, column(dst_ref) * LOG2E
    source = head_sums(total * a_src)
    target = head_sums(total * a_dst)
    rest = source - head_sums(rounded.astype(F32) * a_src)
    rest_hi = rest.astype(BF16).astype(F32)
    extra = stack_rows([rest_hi, rest - rest_hi], pay_ref.shape[1] - rounded.shape[0]).astype(BF16)
    scores = stack_rows([target, leaky(source + target)], sc_ref.shape[1])
    dims, tile = rounded.shape[0], pay_ref.shape[2]
    for b in range(pay_ref.shape[0]):
        at = slice(b * tile, (b + 1) * tile)
        pay_ref[b, :dims, :] = rounded[:, at]
        pay_ref[b, dims:, :] = extra[:, at]
        sc_ref[base + b] = scores[:, at]


def open_kernel(halves, *refs):
    count = (len(refs) - halves) // 2
    sources, outs, sems = refs[:count], refs[count:-1], refs[-1]
    size = outs[0].shape[1]
    sources = [sources[0].at[:, k * size : (k + 1) * size] for k in range(halves)] + list(sources[1:])
    copies = [pltpu.make_async_copy(v, w, sems.at[k]) for k, (v, w) in enumerate(zip(sources, outs))]
    for copy in copies:
        copy.start()
    for copy in copies:
        copy.wait()


def pack_kernel(blocks, place, groups, mp_ref, rows_ref, cols_ref, masks_ref, out_ref, count, place_ref, codes):
    devices, slots = out_ref.shape[0], out_ref.shape[1] - 1
    words = out_ref.shape[2:]
    whole = masks_ref.shape[1]
    low = mp_ref[0] == 0
    half = blocks // 2
    chips = len(place)
    width = slots + 2
    for c in range(chips):
        place_ref[c] = place[c]
    for d in range(devices):
        count[2 * d] = 0
        count[2 * d + 1] = 0
        for n in range(slots):
            codes[d * width + n] = 0

    def body(t, carry):
        row, col = rows_ref[t], cols_ref[t]
        owner, row_at = split(row, blocks)
        holder, col_at = split(col, blocks)
        odd = holder & 1
        have = count[2 * owner + odd]
        count[2 * owner + odd] = have + 1
        at = jnp.where(odd == 1, slots - 1 - have, have)
        mask = masks_ref[t]
        out_ref[owner, at] = mask if words[0] == whole else jnp.where(low, mask[: words[0]], mask[words[0] :])
        back = place_ref[owner >> 1] - place_ref[holder >> 1]
        back = jnp.where(back < 0, back + chips, back)
        step = jnp.minimum(back, chips - back)
        part, j = split(col_at, half)
        last = 2 * back == chips
        before = step == chips // 2 - 1
        spot = col_at + jnp.where(back > step, blocks, 0) + jnp.where(step == 1, blocks, 0)
        spot = jnp.where(before, j + jnp.where(back > step, half, 0), jnp.where(last, j, spot))
        group = jnp.where(step > 0, step - 1, 0) + jnp.where(before | last, part, 0) + jnp.where(last, 1, 0)
        codes[owner * width + at] = (row_at * (4 * blocks) + spot) * groups + group
        return carry

    lax.fori_loop(0, rows_ref.shape[0], body, 0)
    lane = lax.broadcasted_iota(jnp.int32, words, 1)
    for d in range(devices):
        here = jnp.zeros(words, jnp.int32)
        for n in range(slots):
            here = jnp.where(lane == n, codes[d * width + n], here)
        for n in range(2):
            here = jnp.where(lane == slots + n, count[2 * d + n], here)
        out_ref[d, slots] = here


def mix_kernel(mp_ref, *refs):
    *parts, masks_ref = refs
    width = masks_ref.shape[0] // 2
    low = mp_ref[0] == 0
    for side in range(2):
        at = slice(side * width, (side + 1) * width)
        if len(parts) == 2:
            masks_ref[at] = parts[side][...]
        else:
            here, peer = parts[2 * side][...], parts[2 * side + 1][...]
            masks_ref[at, : here.shape[1]] = jnp.where(low, here, peer)
            masks_ref[at, here.shape[1] :] = jnp.where(low, peer, here)


def list_kernel(devices, slots, groups, blocks, final, core_ref, own_ids, other_ids, list_ref, count_ref):
    total = list_ref.shape[0] // groups
    width = devices * (slots + 1)
    core = core_ref[0]
    for g in range(groups):
        count_ref[g] = 0
    for side, ids in enumerate((own_ids, other_ids)):
        turn = 0 if side else 1

        def holder(d, carry, side=side, ids=ids, turn=turn):
            at_ids, at_slots = d * (slots + 2), d * (slots + 1) + side * width
            number = ids[at_ids + slots + core]
            base = jnp.where(core == 1, slots - number, 0)

            def body(n, carry):
                code, group = split(ids[at_ids + n], groups)
                to = group + jnp.where(group == final, turn, 0)
                at = count_ref[to]
                code = code + side * (4 * blocks * blocks)
                list_ref[to * total + at] = (code * (2 * width) + at_slots + n) * 2 + 1
                count_ref[to] = at + 1
                return carry

            return lax.fori_loop(base, base + number, body, carry)

        lax.fori_loop(0, devices, holder, 0)
    for g in range(groups):
        at = count_ref[g]
        for k in range(3 * WIDE):
            list_ref[g * total + at + k] = 0
        count_ref[g] = lax.div(at + WIDE - 1, WIDE)


def prepare(entry, fields, heads, dims, masks_ref, att, buf, edges, tops):
    _, spot, slot = fields
    tile = masks_ref.shape[2]
    up = 31 - lax.broadcasted_iota(jnp.int32, (32, tile), 0)
    packed = masks_ref[slot] & -(entry & 1)
    block = [
        jnp.where((jnp.broadcast_to(packed[w : w + 1], (32, tile)) << up) < 0, 0.0, FAR)
        for w in range(packed.shape[0])
    ]
    block = jnp.concatenate(block, axis=0)
    feats = buf[spot, :dims, :]
    extra = buf[spot, dims:, :].astype(F32)
    source = head_sums(feats.astype(F32) * att) + extra[:heads] + extra[heads : 2 * heads]
    columns = jnp.transpose(stack_rows([source], pad8(heads)))
    for h in range(heads):
        edge = jnp.broadcast_to(columns[:, h : h + 1], (tile, tile)) + block
        edges[h] = edge
        tops[h : h + 1, :] = jnp.max(edge, axis=0, keepdims=True)


def absorb(fields, heads, dims, tscore, buf, edges, tops, state):
    row, spot, _ = fields
    tile = state.shape[2]
    ones = jnp.ones((16, tile), BF16)
    target = tscore[row, :heads, :]
    old = state[row, dims : dims + heads, :]
    new = jnp.maximum(old, leaky(target + tops[:heads, :]))
    state[row, dims : dims + heads, :] = new
    alpha, up1, up2 = jnp.exp2(old - new), target - new, 0.2 * target - new
    values = []
    for h in range(heads):
        edge = edges[h]
        raw = jnp.maximum(edge + up1[h : h + 1], 0.2 * edge + up2[h : h + 1])
        weight = jnp.exp2(raw).astype(BF16)
        left = jnp.concatenate([buf[spot, h * HD : (h + 1) * HD, :], ones], axis=0)
        values.append(jnp.dot(left, weight, preferred_element_type=F32))
    at = slice(dims + heads, dims + 2 * heads)
    mass = jnp.concatenate([v[HD : HD + 1] for v in values], axis=0)
    state[row, at, :] = state[row, at, :] * alpha + mass
    for h in range(heads):
        at = slice(h * HD, (h + 1) * HD)
        state[row, at, :] = state[row, at, :] * alpha[h : h + 1] + values[h][:HD]


def stage_kernel(group, groups, first, short, count, list_ref, count_ref, masks_ref, own_sc, other_sc, src_ref, *refs):
    pays, (tscore, buf, edges0, edges1, tops0, tops1) = refs[:count], refs[-6:]
    outs = refs[count if first else count + 1 : -6]
    state = outs[0]
    total = list_ref.shape[0] // groups
    blocks, dims = own_sc.shape[0], src_ref.shape[1]
    heads = dims // HD
    base = 0
    for pay in pays:
        buf[base : base + pay.shape[0]] = pay[...]
        base += pay.shape[0]
    tscore[:blocks] = own_sc[...]
    tscore[blocks:] = other_sc[...]
    if first:
        tile = state.shape[2]
        rest = state.shape[1] - dims - 2 * heads
        for b in range(blocks):
            state[b, :dims] = buf[b, :dims].astype(F32)
            state[b, dims : dims + heads] = own_sc[b, heads : 2 * heads]
            state[b, dims + heads : dims + 2 * heads] = jnp.ones((heads, tile), F32)
            state[blocks + b, :dims] = jnp.zeros((dims, tile), F32)
            state[blocks + b, dims : dims + heads] = jnp.full((heads, tile), 0.1 * FAR, F32)
            state[blocks + b, dims + heads :] = jnp.zeros((heads + rest, tile), F32)
            if rest:
                state[b, dims + 2 * heads :] = jnp.zeros((rest, tile), F32)
    att = column(src_ref) * LOG2E
    spaces = ((edges0, tops0), (edges1, tops1))

    def fields(entry):
        code, slot = split(entry >> 1, masks_ref.shape[0])
        row, spot = split(code, 4 * blocks)
        return row, spot, slot

    def ready(n, side):
        for k in range(WIDE):
            entry = list_ref[group * total + n * WIDE + k]
            space = [v.at[k] for v in spaces[side]]
            prepare(entry, fields(entry), heads, dims, masks_ref, att, buf, *space)

    def take(n, side):
        for k in range(WIDE):
            entry = list_ref[group * total + n * WIDE + k]
            space = [v.at[k] for v in spaces[side]]
            absorb(fields(entry), heads, dims, tscore, buf, *space, state)

    number = count_ref[group]

    def body(i, carry):
        ready(2 * i + 1, 1)
        take(2 * i, 0)

        @pl.when(2 * i + 1 < number)
        def _():
            ready(2 * i + 2, 0)
            take(2 * i + 1, 1)

        return carry

    def plain(i, carry):
        ready(i, 0)
        take(i, 0)
        return carry

    if short:
        lax.fori_loop(0, number, plain, 0)
    else:

        @pl.when(number > 0)
        def _():
            ready(0, 0)
            lax.fori_loop(0, (number + 1) >> 1, body, 0)

    if len(outs) > 1:
        outs[1][...] = state[blocks:]


def merge_kernel(state_ref, other_ref, x_ref, bias_ref, whole_ref, out_ref, sems):
    blocks, dims, tile = other_ref.shape[0], x_ref.shape[0], other_ref.shape[2]
    heads = dims // HD
    bias = column(bias_ref)
    share, copies = blocks // sems.shape[0], []
    for b in range(blocks):
        m1, m2 = state_ref[b, dims : dims + heads], other_ref[b, dims : dims + heads]
        l1 = state_ref[b, dims + heads : dims + 2 * heads]
        l2 = other_ref[b, dims + heads : dims + 2 * heads]
        best = jnp.maximum(m1, m2)
        c1, c2 = jnp.exp2(m1 - best), jnp.exp2(m2 - best)
        scale = 1.0 / (l1 * c1 + l2 * c2)
        c1, c2 = (c1 * scale)[:, None, :], (c2 * scale)[:, None, :]
        mixed = state_ref[b, :dims].reshape(heads, HD, tile) * c1
        mixed = mixed + other_ref[b, :dims].reshape(heads, HD, tile) * c2
        at = slice(b * tile, (b + 1) * tile)
        v = mixed.reshape(dims, tile) + x_ref[:, at].astype(F32) + bias
        out_ref[:, at] = jnp.where(v > 0, v, jnp.exp(jnp.minimum(v, 0.0)) - 1.0).astype(BF16)
        if (b + 1) % share == 0:
            at = slice((b + 1 - share) * tile, (b + 1) * tile)
            copies.append(pltpu.make_async_copy(out_ref.at[:, at], whole_ref.at[:, at], sems.at[b // share]))
            copies[-1].start()
    for copy in copies:
        copy.wait()


def call(kernel, outs, args, in_specs=None, out_specs=VMEM, scratch=(), aliases=None, flops=1000000):
    return pl.pallas_call(
        kernel,
        out_shape=outs,
        in_specs=in_specs or [VMEM] * len(args),
        out_specs=out_specs,
        scratch_shapes=list(scratch),
        input_output_aliases=aliases or {},
        compiler_params=pltpu.CompilerParams(vmem_limit_bytes=LIMIT),
        cost_estimate=pl.CostEstimate(flops=flops, bytes_accessed=0, transcendentals=0),
    )(*args)


def near(x):
    return pltpu.with_memory_space_constraint(x, pltpu.VMEM)


def held(x):
    return pltpu.with_memory_space_constraint(x, pltpu.SMEM)


def far(x):
    return pltpu.with_memory_space_constraint(x, pltpu.HBM)


def local(node_feats, proj_weight, att_src, att_dst, out_bias, tile_rows, tile_cols, tile_masks):
    nodes = node_feats.shape[1]
    dims = proj_weight.shape[0]
    heads = dims // HD
    words, tile = tile_masks.shape[1:]
    blocks = nodes // tile
    tiles = tile_rows.shape[0]
    n_dp, n_mp = lax.axis_size("dp"), lax.axis_size("mp")
    chips = n_dp // 2
    slots = max(2, 2 * tiles // n_dp)
    half = blocks // 2
    extra = pad8(2 * heads)
    order = ring_order(chips)
    place = [order.index(c) for c in range(chips)]
    me_mp = lax.axis_index("mp")
    steps = chips // 2
    groups = 8
    while groups < steps + 3:
        groups *= 2

    def hop(step):
        pairs = []
        for p, c in enumerate(order):
            to = order[(p + step) % chips]
            pairs += [(2 * c, 2 * to), (2 * c + 1, 2 * to + 1)]
        return sorted(pairs)

    right, left = hop(1), hop(-1)
    swap = [(i, i ^ 1) for i in range(n_dp)]

    mine = jnp.full((1,), me_mp, jnp.int32)
    core = jnp.full((1,), lax.axis_index("dp") & 1, jnp.int32)
    parts = 2 if n_mp == 2 else 1
    moved = [node_feats, proj_weight, att_src.reshape(1, dims), att_dst.reshape(1, dims)]
    moved += [tile_masks, tile_rows, tile_cols]
    shapes = [((node_feats.shape[0], nodes // parts), BF16)] * parts + [(v.shape, v.dtype) for v in moved[1:]]
    spaces = [pltpu.VMEM] * (len(shapes) - 2) + [pltpu.SMEM] * 2
    anywhere = pl.BlockSpec(memory_space=pl.ANY)
    *cuts, weight, a_src, a_dst, near_masks, near_rows, near_cols = call(
        functools.partial(open_kernel, parts),
        [space(*v) for space, v in zip(spaces, shapes)],
        [far(v) for v in moved],
        in_specs=[anywhere] * len(moved),
        out_specs=[pl.BlockSpec(memory_space=v) for v in spaces],
        scratch=[pltpu.SemaphoreType.DMA((len(shapes),))],
    )
    if n_mp == 2:
        flip = [(0, 1), (1, 0)]
        inputs = [[x, lax.ppermute(x, "mp", flip)] for x in cuts]
    else:
        whole = lax.all_gather(node_feats, "mp", axis=0, tiled=True)
        inputs = [[whole[:, k * (nodes // 2) : (k + 1) * (nodes // 2)]] for k in range(2)]
    att = (a_src, a_dst)

    packed = call(
        functools.partial(pack_kernel, blocks, place, groups),
        pltpu.HBM((n_dp, slots + 1, words // parts, tile), jnp.int32),
        [mine, held(near_rows), held(near_cols), near(near_masks)],
        in_specs=[SMEM, SMEM, SMEM, VMEM],
        scratch=[
            pltpu.SMEM((2 * n_dp,), jnp.int32),
            pltpu.SMEM((chips,), jnp.int32),
            pltpu.SMEM((n_dp * (slots + 2),), jnp.int32),
        ],
    )
    got = lax.all_to_all(packed, "dp", split_axis=0, concat_axis=0, tiled=True)
    got = [got.reshape(n_dp * (slots + 1), words // parts, tile)]
    if parts == 2:
        got.append(lax.ppermute(got[0], "mp", flip))
    got_other = [lax.ppermute(v, "dp", swap) for v in got]

    pays, own_sc = [], None
    for k, xs in enumerate(inputs):
        args = [mine] + [near(v) for v in (weight, *att, *xs)]
        if own_sc is not None:
            args.append(near(own_sc))
        pay, own_sc = call(
            functools.partial(project_kernel, len(xs), k * half),
            (
                pltpu.VMEM((half, dims + extra, tile), BF16),
                pltpu.VMEM((blocks, extra, tile), F32),
            ),
            args,
            in_specs=[SMEM] + [VMEM] * (len(args) - 1),
            out_specs=(VMEM, VMEM),
            aliases={len(args) - 1: 1} if k else None,
        )
        pays.append(pay)
    other_sc = lax.ppermute(own_sc, "dp", swap)

    arrivals = []
    going = {w + p: pays["AB".index(p)] for w in "rl" for p in "AB"}
    for k in range(1, steps):
        for way in ("rA", "lA", "rB", "lB"):
            going[way] = lax.ppermute(going[way], "dp", right if way[0] == "r" else left)
        if k < steps - 1:
            arrivals.append([going[w] for w in ("rA", "rB", "lA", "lB")])
        else:
            arrivals += [[going[w] for w in ways] for ways in (("rA", "lA"), ("rB", "lB"))]
    arrivals[0] = pays + arrivals[0]
    for p in "AB":
        both = []
        for w, pairs, cut in (("r", right, slice(0, half // 2)), ("l", left, slice(half // 2, half))):
            both.append(lax.ppermute(going[w + p][cut], "dp", pairs))
        arrivals.append(both)

    width = n_dp * (slots + 1)
    total = 2 * n_dp * slots + 4 * WIDE
    ids = [v.reshape(n_dp, slots + 1, words // parts, tile)[:, slots, 0, : slots + 2] for v in (got[0], got_other[0])]
    lists, counts = call(
        functools.partial(list_kernel, n_dp, slots, groups, blocks, steps + 1),
        (
            pltpu.SMEM((groups * total,), jnp.int32),
            pltpu.SMEM((groups,), jnp.int32),
        ),
        (core, *[v.reshape(n_dp * (slots + 2)) for v in ids]),
        in_specs=[SMEM] * 3,
        out_specs=(SMEM, SMEM),
    )
    masks = call(
        mix_kernel,
        pltpu.VMEM((2 * width, words, tile), jnp.int32),
        (mine, *[near(v) for v in got + got_other]),
        in_specs=[SMEM] + [VMEM] * (2 * parts),
    )

    shared = [masks, own_sc, other_sc, att[0]]
    state_shape = pltpu.VMEM((2 * blocks, dims + extra, tile), F32)
    half_shape = pltpu.VMEM((blocks, dims + extra, tile), F32)

    def stage(g, bufs, state, hand=False):
        args = [held(lists), held(counts)] + [near(v) for v in shared + bufs]
        outs, aliases = [state_shape], {}
        if state is not None:
            args.append(near(state))
            aliases[len(args) - 1] = 0
        if hand:
            outs.append(half_shape)
            for k, v in enumerate(shared + bufs):
                aliases[2 + k] = len(outs)
                outs.append(pltpu.VMEM(v.shape, v.dtype))
        return call(
            functools.partial(stage_kernel, g, groups, state is None, g >= steps, len(bufs)),
            outs,
            args,
            in_specs=[SMEM, SMEM] + [VMEM] * (len(args) - 2),
            out_specs=[VMEM] * len(outs),
            scratch=[
                pltpu.VMEM((2 * blocks, extra, tile), F32),
                pltpu.VMEM((sum(v.shape[0] for v in bufs), dims + extra, tile), BF16),
                *[pltpu.VMEM((WIDE, heads, tile, tile), F32)] * 2,
                *[pltpu.VMEM((WIDE, pad8(heads), tile), F32)] * 2,
            ],
            aliases=aliases,
            flops=8000000000,
        )

    state = None
    for g, bufs in enumerate(arrivals[:-1]):
        (state,) = stage(g, bufs, state)
    state, other, *rest = stage(steps + 1, arrivals[-1], state, True)
    back = lax.ppermute(other, "dp", swap)
    shared = rest[: len(shared)]
    (state,) = stage(steps + 2, rest[len(shared) :], state)
    return call(
        merge_kernel,
        jax.ShapeDtypeStruct((dims, nodes), BF16),
        (near(state), near(back), node_feats, out_bias.reshape(1, dims)),
        out_specs=anywhere,
        scratch=[pltpu.VMEM((dims, nodes), BF16), pltpu.SemaphoreType.DMA((math.gcd(blocks, 4),))],
    )


def solution(mesh):
    return jax.shard_map(
        local,
        mesh=mesh,
        in_specs=(
            P("mp", "dp"),
            P("mp", None),
            P("mp"),
            P("mp"),
            P("mp"),
            P("dp"),
            P("dp"),
            P("dp", None, None),
        ),
        out_specs=P("mp", "dp"),
        check_vma=False,
    )
```

```python
import functools
import math

import jax
import jax.numpy as jnp
from jax import lax
from jax.experimental import pallas as pl
from jax.experimental.pallas import tpu as pltpu
from jax.sharding import PartitionSpec as P


HD = 32
LOG2E = 1.4426950408889634
FAR = -1e30
F32 = jnp.float32
BF16 = jnp.bfloat16


WIDE = 2
LIMIT = 16 * 1024 * 1024

VMEM = pl.BlockSpec(memory_space=pltpu.VMEM)
SMEM = pl.BlockSpec(memory_space=pltpu.SMEM)


def split(value, size):
    if size & (size - 1) == 0:
        return value >> (size.bit_length() - 1), value & (size - 1)
    return lax.div(value, jnp.int32(size)), lax.rem(value, jnp.int32(size))


def pad8(count):
    return -(-count // 8) * 8


def leaky(scores):
    return jnp.maximum(scores, 0.2 * scores)


def head_sums(rows):
    return jnp.sum(rows.reshape(rows.shape[0] // HD, HD, rows.shape[1]), axis=1)


def stack_rows(pieces, total):
    have = sum(p.shape[0] for p in pieces)
    if have < total:
        pieces = pieces + [jnp.zeros((total - have, pieces[0].shape[1]), F32)]
    return jnp.concatenate(pieces, axis=0)


def ring_order(chips):
    columns = max(1, chips // 4)
    rows = chips // columns
    if columns == 1:
        return list(range(chips))
    order = [row * columns for row in range(rows)]
    for row in reversed(range(rows)):
        inner = list(range(1, columns))
        order += [row * columns + col for col in (inner if (rows - 1 - row) % 2 == 0 else inner[::-1])]
    return order


def column(row_ref):
    return jnp.transpose(jnp.broadcast_to(row_ref[...], (8, row_ref.shape[1])))[:, 0:1]


def project_kernel(parts, base, mp_ref, w_ref, src_ref, dst_ref, *refs):
    x_refs, (pay_ref, sc_ref) = refs[:parts], refs[-2:]
    me = mp_ref[0]
    depth = w_ref.shape[1] // parts
    total = None
    for k in range(parts):
        at = pl.multiple_of((me ^ k) * depth, depth) if parts > 1 else 0
        term = jnp.dot(w_ref[:, pl.ds(at, depth)], x_refs[k][...], preferred_element_type=F32)
        total = term if total is None else total + term
    rounded = total.astype(BF16)
    a_src, a_dst = column(src_ref) * LOG2E, column(dst_ref) * LOG2E
    source = head_sums(total * a_src)
    target = head_sums(total * a_dst)
    rest = source - head_sums(rounded.astype(F32) * a_src)
    scores = stack_rows([target, leaky(source + target)], sc_ref.shape[1])
    dims, tile = rounded.shape[0], pay_ref.shape[2]
    for b in range(2 * pay_ref.shape[0]):
        at = slice(b * tile, (b + 1) * tile)
        side = b % 2 * dims
        pay_ref[b // 2, side : side + dims, :] = rounded[:, at]
        sc_ref[base + b] = scores[:, at]
    for p in range(pay_ref.shape[0]):
        rests = [rest[:, k * tile : (k + 1) * tile] for k in (2 * p, 2 * p + 1)]
        pay_ref[p, 2 * dims :, :] = stack_rows(rests, pay_ref.shape[1] - 2 * dims).astype(BF16)


def open_kernel(halves, *refs):
    count = (len(refs) - halves) // 2
    sources, outs, sems = refs[:count], refs[count:-1], refs[-1]
    size = outs[0].shape[1]
    sources = [sources[0].at[:, k * size : (k + 1) * size] for k in range(halves)] + list(sources[1:])
    copies = [pltpu.make_async_copy(v, w, sems.at[k]) for k, (v, w) in enumerate(zip(sources, outs))]
    for copy in copies:
        copy.start()
    for copy in copies:
        copy.wait()


def pack_kernel(blocks, place, groups, mp_ref, rows_ref, cols_ref, masks_ref, out_ref, count, place_ref, codes):
    devices, slots = out_ref.shape[0], out_ref.shape[1] - 1
    words = out_ref.shape[2:]
    whole = masks_ref.shape[1]
    low = mp_ref[0] == 0
    half = blocks // 2
    chips = len(place)
    width = slots + 2
    for c in range(chips):
        place_ref[c] = place[c]
    for d in range(devices):
        count[2 * d] = 0
        count[2 * d + 1] = 0
        for n in range(slots):
            codes[d * width + n] = 0

    def body(t, carry):
        row, col = rows_ref[t], cols_ref[t]
        owner, row_at = split(row, blocks)
        holder, col_at = split(col, blocks)
        odd = holder & 1
        have = count[2 * owner + odd]
        count[2 * owner + odd] = have + 1
        at = jnp.where(odd == 1, slots - 1 - have, have)
        mask = masks_ref[t]
        out_ref[owner, at] = mask if words[0] == whole else jnp.where(low, mask[: words[0]], mask[words[0] :])
        back = place_ref[owner >> 1] - place_ref[holder >> 1]
        back = jnp.where(back < 0, back + chips, back)
        step = jnp.minimum(back, chips - back)
        part, j = split(col_at, half)
        last = 2 * back == chips
        before = step == chips // 2 - 1
        spot = col_at + jnp.where(back > step, blocks, 0) + jnp.where(step == 1, blocks, 0)
        spot = jnp.where(before, j + jnp.where(back > step, half, 0), jnp.where(last, j, spot))
        group = jnp.where(step > 0, step - 1, 0) + jnp.where(before | last, part, 0) + jnp.where(last, 1, 0)
        codes[owner * width + at] = (row_at * (4 * blocks) + spot) * groups + group
        return carry

    lax.fori_loop(0, rows_ref.shape[0], body, 0)
    lane = lax.broadcasted_iota(jnp.int32, words, 1)
    for d in range(devices):
        here = jnp.zeros(words, jnp.int32)
        for n in range(slots):
            here = jnp.where(lane == n, codes[d * width + n], here)
        for n in range(2):
            here = jnp.where(lane == slots + n, count[2 * d + n], here)
        out_ref[d, slots] = here


def mix_kernel(mp_ref, *refs):
    *parts, masks_ref = refs
    width = masks_ref.shape[0] // 2
    low = mp_ref[0] == 0
    for side in range(2):
        at = slice(side * width, (side + 1) * width)
        if len(parts) == 2:
            masks_ref[at] = parts[side][...]
        else:
            here, peer = parts[2 * side][...], parts[2 * side + 1][...]
            masks_ref[at, : here.shape[1]] = jnp.where(low, here, peer)
            masks_ref[at, here.shape[1] :] = jnp.where(low, peer, here)


def list_kernel(devices, slots, groups, blocks, final, core_ref, own_ids, other_ids, list_ref, count_ref):
    total = list_ref.shape[0] // groups
    width = devices * (slots + 1)
    core = core_ref[0]
    for g in range(groups):
        count_ref[g] = 0
    for side, ids in enumerate((own_ids, other_ids)):
        turn = 0 if side else 1

        def holder(d, carry, side=side, ids=ids, turn=turn):
            at_ids, at_slots = d * (slots + 2), d * (slots + 1) + side * width
            number = ids[at_ids + slots + core]
            base = jnp.where(core == 1, slots - number, 0)

            def body(n, carry):
                code, group = split(ids[at_ids + n], groups)
                to = group + jnp.where(group == final, turn, 0)
                at = count_ref[to]
                code = code + side * (4 * blocks * blocks)
                list_ref[to * total + at] = (code * (2 * width) + at_slots + n) * 2 + 1
                count_ref[to] = at + 1
                return carry

            return lax.fori_loop(base, base + number, body, carry)

        lax.fori_loop(0, devices, holder, 0)
    for g in range(groups):
        at = count_ref[g]
        for k in range(3 * WIDE):
            list_ref[g * total + at + k] = 0
        count_ref[g] = lax.div(at + WIDE - 1, WIDE)


def prepare(entry, fields, heads, dims, masks_ref, att, buf, edges, tops):
    _, spot, slot = fields
    tile = masks_ref.shape[2]
    up = 31 - lax.broadcasted_iota(jnp.int32, (32, tile), 0)
    packed = masks_ref[slot] & -(entry & 1)
    block = [
        jnp.where((jnp.broadcast_to(packed[w : w + 1], (32, tile)) << up) < 0, 0.0, FAR)
        for w in range(packed.shape[0])
    ]
    block = jnp.concatenate(block, axis=0)
    side = spot & 1
    feats = buf[spot >> 1, pl.ds(pl.multiple_of(side * dims, dims), dims), :]
    rests = buf[spot >> 1, 2 * dims :, :].astype(F32)
    rest = jnp.where(side == 1, rests[heads : 2 * heads], rests[:heads])
    source = head_sums(feats.astype(F32) * att) + rest
    columns = jnp.transpose(stack_rows([source], pad8(heads)))
    for h in range(heads):
        edge = jnp.broadcast_to(columns[:, h : h + 1], (tile, tile)) + block
        edges[h] = edge
        tops[h : h + 1, :] = jnp.max(edge, axis=0, keepdims=True)


def absorb(fields, heads, dims, tscore, buf, edges, tops, state):
    row, spot, _ = fields
    tile = state.shape[2]
    ones = jnp.ones((16, tile), BF16)
    target = tscore[row, :heads, :]
    old = state[row, dims : dims + heads, :]
    new = jnp.maximum(old, leaky(target + tops[:heads, :]))
    state[row, dims : dims + heads, :] = new
    alpha, up1, up2 = jnp.exp2(old - new), target - new, 0.2 * target - new
    values = []
    for h in range(heads):
        edge = edges[h]
        raw = jnp.maximum(edge + up1[h : h + 1], 0.2 * edge + up2[h : h + 1])
        weight = jnp.exp2(raw).astype(BF16)
        at = pl.multiple_of((spot & 1) * dims + h * HD, HD)
        left = jnp.concatenate([buf[spot >> 1, pl.ds(at, HD), :], ones], axis=0)
        values.append(jnp.dot(left, weight, preferred_element_type=F32))
    at = slice(dims + heads, dims + 2 * heads)
    mass = jnp.concatenate([v[HD : HD + 1] for v in values], axis=0)
    state[row, at, :] = state[row, at, :] * alpha + mass
    for h in range(heads):
        at = slice(h * HD, (h + 1) * HD)
        state[row, at, :] = state[row, at, :] * alpha[h : h + 1] + values[h][:HD]


def stage_kernel(group, groups, first, short, count, list_ref, count_ref, masks_ref, own_sc, other_sc, src_ref, *refs):
    pays, (tscore, buf, edges0, edges1, tops0, tops1) = refs[:count], refs[-6:]
    outs = refs[count if first else count + 1 : -6]
    state = outs[0]
    total = list_ref.shape[0] // groups
    blocks, dims = own_sc.shape[0], src_ref.shape[1]
    heads = dims // HD
    base = 0
    for pay in pays:
        buf[base : base + pay.shape[0]] = pay[...]
        base += pay.shape[0]
    tscore[:blocks] = own_sc[...]
    tscore[blocks:] = other_sc[...]
    if first:
        tile = state.shape[2]
        rest = state.shape[1] - dims - 2 * heads
        for b in range(blocks):
            state[b, :dims] = buf[b // 2, b % 2 * dims : (b % 2 + 1) * dims].astype(F32)
            state[b, dims : dims + heads] = own_sc[b, heads : 2 * heads]
            state[b, dims + heads : dims + 2 * heads] = jnp.ones((heads, tile), F32)
            state[blocks + b, :dims] = jnp.zeros((dims, tile), F32)
            state[blocks + b, dims : dims + heads] = jnp.full((heads, tile), 0.1 * FAR, F32)
            state[blocks + b, dims + heads :] = jnp.zeros((heads + rest, tile), F32)
            if rest:
                state[b, dims + 2 * heads :] = jnp.zeros((rest, tile), F32)
    att = column(src_ref) * LOG2E
    spaces = ((edges0, tops0), (edges1, tops1))

    def fields(entry):
        code, slot = split(entry >> 1, masks_ref.shape[0])
        row, spot = split(code, 4 * blocks)
        return row, spot, slot

    def ready(n, side):
        for k in range(WIDE):
            entry = list_ref[group * total + n * WIDE + k]
            space = [v.at[k] for v in spaces[side]]
            prepare(entry, fields(entry), heads, dims, masks_ref, att, buf, *space)

    def take(n, side):
        for k in range(WIDE):
            entry = list_ref[group * total + n * WIDE + k]
            space = [v.at[k] for v in spaces[side]]
            absorb(fields(entry), heads, dims, tscore, buf, *space, state)

    number = count_ref[group]

    def body(i, carry):
        ready(2 * i + 1, 1)
        take(2 * i, 0)

        @pl.when(2 * i + 1 < number)
        def _():
            ready(2 * i + 2, 0)
            take(2 * i + 1, 1)

        return carry

    def plain(i, carry):
        ready(i, 0)
        take(i, 0)
        return carry

    if short:
        lax.fori_loop(0, number, plain, 0)
    else:

        @pl.when(number > 0)
        def _():
            ready(0, 0)
            lax.fori_loop(0, (number + 1) >> 1, body, 0)

    if len(outs) > 1:
        outs[1][...] = state[blocks:, :dims].astype(BF16)
        outs[2][...] = state[blocks:, dims:]


def merge_kernel(state_ref, sums_ref, levels_ref, x_ref, bias_ref, whole_ref, out_ref, sems):
    blocks, dims, tile = sums_ref.shape
    heads = dims // HD
    bias = column(bias_ref)
    share, copies = blocks // sems.shape[0], []
    for b in range(blocks):
        m1, m2 = state_ref[b, dims : dims + heads], levels_ref[b, :heads]
        l1 = state_ref[b, dims + heads : dims + 2 * heads]
        l2 = levels_ref[b, heads : 2 * heads]
        best = jnp.maximum(m1, m2)
        c1, c2 = jnp.exp2(m1 - best), jnp.exp2(m2 - best)
        scale = 1.0 / (l1 * c1 + l2 * c2)
        c1, c2 = (c1 * scale)[:, None, :], (c2 * scale)[:, None, :]
        mixed = state_ref[b, :dims].reshape(heads, HD, tile) * c1
        mixed = mixed + sums_ref[b].astype(F32).reshape(heads, HD, tile) * c2
        at = slice(b * tile, (b + 1) * tile)
        v = mixed.reshape(dims, tile) + x_ref[:, at].astype(F32) + bias
        out_ref[:, at] = jnp.where(v > 0, v, jnp.exp(jnp.minimum(v, 0.0)) - 1.0).astype(BF16)
        if (b + 1) % share == 0:
            at = slice((b + 1 - share) * tile, (b + 1) * tile)
            copies.append(pltpu.make_async_copy(out_ref.at[:, at], whole_ref.at[:, at], sems.at[b // share]))
            copies[-1].start()
    for copy in copies:
        copy.wait()


def call(kernel, outs, args, in_specs=None, out_specs=VMEM, scratch=(), aliases=None, flops=1000000):
    return pl.pallas_call(
        kernel,
        out_shape=outs,
        in_specs=in_specs or [VMEM] * len(args),
        out_specs=out_specs,
        scratch_shapes=list(scratch),
        input_output_aliases=aliases or {},
        compiler_params=pltpu.CompilerParams(vmem_limit_bytes=LIMIT),
        cost_estimate=pl.CostEstimate(flops=flops, bytes_accessed=0, transcendentals=0),
    )(*args)


def near(x):
    return pltpu.with_memory_space_constraint(x, pltpu.VMEM)


def held(x):
    return pltpu.with_memory_space_constraint(x, pltpu.SMEM)


def far(x):
    return pltpu.with_memory_space_constraint(x, pltpu.HBM)


def local(node_feats, proj_weight, att_src, att_dst, out_bias, tile_rows, tile_cols, tile_masks):
    nodes = node_feats.shape[1]
    dims = proj_weight.shape[0]
    heads = dims // HD
    words, tile = tile_masks.shape[1:]
    blocks = nodes // tile
    tiles = tile_rows.shape[0]
    n_dp, n_mp = lax.axis_size("dp"), lax.axis_size("mp")
    chips = n_dp // 2
    slots = max(2, 2 * tiles // n_dp)
    half = blocks // 2
    extra = pad8(2 * heads)
    order = ring_order(chips)
    place = [order.index(c) for c in range(chips)]
    me_mp = lax.axis_index("mp")
    steps = chips // 2
    groups = 8
    while groups < steps + 3:
        groups *= 2

    def hop(step):
        pairs = []
        for p, c in enumerate(order):
            to = order[(p + step) % chips]
            pairs += [(2 * c, 2 * to), (2 * c + 1, 2 * to + 1)]
        return sorted(pairs)

    right, left = hop(1), hop(-1)
    swap = [(i, i ^ 1) for i in range(n_dp)]

    mine = jnp.full((1,), me_mp, jnp.int32)
    core = jnp.full((1,), lax.axis_index("dp") & 1, jnp.int32)
    parts = 2 if n_mp == 2 else 1
    moved = [node_feats, proj_weight, att_src.reshape(1, dims), att_dst.reshape(1, dims)]
    moved += [tile_masks, tile_rows, tile_cols]
    shapes = [((node_feats.shape[0], nodes // parts), BF16)] * parts + [(v.shape, v.dtype) for v in moved[1:]]
    spaces = [pltpu.VMEM] * (len(shapes) - 2) + [pltpu.SMEM] * 2
    anywhere = pl.BlockSpec(memory_space=pl.ANY)
    *cuts, weight, a_src, a_dst, near_masks, near_rows, near_cols = call(
        functools.partial(open_kernel, parts),
        [space(*v) for space, v in zip(spaces, shapes)],
        [far(v) for v in moved],
        in_specs=[anywhere] * len(moved),
        out_specs=[pl.BlockSpec(memory_space=v) for v in spaces],
        scratch=[pltpu.SemaphoreType.DMA((len(shapes),))],
    )
    if n_mp == 2:
        flip = [(0, 1), (1, 0)]
        inputs = [[x, lax.ppermute(x, "mp", flip)] for x in cuts]
    else:
        whole = lax.all_gather(node_feats, "mp", axis=0, tiled=True)
        inputs = [[whole[:, k * (nodes // 2) : (k + 1) * (nodes // 2)]] for k in range(2)]
    att = (a_src, a_dst)

    packed = call(
        functools.partial(pack_kernel, blocks, place, groups),
        pltpu.HBM((n_dp, slots + 1, words // parts, tile), jnp.int32),
        [mine, held(near_rows), held(near_cols), near(near_masks)],
        in_specs=[SMEM, SMEM, SMEM, VMEM],
        scratch=[
            pltpu.SMEM((2 * n_dp,), jnp.int32),
            pltpu.SMEM((chips,), jnp.int32),
            pltpu.SMEM((n_dp * (slots + 2),), jnp.int32),
        ],
    )
    got = lax.all_to_all(packed, "dp", split_axis=0, concat_axis=0, tiled=True)
    got = [got.reshape(n_dp * (slots + 1), words // parts, tile)]
    if parts == 2:
        got.append(lax.ppermute(got[0], "mp", flip))
    got_other = [lax.ppermute(v, "dp", swap) for v in got]

    pays, own_sc = [], None
    for k, xs in enumerate(inputs):
        args = [mine] + [near(v) for v in (weight, *att, *xs)]
        if own_sc is not None:
            args.append(near(own_sc))
        pay, own_sc = call(
            functools.partial(project_kernel, len(xs), k * half),
            (
                pltpu.VMEM((half // 2, 2 * dims + extra, tile), BF16),
                pltpu.VMEM((blocks, extra, tile), F32),
            ),
            args,
            in_specs=[SMEM] + [VMEM] * (len(args) - 1),
            out_specs=(VMEM, VMEM),
            aliases={len(args) - 1: 1} if k else None,
        )
        pays.append(pay)
    other_sc = lax.ppermute(own_sc, "dp", swap)

    arrivals = []
    going = {w + p: pays["AB".index(p)] for w in "rl" for p in "AB"}
    for k in range(1, steps):
        for way in ("rA", "lA", "rB", "lB"):
            going[way] = lax.ppermute(going[way], "dp", right if way[0] == "r" else left)
        if k < steps - 1:
            arrivals.append([going[w] for w in ("rA", "rB", "lA", "lB")])
        else:
            arrivals += [[going[w] for w in ways] for ways in (("rA", "lA"), ("rB", "lB"))]
    arrivals[0] = pays + arrivals[0]
    for p in "AB":
        both = []
        for w, pairs, cut in (("r", right, slice(0, half // 4)), ("l", left, slice(half // 4, half // 2))):
            both.append(lax.ppermute(going[w + p][cut], "dp", pairs))
        arrivals.append(both)

    width = n_dp * (slots + 1)
    total = 2 * n_dp * slots + 4 * WIDE
    ids = [v.reshape(n_dp, slots + 1, words // parts, tile)[:, slots, 0, : slots + 2] for v in (got[0], got_other[0])]
    lists, counts = call(
        functools.partial(list_kernel, n_dp, slots, groups, blocks, steps + 1),
        (
            pltpu.SMEM((groups * total,), jnp.int32),
            pltpu.SMEM((groups,), jnp.int32),
        ),
        (core, *[v.reshape(n_dp * (slots + 2)) for v in ids]),
        in_specs=[SMEM] * 3,
        out_specs=(SMEM, SMEM),
    )
    masks = call(
        mix_kernel,
        pltpu.VMEM((2 * width, words, tile), jnp.int32),
        (mine, *[near(v) for v in got + got_other]),
        in_specs=[SMEM] + [VMEM] * (2 * parts),
    )

    shared = [masks, own_sc, other_sc, att[0]]
    state_shape = pltpu.VMEM((2 * blocks, dims + extra, tile), F32)
    half_shapes = [pltpu.VMEM((blocks, dims, tile), BF16), pltpu.VMEM((blocks, extra, tile), F32)]

    def stage(g, bufs, state, hand=False):
        args = [held(lists), held(counts)] + [near(v) for v in shared + bufs]
        outs, aliases = [state_shape], {}
        if state is not None:
            args.append(near(state))
            aliases[len(args) - 1] = 0
        if hand:
            outs += half_shapes
            for k, v in enumerate(shared + bufs):
                aliases[2 + k] = len(outs)
                outs.append(pltpu.VMEM(v.shape, v.dtype))
        return call(
            functools.partial(stage_kernel, g, groups, state is None, g >= steps, len(bufs)),
            outs,
            args,
            in_specs=[SMEM, SMEM] + [VMEM] * (len(args) - 2),
            out_specs=[VMEM] * len(outs),
            scratch=[
                pltpu.VMEM((2 * blocks, extra, tile), F32),
                pltpu.VMEM((sum(v.shape[0] for v in bufs), 2 * dims + extra, tile), BF16),
                *[pltpu.VMEM((WIDE, heads, tile, tile), F32)] * 2,
                *[pltpu.VMEM((WIDE, pad8(heads), tile), F32)] * 2,
            ],
            aliases=aliases,
            flops=8000000000,
        )

    state = None
    for g, bufs in enumerate(arrivals[:-1]):
        (state,) = stage(g, bufs, state)
    state, sums, levels, *rest = stage(steps + 1, arrivals[-1], state, True)
    back = lax.ppermute(sums, "dp", swap), lax.ppermute(levels, "dp", swap)
    shared = rest[: len(shared)]
    (state,) = stage(steps + 2, rest[len(shared) :], state)
    return call(
        merge_kernel,
        jax.ShapeDtypeStruct((dims, nodes), BF16),
        (near(state), *[near(v) for v in back], node_feats, out_bias.reshape(1, dims)),
        out_specs=anywhere,
        scratch=[pltpu.VMEM((dims, nodes), BF16), pltpu.SemaphoreType.DMA((math.gcd(blocks, 4),))],
    )


def solution(mesh):
    return jax.shard_map(
        local,
        mesh=mesh,
        in_specs=(
            P("mp", "dp"),
            P("mp", None),
            P("mp"),
            P("mp"),
            P("mp"),
            P("dp"),
            P("dp"),
            P("dp", None, None),
        ),
        out_specs=P("mp", "dp"),
        check_vma=False,
    )
```

```python
import functools
import math

import jax
import jax.numpy as jnp
from jax import lax
from jax.experimental import pallas as pl
from jax.experimental.pallas import tpu as pltpu
from jax.sharding import PartitionSpec as P


HD = 32
LOG2E = 1.4426950408889634
FAR = -1e30
F32 = jnp.float32
BF16 = jnp.bfloat16


WIDE = 2
LIMIT = 16 * 1024 * 1024

VMEM = pl.BlockSpec(memory_space=pltpu.VMEM)
SMEM = pl.BlockSpec(memory_space=pltpu.SMEM)


def split(value, size):
    if size & (size - 1) == 0:
        return value >> (size.bit_length() - 1), value & (size - 1)
    return lax.div(value, jnp.int32(size)), lax.rem(value, jnp.int32(size))


def pad8(count):
    return -(-count // 8) * 8


def leaky(scores):
    return jnp.maximum(scores, 0.2 * scores)


def head_sums(rows):
    return jnp.sum(rows.reshape(rows.shape[0] // HD, HD, rows.shape[1]), axis=1)


def stack_rows(pieces, total):
    have = sum(p.shape[0] for p in pieces)
    if have < total:
        pieces = pieces + [jnp.zeros((total - have, pieces[0].shape[1]), F32)]
    return jnp.concatenate(pieces, axis=0)


def ring_order(chips):
    columns = max(1, chips // 4)
    rows = chips // columns
    if columns == 1:
        return list(range(chips))
    order = [row * columns for row in range(rows)]
    for row in reversed(range(rows)):
        inner = list(range(1, columns))
        order += [row * columns + col for col in (inner if (rows - 1 - row) % 2 == 0 else inner[::-1])]
    return order


def column(row_ref):
    return jnp.transpose(jnp.broadcast_to(row_ref[...], (8, row_ref.shape[1])))[:, 0:1]


def project_kernel(parts, base, mp_ref, w_ref, src_ref, dst_ref, *refs):
    x_refs, (pay_ref, sc_ref) = refs[:parts], refs[-2:]
    me = mp_ref[0]
    depth = w_ref.shape[1] // parts
    total = None
    for k in range(parts):
        at = pl.multiple_of((me ^ k) * depth, depth) if parts > 1 else 0
        term = jnp.dot(w_ref[:, pl.ds(at, depth)], x_refs[k][...], preferred_element_type=F32)
        total = term if total is None else total + term
    rounded = total.astype(BF16)
    a_src, a_dst = column(src_ref) * LOG2E, column(dst_ref) * LOG2E
    source = head_sums(total * a_src)
    target = head_sums(total * a_dst)
    rest = source - head_sums(rounded.astype(F32) * a_src)
    scores = stack_rows([target, leaky(source + target)], sc_ref.shape[1])
    dims, tile = rounded.shape[0], pay_ref.shape[2]
    for b in range(2 * pay_ref.shape[0]):
        at = slice(b * tile, (b + 1) * tile)
        side = b % 2 * dims
        pay_ref[b // 2, side : side + dims, :] = rounded[:, at]
        sc_ref[base + b] = scores[:, at]
    for p in range(pay_ref.shape[0]):
        rests = [rest[:, k * tile : (k + 1) * tile] for k in (2 * p, 2 * p + 1)]
        pay_ref[p, 2 * dims :, :] = stack_rows(rests, pay_ref.shape[1] - 2 * dims).astype(BF16)


def open_kernel(halves, *refs):
    count = (len(refs) - halves) // 2
    sources, outs, sems = refs[:count], refs[count:-1], refs[-1]
    size = outs[0].shape[1]
    sources = [sources[0].at[:, k * size : (k + 1) * size] for k in range(halves)] + list(sources[1:])
    copies = [pltpu.make_async_copy(v, w, sems.at[k]) for k, (v, w) in enumerate(zip(sources, outs))]
    for copy in copies:
        copy.start()
    for copy in copies:
        copy.wait()


def pack_kernel(blocks, place, groups, mp_ref, rows_ref, cols_ref, masks_ref, out_ref, count, place_ref, codes):
    devices, slots = out_ref.shape[0], out_ref.shape[1] - 1
    words = out_ref.shape[2:]
    whole = masks_ref.shape[1]
    low = mp_ref[0] == 0
    half = blocks // 2
    chips = len(place)
    width = slots + 2
    for c in range(chips):
        place_ref[c] = place[c]
    for d in range(devices):
        count[2 * d] = 0
        count[2 * d + 1] = 0

    def body(t, carry):
        row, col = rows_ref[t], cols_ref[t]
        owner, row_at = split(row, blocks)
        holder, col_at = split(col, blocks)
        odd = holder & 1
        have = count[2 * owner + odd]
        count[2 * owner + odd] = have + 1
        at = jnp.where(odd == 1, slots - 1 - have, have)
        mask = masks_ref[t]
        out_ref[owner, at] = mask if words[0] == whole else jnp.where(low, mask[: words[0]], mask[words[0] :])
        back = place_ref[owner >> 1] - place_ref[holder >> 1]
        back = jnp.where(back < 0, back + chips, back)
        step = jnp.minimum(back, chips - back)
        part, j = split(col_at, half)
        last = 2 * back == chips
        before = step == chips // 2 - 1
        spot = col_at + jnp.where(back > step, blocks, 0) + jnp.where(step == 1, blocks, 0)
        spot = jnp.where(before, j + jnp.where(back > step, half, 0), jnp.where(last, j, spot))
        group = jnp.where(step > 0, step - 1, 0) + jnp.where(before | last, part, 0) + jnp.where(last, 1, 0)
        codes[owner * width + at] = (row_at * (4 * blocks) + spot) * groups + group
        return carry

    lax.fori_loop(0, rows_ref.shape[0], body, 0, unroll=4)
    lane = lax.broadcasted_iota(jnp.int32, words, 1)
    for d in range(devices):
        here = jnp.zeros(words, jnp.int32)
        for n in range(slots):
            here = jnp.where(lane == n, codes[d * width + n], here)
        for n in range(2):
            here = jnp.where(lane == slots + n, count[2 * d + n], here)
        out_ref[d, slots] = here


def mix_kernel(mp_ref, *refs):
    *parts, masks_ref = refs
    width = masks_ref.shape[0] // 2
    low = mp_ref[0] == 0
    for side in range(2):
        at = slice(side * width, (side + 1) * width)
        if len(parts) == 2:
            masks_ref[at] = parts[side][...]
        else:
            here, peer = parts[2 * side][...], parts[2 * side + 1][...]
            masks_ref[at, : here.shape[1]] = jnp.where(low, here, peer)
            masks_ref[at, here.shape[1] :] = jnp.where(low, peer, here)


def list_kernel(devices, slots, groups, blocks, final, core_ref, own_ids, other_ids, list_ref, count_ref):
    total = list_ref.shape[0] // groups
    width = devices * (slots + 1)
    core = core_ref[0]
    for g in range(groups):
        count_ref[g] = 0
    for side, ids in enumerate((own_ids, other_ids)):
        turn = 0 if side else 1

        def holder(d, carry, side=side, ids=ids, turn=turn):
            at_ids, at_slots = d * (slots + 2), d * (slots + 1) + side * width
            number = ids[at_ids + slots + core]
            base = jnp.where(core == 1, slots - number, 0)

            def body(n, carry):
                code, group = split(ids[at_ids + n], groups)
                to = group + jnp.where(group == final, turn, 0)
                at = count_ref[to]
                code = code + side * (4 * blocks * blocks)
                list_ref[to * total + at] = (code * (2 * width) + at_slots + n) * 2 + 1
                count_ref[to] = at + 1
                return carry

            return lax.fori_loop(base, base + number, body, carry)

        lax.fori_loop(0, devices, holder, 0)
    for g in range(groups):
        at = count_ref[g]
        for k in range(3 * WIDE):
            list_ref[g * total + at + k] = 0
        count_ref[g] = lax.div(at + WIDE - 1, WIDE)


def prepare(entry, fields, heads, dims, masks_ref, att, buf, edges, tops):
    _, spot, slot = fields
    tile = masks_ref.shape[2]
    up = 31 - lax.broadcasted_iota(jnp.int32, (32, tile), 0)
    packed = masks_ref[slot] & -(entry & 1)
    block = [
        jnp.where((jnp.broadcast_to(packed[w : w + 1], (32, tile)) << up) < 0, 0.0, FAR)
        for w in range(packed.shape[0])
    ]
    block = jnp.concatenate(block, axis=0)
    side = spot & 1
    feats = buf[spot >> 1, pl.ds(pl.multiple_of(side * dims, dims), dims), :]
    rests = buf[spot >> 1, 2 * dims :, :].astype(F32)
    rest = jnp.where(side == 1, rests[heads : 2 * heads], rests[:heads])
    source = head_sums(feats.astype(F32) * att) + rest
    columns = jnp.transpose(stack_rows([source], pad8(heads)))
    for h in range(heads):
        edge = jnp.broadcast_to(columns[:, h : h + 1], (tile, tile)) + block
        edges[h] = edge
        tops[h : h + 1, :] = jnp.max(edge, axis=0, keepdims=True)


def absorb(fields, heads, dims, tscore, buf, edges, tops, state):
    row, spot, _ = fields
    tile = state.shape[2]
    ones = jnp.ones((16, tile), BF16)
    target = tscore[row, :heads, :]
    old = state[row, dims : dims + heads, :]
    new = jnp.maximum(old, leaky(target + tops[:heads, :]))
    state[row, dims : dims + heads, :] = new
    alpha, up1, up2 = jnp.exp2(old - new), target - new, 0.2 * target - new
    values = []
    for h in range(heads):
        edge = edges[h]
        raw = jnp.maximum(edge + up1[h : h + 1], 0.2 * edge + up2[h : h + 1])
        weight = jnp.exp2(raw).astype(BF16)
        at = pl.multiple_of((spot & 1) * dims + h * HD, HD)
        left = jnp.concatenate([buf[spot >> 1, pl.ds(at, HD), :], ones], axis=0)
        values.append(jnp.dot(left, weight, preferred_element_type=F32))
    at = slice(dims + heads, dims + 2 * heads)
    mass = jnp.concatenate([v[HD : HD + 1] for v in values], axis=0)
    state[row, at, :] = state[row, at, :] * alpha + mass
    for h in range(heads):
        at = slice(h * HD, (h + 1) * HD)
        state[row, at, :] = state[row, at, :] * alpha[h : h + 1] + values[h][:HD]


def stage_kernel(group, groups, first, short, count, list_ref, count_ref, masks_ref, own_sc, other_sc, src_ref, *refs):
    pays, (tscore, buf, edges0, edges1, tops0, tops1) = refs[:count], refs[-6:]
    outs = refs[count if first else count + 1 : -6]
    state = outs[0]
    total = list_ref.shape[0] // groups
    blocks, dims = own_sc.shape[0], src_ref.shape[1]
    heads = dims // HD
    base = 0
    for pay in pays:
        buf[base : base + pay.shape[0]] = pay[...]
        base += pay.shape[0]
    tscore[:blocks] = own_sc[...]
    tscore[blocks:] = other_sc[...]
    if first:
        tile = state.shape[2]
        rest = state.shape[1] - dims - 2 * heads
        for b in range(blocks):
            state[b, :dims] = buf[b // 2, b % 2 * dims : (b % 2 + 1) * dims].astype(F32)
            state[b, dims : dims + heads] = own_sc[b, heads : 2 * heads]
            state[b, dims + heads : dims + 2 * heads] = jnp.ones((heads, tile), F32)
            state[blocks + b, :dims] = jnp.zeros((dims, tile), F32)
            state[blocks + b, dims : dims + heads] = jnp.full((heads, tile), 0.1 * FAR, F32)
            state[blocks + b, dims + heads :] = jnp.zeros((heads + rest, tile), F32)
            if rest:
                state[b, dims + 2 * heads :] = jnp.zeros((rest, tile), F32)
    att = column(src_ref) * LOG2E
    spaces = ((edges0, tops0), (edges1, tops1))

    def fields(entry):
        code, slot = split(entry >> 1, masks_ref.shape[0])
        row, spot = split(code, 4 * blocks)
        return row, spot, slot

    def ready(n, side):
        for k in range(WIDE):
            entry = list_ref[group * total + n * WIDE + k]
            space = [v.at[k] for v in spaces[side]]
            prepare(entry, fields(entry), heads, dims, masks_ref, att, buf, *space)

    def take(n, side):
        for k in range(WIDE):
            entry = list_ref[group * total + n * WIDE + k]
            space = [v.at[k] for v in spaces[side]]
            absorb(fields(entry), heads, dims, tscore, buf, *space, state)

    number = count_ref[group]

    def body(i, carry):
        ready(2 * i + 1, 1)
        take(2 * i, 0)

        @pl.when(2 * i + 1 < number)
        def _():
            ready(2 * i + 2, 0)
            take(2 * i + 1, 1)

        return carry

    def plain(i, carry):
        ready(i, 0)
        take(i, 0)
        return carry

    if short:
        lax.fori_loop(0, number, plain, 0)
    else:

        @pl.when(number > 0)
        def _():
            ready(0, 0)
            lax.fori_loop(0, (number + 1) >> 1, body, 0)

    if len(outs) > 1:
        outs[1][...] = state[blocks:, :dims].astype(BF16)
        outs[2][...] = state[blocks:, dims:]


def merge_kernel(state_ref, sums_ref, levels_ref, x_ref, bias_ref, whole_ref, out_ref, sems):
    blocks, dims, tile = sums_ref.shape
    heads = dims // HD
    bias = column(bias_ref)
    share, copies = blocks // sems.shape[0], []
    for b in range(blocks):
        m1, m2 = state_ref[b, dims : dims + heads], levels_ref[b, :heads]
        l1 = state_ref[b, dims + heads : dims + 2 * heads]
        l2 = levels_ref[b, heads : 2 * heads]
        best = jnp.maximum(m1, m2)
        c1, c2 = jnp.exp2(m1 - best), jnp.exp2(m2 - best)
        scale = 1.0 / (l1 * c1 + l2 * c2)
        c1, c2 = (c1 * scale)[:, None, :], (c2 * scale)[:, None, :]
        mixed = state_ref[b, :dims].reshape(heads, HD, tile) * c1
        mixed = mixed + sums_ref[b].astype(F32).reshape(heads, HD, tile) * c2
        at = slice(b * tile, (b + 1) * tile)
        v = mixed.reshape(dims, tile) + x_ref[:, at].astype(F32) + bias
        out_ref[:, at] = jnp.where(v > 0, v, jnp.exp(v) - 1.0).astype(BF16)
        if (b + 1) % share == 0:
            at = slice((b + 1 - share) * tile, (b + 1) * tile)
            copies.append(pltpu.make_async_copy(out_ref.at[:, at], whole_ref.at[:, at], sems.at[b // share]))
            copies[-1].start()
    for copy in copies:
        copy.wait()


def call(kernel, outs, args, in_specs=None, out_specs=VMEM, scratch=(), aliases=None, flops=1000000):
    return pl.pallas_call(
        kernel,
        out_shape=outs,
        in_specs=in_specs or [VMEM] * len(args),
        out_specs=out_specs,
        scratch_shapes=list(scratch),
        input_output_aliases=aliases or {},
        compiler_params=pltpu.CompilerParams(vmem_limit_bytes=LIMIT),
        cost_estimate=pl.CostEstimate(flops=flops, bytes_accessed=0, transcendentals=0),
    )(*args)


def near(x):
    return pltpu.with_memory_space_constraint(x, pltpu.VMEM)


def held(x):
    return pltpu.with_memory_space_constraint(x, pltpu.SMEM)


def far(x):
    return pltpu.with_memory_space_constraint(x, pltpu.HBM)


def local(node_feats, proj_weight, att_src, att_dst, out_bias, tile_rows, tile_cols, tile_masks):
    nodes = node_feats.shape[1]
    dims = proj_weight.shape[0]
    heads = dims // HD
    words, tile = tile_masks.shape[1:]
    blocks = nodes // tile
    tiles = tile_rows.shape[0]
    n_dp, n_mp = lax.axis_size("dp"), lax.axis_size("mp")
    chips = n_dp // 2
    slots = max(2, 2 * tiles // n_dp)
    half = blocks // 2
    extra = pad8(2 * heads)
    order = ring_order(chips)
    place = [order.index(c) for c in range(chips)]
    me_mp = lax.axis_index("mp")
    steps = chips // 2
    groups = 8
    while groups < steps + 3:
        groups *= 2

    def hop(step):
        pairs = []
        for p, c in enumerate(order):
            to = order[(p + step) % chips]
            pairs += [(2 * c, 2 * to), (2 * c + 1, 2 * to + 1)]
        return sorted(pairs)

    right, left = hop(1), hop(-1)
    swap = [(i, i ^ 1) for i in range(n_dp)]

    mine = jnp.full((1,), me_mp, jnp.int32)
    core = jnp.full((1,), lax.axis_index("dp") & 1, jnp.int32)
    parts = 2 if n_mp == 2 else 1
    moved = [node_feats, proj_weight, att_src.reshape(1, dims), att_dst.reshape(1, dims)]
    moved += [tile_masks, tile_rows, tile_cols]
    shapes = [((node_feats.shape[0], nodes // parts), BF16)] * parts + [(v.shape, v.dtype) for v in moved[1:]]
    spaces = [pltpu.VMEM] * (len(shapes) - 2) + [pltpu.SMEM] * 2
    anywhere = pl.BlockSpec(memory_space=pl.ANY)
    *cuts, weight, a_src, a_dst, near_masks, near_rows, near_cols = call(
        functools.partial(open_kernel, parts),
        [space(*v) for space, v in zip(spaces, shapes)],
        [far(v) for v in moved],
        in_specs=[anywhere] * len(moved),
        out_specs=[pl.BlockSpec(memory_space=v) for v in spaces],
        scratch=[pltpu.SemaphoreType.DMA((len(shapes),))],
    )
    if n_mp == 2:
        flip = [(0, 1), (1, 0)]
        inputs = [[x, lax.ppermute(x, "mp", flip)] for x in cuts]
    else:
        whole = lax.all_gather(node_feats, "mp", axis=0, tiled=True)
        inputs = [[whole[:, k * (nodes // 2) : (k + 1) * (nodes // 2)]] for k in range(2)]
    att = (a_src, a_dst)

    packed = call(
        functools.partial(pack_kernel, blocks, place, groups),
        pltpu.HBM((n_dp, slots + 1, words // parts, tile), jnp.int32),
        [mine, held(near_rows), held(near_cols), near(near_masks)],
        in_specs=[SMEM, SMEM, SMEM, VMEM],
        scratch=[
            pltpu.SMEM((2 * n_dp,), jnp.int32),
            pltpu.SMEM((chips,), jnp.int32),
            pltpu.SMEM((n_dp * (slots + 2),), jnp.int32),
        ],
    )
    got = lax.all_to_all(packed, "dp", split_axis=0, concat_axis=0, tiled=True)
    got = [got.reshape(n_dp * (slots + 1), words // parts, tile)]
    if parts == 2:
        got.append(lax.ppermute(got[0], "mp", flip))
    got_other = [lax.ppermute(v, "dp", swap) for v in got]

    pays, own_sc = [], None
    for k, xs in enumerate(inputs):
        args = [mine] + [near(v) for v in (weight, *att, *xs)]
        if own_sc is not None:
            args.append(near(own_sc))
        pay, own_sc = call(
            functools.partial(project_kernel, len(xs), k * half),
            (
                pltpu.VMEM((half // 2, 2 * dims + extra, tile), BF16),
                pltpu.VMEM((blocks, extra, tile), F32),
            ),
            args,
            in_specs=[SMEM] + [VMEM] * (len(args) - 1),
            out_specs=(VMEM, VMEM),
            aliases={len(args) - 1: 1} if k else None,
        )
        pays.append(pay)
    other_sc = lax.ppermute(own_sc, "dp", swap)

    arrivals = []
    going = {w + p: pays["AB".index(p)] for w in "rl" for p in "AB"}
    for k in range(1, steps):
        for way in ("rA", "lA", "rB", "lB"):
            going[way] = lax.ppermute(going[way], "dp", right if way[0] == "r" else left)
        if k < steps - 1:
            arrivals.append([going[w] for w in ("rA", "rB", "lA", "lB")])
        else:
            arrivals += [[going[w] for w in ways] for ways in (("rA", "lA"), ("rB", "lB"))]
    arrivals[0] = pays + arrivals[0]
    for p in "AB":
        both = []
        for w, pairs, cut in (("r", right, slice(0, half // 4)), ("l", left, slice(half // 4, half // 2))):
            both.append(lax.ppermute(going[w + p][cut], "dp", pairs))
        arrivals.append(both)

    width = n_dp * (slots + 1)
    total = 2 * n_dp * slots + 4 * WIDE
    ids = [v.reshape(n_dp, slots + 1, words // parts, tile)[:, slots, 0, : slots + 2] for v in (got[0], got_other[0])]
    lists, counts = call(
        functools.partial(list_kernel, n_dp, slots, groups, blocks, steps + 1),
        (
            pltpu.SMEM((groups * total,), jnp.int32),
            pltpu.SMEM((groups,), jnp.int32),
        ),
        (core, *[v.reshape(n_dp * (slots + 2)) for v in ids]),
        in_specs=[SMEM] * 3,
        out_specs=(SMEM, SMEM),
    )
    masks = call(
        mix_kernel,
        pltpu.VMEM((2 * width, words, tile), jnp.int32),
        (mine, *[near(v) for v in got + got_other]),
        in_specs=[SMEM] + [VMEM] * (2 * parts),
    )

    shared = [masks, own_sc, other_sc, att[0]]
    state_shape = pltpu.VMEM((2 * blocks, dims + extra, tile), F32)
    half_shapes = [pltpu.VMEM((blocks, dims, tile), BF16), pltpu.VMEM((blocks, extra, tile), F32)]

    def stage(g, bufs, state, hand=False):
        args = [held(lists), held(counts)] + [near(v) for v in shared + bufs]
        outs, aliases = [state_shape], {}
        if state is not None:
            args.append(near(state))
            aliases[len(args) - 1] = 0
        if hand:
            outs += half_shapes
            for k, v in enumerate(shared + bufs):
                aliases[2 + k] = len(outs)
                outs.append(pltpu.VMEM(v.shape, v.dtype))
        return call(
            functools.partial(stage_kernel, g, groups, state is None, g >= steps, len(bufs)),
            outs,
            args,
            in_specs=[SMEM, SMEM] + [VMEM] * (len(args) - 2),
            out_specs=[VMEM] * len(outs),
            scratch=[
                pltpu.VMEM((2 * blocks, extra, tile), F32),
                pltpu.VMEM((sum(v.shape[0] for v in bufs), 2 * dims + extra, tile), BF16),
                *[pltpu.VMEM((WIDE, heads, tile, tile), F32)] * 2,
                *[pltpu.VMEM((WIDE, pad8(heads), tile), F32)] * 2,
            ],
            aliases=aliases,
            flops=8000000000,
        )

    state = None
    for g, bufs in enumerate(arrivals[:-1]):
        (state,) = stage(g, bufs, state)
    state, sums, levels, *rest = stage(steps + 1, arrivals[-1], state, True)
    back = lax.ppermute(sums, "dp", swap), lax.ppermute(levels, "dp", swap)
    shared = rest[: len(shared)]
    (state,) = stage(steps + 2, rest[len(shared) :], state)
    return call(
        merge_kernel,
        jax.ShapeDtypeStruct((dims, nodes), BF16),
        (near(state), *[near(v) for v in back], node_feats, out_bias.reshape(1, dims)),
        out_specs=anywhere,
        scratch=[pltpu.VMEM((dims, nodes), BF16), pltpu.SemaphoreType.DMA((math.gcd(blocks, 8),))],
    )


def solution(mesh):
    return jax.shard_map(
        local,
        mesh=mesh,
        in_specs=(
            P("mp", "dp"),
            P("mp", None),
            P("mp"),
            P("mp"),
            P("mp"),
            P("dp"),
            P("dp"),
            P("dp", None, None),
        ),
        out_specs=P("mp", "dp"),
        check_vma=False,
    )
```

```python
import functools
import math

import jax
import jax.numpy as jnp
from jax import lax
from jax.experimental import pallas as pl
from jax.experimental.pallas import tpu as pltpu
from jax.sharding import PartitionSpec as P


HD = 32
LOG2E = 1.4426950408889634
FAR = -1e30
F32 = jnp.float32
BF16 = jnp.bfloat16


WIDE = 2
LIMIT = 16 * 1024 * 1024

VMEM = pl.BlockSpec(memory_space=pltpu.VMEM)
SMEM = pl.BlockSpec(memory_space=pltpu.SMEM)


def split(value, size):
    if size & (size - 1) == 0:
        return value >> (size.bit_length() - 1), value & (size - 1)
    return lax.div(value, jnp.int32(size)), lax.rem(value, jnp.int32(size))


def pad8(count):
    return -(-count // 8) * 8


def leaky(scores):
    return jnp.maximum(scores, 0.2 * scores)


def head_sums(rows):
    return jnp.sum(rows.reshape(rows.shape[0] // HD, HD, rows.shape[1]), axis=1)


def stack_rows(pieces, total):
    have = sum(p.shape[0] for p in pieces)
    if have < total:
        pieces = pieces + [jnp.zeros((total - have, pieces[0].shape[1]), F32)]
    return jnp.concatenate(pieces, axis=0)


def ring_order(chips):
    columns = max(1, chips // 4)
    rows = chips // columns
    if columns == 1:
        return list(range(chips))
    order = [row * columns for row in range(rows)]
    for row in reversed(range(rows)):
        inner = list(range(1, columns))
        order += [row * columns + col for col in (inner if (rows - 1 - row) % 2 == 0 else inner[::-1])]
    return order


def column(row_ref):
    return jnp.transpose(jnp.broadcast_to(row_ref[...], (8, row_ref.shape[1])))[:, 0:1]


def project_kernel(parts, base, mp_ref, w_ref, src_ref, dst_ref, *refs):
    x_refs, (pay_ref, sc_ref) = refs[:parts], refs[-2:]
    me = mp_ref[0]
    depth = w_ref.shape[1] // parts
    total = None
    for k in range(parts):
        at = pl.multiple_of((me ^ k) * depth, depth) if parts > 1 else 0
        term = jnp.dot(w_ref[:, pl.ds(at, depth)], x_refs[k][...], preferred_element_type=F32)
        total = term if total is None else total + term
    rounded = total.astype(BF16)
    a_src, a_dst = column(src_ref) * LOG2E, column(dst_ref) * LOG2E
    source = head_sums(total * a_src)
    target = head_sums(total * a_dst)
    rest = source - head_sums(rounded.astype(F32) * a_src)
    scores = stack_rows([target, leaky(source + target)], sc_ref.shape[1])
    dims, tile = rounded.shape[0], pay_ref.shape[2]
    for b in range(2 * pay_ref.shape[0]):
        at = slice(b * tile, (b + 1) * tile)
        side = b % 2 * dims
        pay_ref[b // 2, side : side + dims, :] = rounded[:, at]
        sc_ref[base + b] = scores[:, at]
    for p in range(pay_ref.shape[0]):
        rests = [rest[:, k * tile : (k + 1) * tile] for k in (2 * p, 2 * p + 1)]
        pay_ref[p, 2 * dims :, :] = stack_rows(rests, pay_ref.shape[1] - 2 * dims).astype(BF16)


def open_kernel(halves, *refs):
    count = (len(refs) - halves) // 2
    sources, outs, sems = refs[:count], refs[count:-1], refs[-1]
    size = outs[0].shape[1]
    sources = [sources[0].at[:, k * size : (k + 1) * size] for k in range(halves)] + list(sources[1:])
    copies = [pltpu.make_async_copy(v, w, sems.at[k]) for k, (v, w) in enumerate(zip(sources, outs))]
    for copy in copies:
        copy.start()
    for copy in copies:
        copy.wait()


def pack_kernel(blocks, place, groups, mp_ref, rows_ref, cols_ref, masks_ref, out_ref, count, place_ref, codes):
    devices, slots = out_ref.shape[0], out_ref.shape[1] - 1
    words = out_ref.shape[2:]
    whole = masks_ref.shape[1]
    low = mp_ref[0] == 0
    half = blocks // 2
    chips = len(place)
    width = slots + 2
    for c in range(chips):
        place_ref[c] = place[c]
    for d in range(devices):
        count[2 * d] = 0
        count[2 * d + 1] = 0

    def body(t, carry):
        row, col = rows_ref[t], cols_ref[t]
        owner, row_at = split(row, blocks)
        holder, col_at = split(col, blocks)
        odd = holder & 1
        have = count[2 * owner + odd]
        count[2 * owner + odd] = have + 1
        at = jnp.where(odd == 1, slots - 1 - have, have)
        mask = masks_ref[t]
        out_ref[owner, at] = mask if words[0] == whole else jnp.where(low, mask[: words[0]], mask[words[0] :])
        back = place_ref[owner >> 1] - place_ref[holder >> 1]
        back = jnp.where(back < 0, back + chips, back)
        step = jnp.minimum(back, chips - back)
        part, j = split(col_at, half)
        last = 2 * back == chips
        before = step == chips // 2 - 1
        spot = col_at + jnp.where(back > step, blocks, 0) + jnp.where(step == 1, blocks, 0)
        spot = jnp.where(before, j + jnp.where(back > step, half, 0), jnp.where(last, j, spot))
        group = jnp.where(step > 0, step - 1, 0) + jnp.where(before | last, part, 0) + jnp.where(last, 1, 0)
        codes[owner * width + at] = (row_at * (4 * blocks) + spot) * groups + group
        return carry

    lax.fori_loop(0, rows_ref.shape[0], body, 0, unroll=4)
    lane = lax.broadcasted_iota(jnp.int32, words, 1)
    for d in range(devices):
        here = jnp.zeros(words, jnp.int32)
        for n in range(slots):
            here = jnp.where(lane == n, codes[d * width + n], here)
        for n in range(2):
            here = jnp.where(lane == slots + n, count[2 * d + n], here)
        out_ref[d, slots] = here


def mix_kernel(mp_ref, *refs):
    *parts, masks_ref = refs
    width = masks_ref.shape[0] // 2
    low = mp_ref[0] == 0
    for side in range(2):
        at = slice(side * width, (side + 1) * width)
        if len(parts) == 2:
            masks_ref[at] = parts[side][...]
        else:
            here, peer = parts[2 * side][...], parts[2 * side + 1][...]
            masks_ref[at, : here.shape[1]] = jnp.where(low, here, peer)
            masks_ref[at, here.shape[1] :] = jnp.where(low, peer, here)


def list_kernel(devices, slots, groups, blocks, final, core_ref, own_ids, other_ids, list_ref, count_ref):
    total = list_ref.shape[0] // groups
    width = devices * (slots + 1)
    core = core_ref[0]
    for g in range(groups):
        count_ref[g] = 0
    for side, ids in enumerate((own_ids, other_ids)):
        turn = 0 if side else 1

        def holder(d, carry, side=side, ids=ids, turn=turn):
            at_ids, at_slots = d * (slots + 2), d * (slots + 1) + side * width
            number = ids[at_ids + slots + core]
            base = jnp.where(core == 1, slots - number, 0)

            def body(n, carry):
                code, group = split(ids[at_ids + n], groups)
                to = group + jnp.where(group == final, turn, 0)
                at = count_ref[to]
                code = code + side * (4 * blocks * blocks)
                list_ref[to * total + at] = (code * (2 * width) + at_slots + n) * 2 + 1
                count_ref[to] = at + 1
                return carry

            return lax.fori_loop(base, base + number, body, carry)

        lax.fori_loop(0, devices, holder, 0)
    for g in range(groups):
        at = count_ref[g]
        for k in range(3 * WIDE):
            list_ref[g * total + at + k] = 0
        count_ref[g] = lax.div(at + WIDE - 1, WIDE)


def prepare(entry, fields, heads, dims, masks_ref, att, buf, edges, tops):
    _, spot, slot = fields
    tile = masks_ref.shape[2]
    up = 31 - lax.broadcasted_iota(jnp.int32, (32, tile), 0)
    packed = masks_ref[slot] & -(entry & 1)
    block = [
        jnp.where((jnp.broadcast_to(packed[w : w + 1], (32, tile)) << up) < 0, 0.0, FAR)
        for w in range(packed.shape[0])
    ]
    block = jnp.concatenate(block, axis=0)
    side = spot & 1
    feats = buf[spot >> 1, pl.ds(pl.multiple_of(side * dims, dims), dims), :]
    rests = buf[spot >> 1, 2 * dims :, :].astype(F32)
    rest = jnp.where(side == 1, rests[heads : 2 * heads], rests[:heads])
    source = head_sums(feats.astype(F32) * att) + rest
    columns = jnp.transpose(stack_rows([source], pad8(heads)))
    for h in range(heads):
        edge = jnp.broadcast_to(columns[:, h : h + 1], (tile, tile)) + block
        edges[h] = edge
        tops[h : h + 1, :] = jnp.max(edge, axis=0, keepdims=True)


def absorb(fields, heads, dims, tscore, buf, edges, tops, state):
    row, spot, _ = fields
    tile = state.shape[2]
    ones = jnp.ones((16, tile), BF16)
    target = tscore[row, :heads, :]
    old = state[row, dims : dims + heads, :]
    new = jnp.maximum(old, leaky(target + tops[:heads, :]))
    state[row, dims : dims + heads, :] = new
    alpha, up1, up2 = jnp.exp2(old - new), target - new, 0.2 * target - new
    values = []
    for h in range(heads):
        edge = edges[h]
        raw = jnp.maximum(edge + up1[h : h + 1], 0.2 * edge + up2[h : h + 1])
        weight = jnp.exp2(raw).astype(BF16)
        at = pl.multiple_of((spot & 1) * dims + h * HD, HD)
        left = jnp.concatenate([buf[spot >> 1, pl.ds(at, HD), :], ones], axis=0)
        values.append(jnp.dot(left, weight, preferred_element_type=F32))
    at = slice(dims + heads, dims + 2 * heads)
    mass = jnp.concatenate([v[HD : HD + 1] for v in values], axis=0)
    state[row, at, :] = state[row, at, :] * alpha + mass
    for h in range(heads):
        at = slice(h * HD, (h + 1) * HD)
        state[row, at, :] = state[row, at, :] * alpha[h : h + 1] + values[h][:HD]


def stage_kernel(group, groups, first, short, count, list_ref, count_ref, masks_ref, own_sc, other_sc, src_ref, *refs):
    pays, (tscore, buf, edges0, edges1, tops0, tops1) = refs[:count], refs[-6:]
    outs = refs[count if first else count + 1 : -6]
    state = outs[0]
    total = list_ref.shape[0] // groups
    blocks, dims = own_sc.shape[0], src_ref.shape[1]
    heads = dims // HD
    base = 0
    for pay in pays:
        buf[base : base + pay.shape[0]] = pay[...]
        base += pay.shape[0]
    tscore[:blocks] = own_sc[...]
    tscore[blocks:] = other_sc[...]
    if first:
        tile = state.shape[2]
        rest = state.shape[1] - dims - 2 * heads
        for b in range(blocks):
            state[b, :dims] = buf[b // 2, b % 2 * dims : (b % 2 + 1) * dims].astype(F32)
            state[b, dims : dims + heads] = own_sc[b, heads : 2 * heads]
            state[b, dims + heads : dims + 2 * heads] = jnp.ones((heads, tile), F32)
            state[blocks + b, :dims] = jnp.zeros((dims, tile), F32)
            state[blocks + b, dims : dims + heads] = jnp.full((heads, tile), 0.1 * FAR, F32)
            state[blocks + b, dims + heads :] = jnp.zeros((heads + rest, tile), F32)
            if rest:
                state[b, dims + 2 * heads :] = jnp.zeros((rest, tile), F32)
    att = column(src_ref) * LOG2E
    spaces = ((edges0, tops0), (edges1, tops1))

    def fields(entry):
        code, slot = split(entry >> 1, masks_ref.shape[0])
        row, spot = split(code, 4 * blocks)
        return row, spot, slot

    def ready(n, side):
        for k in range(WIDE):
            entry = list_ref[group * total + n * WIDE + k]
            space = [v.at[k] for v in spaces[side]]
            prepare(entry, fields(entry), heads, dims, masks_ref, att, buf, *space)

    def take(n, side):
        for k in range(WIDE):
            entry = list_ref[group * total + n * WIDE + k]
            space = [v.at[k] for v in spaces[side]]
            absorb(fields(entry), heads, dims, tscore, buf, *space, state)

    number = count_ref[group]

    def body(i, carry):
        ready(2 * i + 1, 1)
        take(2 * i, 0)

        @pl.when(2 * i + 1 < number)
        def _():
            ready(2 * i + 2, 0)
            take(2 * i + 1, 1)

        return carry

    def plain(i, carry):
        ready(i, 0)
        take(i, 0)
        return carry

    least = 2 if short else 1
    if short:

        @pl.when(number == 1)
        def _():
            plain(0, 0)

    @pl.when(number >= least)
    def _():
        ready(0, 0)
        lax.fori_loop(0, (number + 1) >> 1, body, 0)

    if len(outs) > 1:
        outs[1][...] = state[blocks:, :dims].astype(BF16)
        outs[2][...] = state[blocks:, dims:]


def merge_kernel(state_ref, sums_ref, levels_ref, x_ref, bias_ref, whole_ref, out_ref, sems):
    blocks, dims, tile = sums_ref.shape
    heads = dims // HD
    bias = column(bias_ref)
    share, copies = blocks // sems.shape[0], []
    for b in range(blocks):
        m1, m2 = state_ref[b, dims : dims + heads], levels_ref[b, :heads]
        l1 = state_ref[b, dims + heads : dims + 2 * heads]
        l2 = levels_ref[b, heads : 2 * heads]
        best = jnp.maximum(m1, m2)
        c1, c2 = jnp.exp2(m1 - best), jnp.exp2(m2 - best)
        scale = 1.0 / (l1 * c1 + l2 * c2)
        c1, c2 = (c1 * scale)[:, None, :], (c2 * scale)[:, None, :]
        mixed = state_ref[b, :dims].reshape(heads, HD, tile) * c1
        mixed = mixed + sums_ref[b].astype(F32).reshape(heads, HD, tile) * c2
        at = slice(b * tile, (b + 1) * tile)
        v = mixed.reshape(dims, tile) + x_ref[:, at].astype(F32) + bias
        out_ref[:, at] = jnp.where(v > 0, v, jnp.exp(v) - 1.0).astype(BF16)
        if (b + 1) % share == 0:
            at = slice((b + 1 - share) * tile, (b + 1) * tile)
            copies.append(pltpu.make_async_copy(out_ref.at[:, at], whole_ref.at[:, at], sems.at[b // share]))
            copies[-1].start()
    for copy in copies:
        copy.wait()


def call(kernel, outs, args, in_specs=None, out_specs=VMEM, scratch=(), aliases=None, flops=1000000):
    return pl.pallas_call(
        kernel,
        out_shape=outs,
        in_specs=in_specs or [VMEM] * len(args),
        out_specs=out_specs,
        scratch_shapes=list(scratch),
        input_output_aliases=aliases or {},
        compiler_params=pltpu.CompilerParams(vmem_limit_bytes=LIMIT),
        cost_estimate=pl.CostEstimate(flops=flops, bytes_accessed=0, transcendentals=0),
    )(*args)


def near(x):
    return pltpu.with_memory_space_constraint(x, pltpu.VMEM)


def held(x):
    return pltpu.with_memory_space_constraint(x, pltpu.SMEM)


def far(x):
    return pltpu.with_memory_space_constraint(x, pltpu.HBM)


def local(node_feats, proj_weight, att_src, att_dst, out_bias, tile_rows, tile_cols, tile_masks):
    nodes = node_feats.shape[1]
    dims = proj_weight.shape[0]
    heads = dims // HD
    words, tile = tile_masks.shape[1:]
    blocks = nodes // tile
    tiles = tile_rows.shape[0]
    n_dp, n_mp = lax.axis_size("dp"), lax.axis_size("mp")
    chips = n_dp // 2
    slots = max(2, 2 * tiles // n_dp)
    half = blocks // 2
    extra = pad8(2 * heads)
    order = ring_order(chips)
    place = [order.index(c) for c in range(chips)]
    me_mp = lax.axis_index("mp")
    steps = chips // 2
    groups = 8
    while groups < steps + 3:
        groups *= 2

    def hop(step):
        pairs = []
        for p, c in enumerate(order):
            to = order[(p + step) % chips]
            pairs += [(2 * c, 2 * to), (2 * c + 1, 2 * to + 1)]
        return sorted(pairs)

    right, left = hop(1), hop(-1)
    swap = [(i, i ^ 1) for i in range(n_dp)]

    mine = jnp.full((1,), me_mp, jnp.int32)
    core = jnp.full((1,), lax.axis_index("dp") & 1, jnp.int32)
    parts = 2 if n_mp == 2 else 1
    moved = [node_feats, proj_weight, att_src.reshape(1, dims), att_dst.reshape(1, dims)]
    moved += [tile_masks, tile_rows, tile_cols]
    shapes = [((node_feats.shape[0], nodes // parts), BF16)] * parts + [(v.shape, v.dtype) for v in moved[1:]]
    spaces = [pltpu.VMEM] * (len(shapes) - 2) + [pltpu.SMEM] * 2
    anywhere = pl.BlockSpec(memory_space=pl.ANY)
    *cuts, weight, a_src, a_dst, near_masks, near_rows, near_cols = call(
        functools.partial(open_kernel, parts),
        [space(*v) for space, v in zip(spaces, shapes)],
        [far(v) for v in moved],
        in_specs=[anywhere] * len(moved),
        out_specs=[pl.BlockSpec(memory_space=v) for v in spaces],
        scratch=[pltpu.SemaphoreType.DMA((len(shapes),))],
    )
    if n_mp == 2:
        flip = [(0, 1), (1, 0)]
        inputs = [[x, lax.ppermute(x, "mp", flip)] for x in cuts]
    else:
        whole = lax.all_gather(node_feats, "mp", axis=0, tiled=True)
        inputs = [[whole[:, k * (nodes // 2) : (k + 1) * (nodes // 2)]] for k in range(2)]
    att = (a_src, a_dst)

    packed = call(
        functools.partial(pack_kernel, blocks, place, groups),
        pltpu.HBM((n_dp, slots + 1, words // parts, tile), jnp.int32),
        [mine, held(near_rows), held(near_cols), near(near_masks)],
        in_specs=[SMEM, SMEM, SMEM, VMEM],
        scratch=[
            pltpu.SMEM((2 * n_dp,), jnp.int32),
            pltpu.SMEM((chips,), jnp.int32),
            pltpu.SMEM((n_dp * (slots + 2),), jnp.int32),
        ],
    )
    got = lax.all_to_all(packed, "dp", split_axis=0, concat_axis=0, tiled=True)
    got = [got.reshape(n_dp * (slots + 1), words // parts, tile)]
    if parts == 2:
        got.append(lax.ppermute(got[0], "mp", flip))
    got_other = [lax.ppermute(v, "dp", swap) for v in got]

    pays, own_sc = [], None
    for k, xs in enumerate(inputs):
        args = [mine] + [near(v) for v in (weight, *att, *xs)]
        if own_sc is not None:
            args.append(near(own_sc))
        pay, own_sc = call(
            functools.partial(project_kernel, len(xs), k * half),
            (
                pltpu.VMEM((half // 2, 2 * dims + extra, tile), BF16),
                pltpu.VMEM((blocks, extra, tile), F32),
            ),
            args,
            in_specs=[SMEM] + [VMEM] * (len(args) - 1),
            out_specs=(VMEM, VMEM),
            aliases={len(args) - 1: 1} if k else None,
        )
        pays.append(pay)
    other_sc = lax.ppermute(own_sc, "dp", swap)

    arrivals = []
    going = {w + p: pays["AB".index(p)] for w in "rl" for p in "AB"}
    for k in range(1, steps):
        for way in ("rA", "lA", "rB", "lB"):
            going[way] = lax.ppermute(going[way], "dp", right if way[0] == "r" else left)
        if k < steps - 1:
            arrivals.append([going[w] for w in ("rA", "rB", "lA", "lB")])
        else:
            arrivals += [[going[w] for w in ways] for ways in (("rA", "lA"), ("rB", "lB"))]
    arrivals[0] = pays + arrivals[0]
    for p in "AB":
        both = []
        for w, pairs, cut in (("r", right, slice(0, half // 4)), ("l", left, slice(half // 4, half // 2))):
            both.append(lax.ppermute(going[w + p][cut], "dp", pairs))
        arrivals.append(both)

    width = n_dp * (slots + 1)
    total = 2 * n_dp * slots + 4 * WIDE
    ids = [v.reshape(n_dp, slots + 1, words // parts, tile)[:, slots, 0, : slots + 2] for v in (got[0], got_other[0])]
    lists, counts = call(
        functools.partial(list_kernel, n_dp, slots, groups, blocks, steps + 1),
        (
            pltpu.SMEM((groups * total,), jnp.int32),
            pltpu.SMEM((groups,), jnp.int32),
        ),
        (core, *[v.reshape(n_dp * (slots + 2)) for v in ids]),
        in_specs=[SMEM] * 3,
        out_specs=(SMEM, SMEM),
    )
    masks = call(
        mix_kernel,
        pltpu.VMEM((2 * width, words, tile), jnp.int32),
        (mine, *[near(v) for v in got + got_other]),
        in_specs=[SMEM] + [VMEM] * (2 * parts),
    )

    shared = [masks, own_sc, other_sc, att[0]]
    state_shape = pltpu.VMEM((2 * blocks, dims + extra, tile), F32)
    half_shapes = [pltpu.VMEM((blocks, dims, tile), BF16), pltpu.VMEM((blocks, extra, tile), F32)]

    def stage(g, bufs, state, hand=False):
        args = [held(lists), held(counts)] + [near(v) for v in shared + bufs]
        outs, aliases = [state_shape], {}
        if state is not None:
            args.append(near(state))
            aliases[len(args) - 1] = 0
        if hand:
            outs += half_shapes
            for k, v in enumerate(shared + bufs):
                aliases[2 + k] = len(outs)
                outs.append(pltpu.VMEM(v.shape, v.dtype))
        return call(
            functools.partial(stage_kernel, g, groups, state is None, g >= steps, len(bufs)),
            outs,
            args,
            in_specs=[SMEM, SMEM] + [VMEM] * (len(args) - 2),
            out_specs=[VMEM] * len(outs),
            scratch=[
                pltpu.VMEM((2 * blocks, extra, tile), F32),
                pltpu.VMEM((sum(v.shape[0] for v in bufs), 2 * dims + extra, tile), BF16),
                *[pltpu.VMEM((WIDE, heads, tile, tile), F32)] * 2,
                *[pltpu.VMEM((WIDE, pad8(heads), tile), F32)] * 2,
            ],
            aliases=aliases,
            flops=8000000000,
        )

    state = None
    for g, bufs in enumerate(arrivals[:-1]):
        (state,) = stage(g, bufs, state)
    state, sums, levels, *rest = stage(steps + 1, arrivals[-1], state, True)
    back = lax.ppermute(sums, "dp", swap), lax.ppermute(levels, "dp", swap)
    shared = rest[: len(shared)]
    (state,) = stage(steps + 2, rest[len(shared) :], state)
    return call(
        merge_kernel,
        jax.ShapeDtypeStruct((dims, nodes), BF16),
        (near(state), *[near(v) for v in back], node_feats, out_bias.reshape(1, dims)),
        out_specs=anywhere,
        scratch=[pltpu.VMEM((dims, nodes), BF16), pltpu.SemaphoreType.DMA((math.gcd(blocks, 8),))],
    )


def solution(mesh):
    return jax.shard_map(
        local,
        mesh=mesh,
        in_specs=(
            P("mp", "dp"),
            P("mp", None),
            P("mp"),
            P("mp"),
            P("mp"),
            P("dp"),
            P("dp"),
            P("dp", None, None),
        ),
        out_specs=P("mp", "dp"),
        check_vma=False,
    )
```

```python
import functools
import math

import jax
import jax.numpy as jnp
from jax import lax
from jax.experimental import pallas as pl
from jax.experimental.pallas import tpu as pltpu
from jax.sharding import PartitionSpec as P


HD = 32
LOG2E = 1.4426950408889634
FAR = -1e30
F32 = jnp.float32
BF16 = jnp.bfloat16


WIDE = 2
LIMIT = 16 * 1024 * 1024

VMEM = pl.BlockSpec(memory_space=pltpu.VMEM)
SMEM = pl.BlockSpec(memory_space=pltpu.SMEM)


def split(value, size):
    if size & (size - 1) == 0:
        return value >> (size.bit_length() - 1), value & (size - 1)
    return lax.div(value, jnp.int32(size)), lax.rem(value, jnp.int32(size))


def pad8(count):
    return -(-count // 8) * 8


def leaky(scores):
    return jnp.maximum(scores, 0.2 * scores)


def head_sums(rows):
    return jnp.sum(rows.reshape(rows.shape[0] // HD, HD, rows.shape[1]), axis=1)


def stack_rows(pieces, total):
    have = sum(p.shape[0] for p in pieces)
    if have < total:
        pieces = pieces + [jnp.zeros((total - have, pieces[0].shape[1]), F32)]
    return jnp.concatenate(pieces, axis=0)


def ring_order(chips):
    columns = max(1, chips // 4)
    rows = chips // columns
    if columns == 1:
        return list(range(chips))
    order = [row * columns for row in range(rows)]
    for row in reversed(range(rows)):
        inner = list(range(1, columns))
        order += [row * columns + col for col in (inner if (rows - 1 - row) % 2 == 0 else inner[::-1])]
    return order


def column(row_ref):
    return jnp.transpose(jnp.broadcast_to(row_ref[...], (8, row_ref.shape[1])))[:, 0:1]


def project_kernel(parts, base, mp_ref, w_ref, src_ref, dst_ref, *refs):
    x_refs, (pay_ref, sc_ref) = refs[:parts], refs[-2:]
    me = mp_ref[0]
    depth = w_ref.shape[1] // parts
    total = None
    for k in range(parts):
        at = pl.multiple_of((me ^ k) * depth, depth) if parts > 1 else 0
        term = jnp.dot(w_ref[:, pl.ds(at, depth)], x_refs[k][...], preferred_element_type=F32)
        total = term if total is None else total + term
    rounded = total.astype(BF16)
    a_src, a_dst = column(src_ref) * LOG2E, column(dst_ref) * LOG2E
    source = head_sums(total * a_src)
    target = head_sums(total * a_dst)
    rest = source - head_sums(rounded.astype(F32) * a_src)
    scores = stack_rows([target, leaky(source + target)], sc_ref.shape[1])
    dims, tile = rounded.shape[0], pay_ref.shape[2]
    for b in range(2 * pay_ref.shape[0]):
        at = slice(b * tile, (b + 1) * tile)
        side = b % 2 * dims
        pay_ref[b // 2, side : side + dims, :] = rounded[:, at]
        sc_ref[base + b] = scores[:, at]
    for p in range(pay_ref.shape[0]):
        rests = [rest[:, k * tile : (k + 1) * tile] for k in (2 * p, 2 * p + 1)]
        pay_ref[p, 2 * dims :, :] = stack_rows(rests, pay_ref.shape[1] - 2 * dims).astype(BF16)


def open_kernel(halves, *refs):
    count = (len(refs) - halves) // 2
    sources, outs, sems = refs[:count], refs[count:-1], refs[-1]
    size = outs[0].shape[1]
    sources = [sources[0].at[:, k * size : (k + 1) * size] for k in range(halves)] + list(sources[1:])
    copies = [pltpu.make_async_copy(v, w, sems.at[k]) for k, (v, w) in enumerate(zip(sources, outs))]
    for copy in copies:
        copy.start()
    for copy in copies:
        copy.wait()


def pack_kernel(blocks, place, groups, mp_ref, rows_ref, cols_ref, masks_ref, out_ref, count, place_ref, codes):
    devices, slots = out_ref.shape[0], out_ref.shape[1] - 1
    words = out_ref.shape[2:]
    whole = masks_ref.shape[1]
    low = mp_ref[0] == 0
    half = blocks // 2
    chips = len(place)
    width = slots + 2
    for c in range(chips):
        place_ref[c] = place[c]
    for d in range(devices):
        count[2 * d] = 0
        count[2 * d + 1] = 0

    def body(t, carry):
        row, col = rows_ref[t], cols_ref[t]
        owner, row_at = split(row, blocks)
        holder, col_at = split(col, blocks)
        odd = holder & 1
        have = count[2 * owner + odd]
        count[2 * owner + odd] = have + 1
        at = jnp.where(odd == 1, slots - 1 - have, have)
        mask = masks_ref[t]
        out_ref[owner, at] = mask if words[0] == whole else jnp.where(low, mask[: words[0]], mask[words[0] :])
        back = place_ref[owner >> 1] - place_ref[holder >> 1]
        back = jnp.where(back < 0, back + chips, back)
        step = jnp.minimum(back, chips - back)
        part, j = split(col_at, half)
        last = 2 * back == chips
        before = step == chips // 2 - 1
        spot = col_at + jnp.where(back > step, blocks, 0) + jnp.where(step == 1, blocks, 0)
        spot = jnp.where(before, j + jnp.where(back > step, half, 0), jnp.where(last, j, spot))
        group = jnp.where(step > 0, step - 1, 0) + jnp.where(before | last, part, 0) + jnp.where(last, 1, 0)
        codes[owner * width + at] = (row_at * (4 * blocks) + spot) * groups + group
        return carry

    lax.fori_loop(0, rows_ref.shape[0], body, 0, unroll=4)
    lane = lax.broadcasted_iota(jnp.int32, words, 1)
    for d in range(devices):
        here = jnp.zeros(words, jnp.int32)
        for n in range(slots):
            here = jnp.where(lane == n, codes[d * width + n], here)
        for n in range(2):
            here = jnp.where(lane == slots + n, count[2 * d + n], here)
        out_ref[d, slots] = here


def mix_kernel(mp_ref, *refs):
    *parts, masks_ref = refs
    width = masks_ref.shape[0] // 2
    low = mp_ref[0] == 0
    for side in range(2):
        at = slice(side * width, (side + 1) * width)
        if len(parts) == 2:
            masks_ref[at] = parts[side][...]
        else:
            here, peer = parts[2 * side][...], parts[2 * side + 1][...]
            masks_ref[at, : here.shape[1]] = jnp.where(low, here, peer)
            masks_ref[at, here.shape[1] :] = jnp.where(low, peer, here)


def list_kernel(devices, slots, groups, blocks, final, core_ref, own_ids, other_ids, list_ref, count_ref):
    total = list_ref.shape[0] // groups
    width = devices * (slots + 1)
    core = core_ref[0]
    for g in range(groups):
        count_ref[g] = 0
    for side, ids in enumerate((own_ids, other_ids)):
        turn = 0 if side else 1

        def holder(d, carry, side=side, ids=ids, turn=turn):
            at_ids, at_slots = d * (slots + 2), d * (slots + 1) + side * width
            number = ids[at_ids + slots + core]
            base = jnp.where(core == 1, slots - number, 0)

            def body(n, carry):
                code, group = split(ids[at_ids + n], groups)
                to = group + jnp.where(group == final, turn, 0)
                at = count_ref[to]
                code = code + side * (4 * blocks * blocks)
                list_ref[to * total + at] = (code * (2 * width) + at_slots + n) * 2 + 1
                count_ref[to] = at + 1
                return carry

            return lax.fori_loop(base, base + number, body, carry)

        lax.fori_loop(0, devices, holder, 0)
    for g in range(groups):
        at = count_ref[g]
        for k in range(3 * WIDE):
            list_ref[g * total + at + k] = 0
        count_ref[g] = lax.div(at + WIDE - 1, WIDE)


def prepare(entry, fields, heads, dims, masks_ref, att, buf, edges, tops):
    _, spot, slot = fields
    tile = masks_ref.shape[2]
    up = 31 - lax.broadcasted_iota(jnp.int32, (32, tile), 0)
    packed = masks_ref[slot] & -(entry & 1)
    block = [
        jnp.where((jnp.broadcast_to(packed[w : w + 1], (32, tile)) << up) < 0, 0.0, FAR)
        for w in range(packed.shape[0])
    ]
    block = jnp.concatenate(block, axis=0)
    side = spot & 1
    feats = buf[spot >> 1, pl.ds(pl.multiple_of(side * dims, dims), dims), :]
    rests = buf[spot >> 1, 2 * dims :, :].astype(F32)
    rest = jnp.where(side == 1, rests[heads : 2 * heads], rests[:heads])
    source = head_sums(feats.astype(F32) * att) + rest
    columns = jnp.transpose(stack_rows([source], pad8(heads)))
    for h in range(heads):
        edge = jnp.broadcast_to(columns[:, h : h + 1], (tile, tile)) + block
        edges[h] = edge
        tops[h : h + 1, :] = jnp.max(edge, axis=0, keepdims=True)


def absorb(fields, heads, dims, tscore, buf, edges, tops, state):
    row, spot, _ = fields
    tile = state.shape[2]
    ones = jnp.ones((16, tile), BF16)
    target = tscore[row, :heads, :]
    old = state[row, dims : dims + heads, :]
    new = jnp.maximum(old, leaky(target + tops[:heads, :]))
    state[row, dims : dims + heads, :] = new
    alpha, up1, up2 = jnp.exp2(old - new), target - new, 0.2 * target - new
    values = []
    for h in range(heads):
        edge = edges[h]
        raw = jnp.maximum(edge + up1[h : h + 1], 0.2 * edge + up2[h : h + 1])
        weight = jnp.exp2(raw).astype(BF16)
        at = pl.multiple_of((spot & 1) * dims + h * HD, HD)
        left = jnp.concatenate([buf[spot >> 1, pl.ds(at, HD), :], ones], axis=0)
        values.append(jnp.dot(left, weight, preferred_element_type=F32))
    at = slice(dims + heads, dims + 2 * heads)
    mass = jnp.concatenate([v[HD : HD + 1] for v in values], axis=0)
    state[row, at, :] = state[row, at, :] * alpha + mass
    for h in range(heads):
        at = slice(h * HD, (h + 1) * HD)
        state[row, at, :] = state[row, at, :] * alpha[h : h + 1] + values[h][:HD]


def stage_kernel(group, groups, first, short, count, list_ref, count_ref, masks_ref, own_sc, other_sc, src_ref, *refs):
    pays, (tscore, buf, edges0, edges1, tops0, tops1) = refs[:count], refs[-6:]
    outs = refs[count if first else count + 1 : -6]
    state = outs[0]
    total = list_ref.shape[0] // groups
    blocks, dims = own_sc.shape[0], src_ref.shape[1]
    heads = dims // HD
    base = 0
    for pay in pays:
        buf[base : base + pay.shape[0]] = pay[...]
        base += pay.shape[0]
    tscore[:blocks] = own_sc[...]
    tscore[blocks:] = other_sc[...]
    if first:
        tile = state.shape[2]
        rest = state.shape[1] - dims - 2 * heads
        for b in range(blocks):
            state[b, :dims] = buf[b // 2, b % 2 * dims : (b % 2 + 1) * dims].astype(F32)
            state[b, dims : dims + heads] = own_sc[b, heads : 2 * heads]
            state[b, dims + heads : dims + 2 * heads] = jnp.ones((heads, tile), F32)
            state[blocks + b, :dims] = jnp.zeros((dims, tile), F32)
            state[blocks + b, dims : dims + heads] = jnp.full((heads, tile), 0.1 * FAR, F32)
            state[blocks + b, dims + heads :] = jnp.zeros((heads + rest, tile), F32)
            if rest:
                state[b, dims + 2 * heads :] = jnp.zeros((rest, tile), F32)
    att = column(src_ref) * LOG2E
    spaces = ((edges0, tops0), (edges1, tops1))

    def fields(entry):
        code, slot = split(entry >> 1, masks_ref.shape[0])
        row, spot = split(code, 4 * blocks)
        return row, spot, slot

    def ready(n, side):
        for k in range(WIDE):
            entry = list_ref[group * total + n * WIDE + k]
            space = [v.at[k] for v in spaces[side]]
            prepare(entry, fields(entry), heads, dims, masks_ref, att, buf, *space)

    def take(n, side):
        for k in range(WIDE):
            entry = list_ref[group * total + n * WIDE + k]
            space = [v.at[k] for v in spaces[side]]
            absorb(fields(entry), heads, dims, tscore, buf, *space, state)

    number = count_ref[group]

    def body(i, carry):
        ready(2 * i + 1, 1)
        take(2 * i, 0)

        @pl.when(2 * i + 1 < number)
        def _():
            ready(2 * i + 2, 0)
            take(2 * i + 1, 1)

        return carry

    def plain(i, carry):
        ready(i, 0)
        take(i, 0)
        return carry

    if short:
        lax.fori_loop(0, number, plain, 0)
    else:

        @pl.when(number > 0)
        def _():
            ready(0, 0)
            lax.fori_loop(0, (number + 1) >> 1, body, 0)

    if len(outs) > 1:
        outs[1][...] = state[blocks:, :dims].astype(BF16)
        outs[2][...] = state[blocks:, dims:]


def merge_kernel(state_ref, sums_ref, levels_ref, x_ref, bias_ref, whole_ref, out_ref, sems):
    blocks, dims, tile = sums_ref.shape
    heads = dims // HD
    bias = column(bias_ref)
    share, copies = blocks // sems.shape[0], []
    for b in range(blocks):
        m1, m2 = state_ref[b, dims : dims + heads], levels_ref[b, :heads]
        l1 = state_ref[b, dims + heads : dims + 2 * heads]
        l2 = levels_ref[b, heads : 2 * heads]
        best = jnp.maximum(m1, m2)
        c1, c2 = jnp.exp2(m1 - best), jnp.exp2(m2 - best)
        scale = 1.0 / (l1 * c1 + l2 * c2)
        c1, c2 = (c1 * scale)[:, None, :], (c2 * scale)[:, None, :]
        mixed = state_ref[b, :dims].reshape(heads, HD, tile) * c1
        mixed = mixed + sums_ref[b].astype(F32).reshape(heads, HD, tile) * c2
        at = slice(b * tile, (b + 1) * tile)
        v = mixed.reshape(dims, tile) + x_ref[:, at].astype(F32) + bias
        out_ref[:, at] = jnp.where(v > 0, v, jnp.exp(v) - 1.0).astype(BF16)
        if (b + 1) % share == 0:
            at = slice((b + 1 - share) * tile, (b + 1) * tile)
            copies.append(pltpu.make_async_copy(out_ref.at[:, at], whole_ref.at[:, at], sems.at[b // share]))
            copies[-1].start()
    for copy in copies:
        copy.wait()


def call(kernel, outs, args, in_specs=None, out_specs=VMEM, scratch=(), aliases=None, flops=1000000):
    return pl.pallas_call(
        kernel,
        out_shape=outs,
        in_specs=in_specs or [VMEM] * len(args),
        out_specs=out_specs,
        scratch_shapes=list(scratch),
        input_output_aliases=aliases or {},
        compiler_params=pltpu.CompilerParams(vmem_limit_bytes=LIMIT),
        cost_estimate=pl.CostEstimate(flops=flops, bytes_accessed=0, transcendentals=0),
    )(*args)


def near(x):
    return pltpu.with_memory_space_constraint(x, pltpu.VMEM)


def held(x):
    return pltpu.with_memory_space_constraint(x, pltpu.SMEM)


def far(x):
    return pltpu.with_memory_space_constraint(x, pltpu.HBM)


def local(node_feats, proj_weight, att_src, att_dst, out_bias, tile_rows, tile_cols, tile_masks):
    nodes = node_feats.shape[1]
    dims = proj_weight.shape[0]
    heads = dims // HD
    words, tile = tile_masks.shape[1:]
    blocks = nodes // tile
    tiles = tile_rows.shape[0]
    n_dp, n_mp = lax.axis_size("dp"), lax.axis_size("mp")
    chips = n_dp // 2
    slots = max(2, 2 * tiles // n_dp)
    half = blocks // 2
    extra = pad8(2 * heads)
    order = ring_order(chips)
    place = [order.index(c) for c in range(chips)]
    me_mp = lax.axis_index("mp")
    steps = chips // 2
    groups = 8
    while groups < steps + 3:
        groups *= 2

    def hop(step):
        pairs = []
        for p, c in enumerate(order):
            to = order[(p + step) % chips]
            pairs += [(2 * c, 2 * to), (2 * c + 1, 2 * to + 1)]
        return sorted(pairs)

    right, left = hop(1), hop(-1)
    swap = [(i, i ^ 1) for i in range(n_dp)]

    mine = jnp.full((1,), me_mp, jnp.int32)
    core = jnp.full((1,), lax.axis_index("dp") & 1, jnp.int32)
    parts = 2 if n_mp == 2 else 1
    moved = [node_feats, proj_weight, att_src.reshape(1, dims), att_dst.reshape(1, dims)]
    moved += [out_bias.reshape(1, dims), tile_masks, tile_rows, tile_cols]
    shapes = [((node_feats.shape[0], nodes // parts), BF16)] * parts + [(v.shape, v.dtype) for v in moved[1:]]
    spaces = [pltpu.VMEM] * (len(shapes) - 2) + [pltpu.SMEM] * 2
    anywhere = pl.BlockSpec(memory_space=pl.ANY)
    *cuts, weight, a_src, a_dst, near_bias, near_masks, near_rows, near_cols = call(
        functools.partial(open_kernel, parts),
        [space(*v) for space, v in zip(spaces, shapes)],
        [far(v) for v in moved],
        in_specs=[anywhere] * len(moved),
        out_specs=[pl.BlockSpec(memory_space=v) for v in spaces],
        scratch=[pltpu.SemaphoreType.DMA((len(shapes),))],
    )
    if n_mp == 2:
        flip = [(0, 1), (1, 0)]
        inputs = [[x, lax.ppermute(x, "mp", flip)] for x in cuts]
    else:
        whole = lax.all_gather(node_feats, "mp", axis=0, tiled=True)
        inputs = [[whole[:, k * (nodes // 2) : (k + 1) * (nodes // 2)]] for k in range(2)]
    att = (a_src, a_dst)

    packed = call(
        functools.partial(pack_kernel, blocks, place, groups),
        pltpu.HBM((n_dp, slots + 1, words // parts, tile), jnp.int32),
        [mine, held(near_rows), held(near_cols), near(near_masks)],
        in_specs=[SMEM, SMEM, SMEM, VMEM],
        scratch=[
            pltpu.SMEM((2 * n_dp,), jnp.int32),
            pltpu.SMEM((chips,), jnp.int32),
            pltpu.SMEM((n_dp * (slots + 2),), jnp.int32),
        ],
    )
    got = lax.all_to_all(packed, "dp", split_axis=0, concat_axis=0, tiled=True)
    got = [got.reshape(n_dp * (slots + 1), words // parts, tile)]
    if parts == 2:
        got.append(lax.ppermute(got[0], "mp", flip))
    got_other = [lax.ppermute(v, "dp", swap) for v in got]

    pays, own_sc = [], None
    for k, xs in enumerate(inputs):
        args = [mine] + [near(v) for v in (weight, *att, *xs)]
        if own_sc is not None:
            args.append(near(own_sc))
        pay, own_sc = call(
            functools.partial(project_kernel, len(xs), k * half),
            (
                pltpu.VMEM((half // 2, 2 * dims + extra, tile), BF16),
                pltpu.VMEM((blocks, extra, tile), F32),
            ),
            args,
            in_specs=[SMEM] + [VMEM] * (len(args) - 1),
            out_specs=(VMEM, VMEM),
            aliases={len(args) - 1: 1} if k else None,
        )
        pays.append(pay)
    other_sc = lax.ppermute(own_sc, "dp", swap)

    arrivals = []
    going = {w + p: pays["AB".index(p)] for w in "rl" for p in "AB"}
    for k in range(1, steps):
        for way in ("rA", "lA", "rB", "lB"):
            going[way] = lax.ppermute(going[way], "dp", right if way[0] == "r" else left)
        if k < steps - 1:
            arrivals.append([going[w] for w in ("rA", "rB", "lA", "lB")])
        else:
            arrivals += [[going[w] for w in ways] for ways in (("rA", "lA"), ("rB", "lB"))]
    arrivals[0] = pays + arrivals[0]
    for p in "AB":
        both = []
        for w, pairs, cut in (("r", right, slice(0, half // 4)), ("l", left, slice(half // 4, half // 2))):
            both.append(lax.ppermute(going[w + p][cut], "dp", pairs))
        arrivals.append(both)

    width = n_dp * (slots + 1)
    total = 2 * n_dp * slots + 4 * WIDE
    ids = [v.reshape(n_dp, slots + 1, words // parts, tile)[:, slots, 0, : slots + 2] for v in (got[0], got_other[0])]
    lists, counts = call(
        functools.partial(list_kernel, n_dp, slots, groups, blocks, steps + 1),
        (
            pltpu.SMEM((groups * total,), jnp.int32),
            pltpu.SMEM((groups,), jnp.int32),
        ),
        (core, *[v.reshape(n_dp * (slots + 2)) for v in ids]),
        in_specs=[SMEM] * 3,
        out_specs=(SMEM, SMEM),
    )
    masks = call(
        mix_kernel,
        pltpu.VMEM((2 * width, words, tile), jnp.int32),
        (mine, *[near(v) for v in got + got_other]),
        in_specs=[SMEM] + [VMEM] * (2 * parts),
    )

    shared = [masks, own_sc, other_sc, att[0]]
    state_shape = pltpu.VMEM((2 * blocks, dims + extra, tile), F32)
    half_shapes = [pltpu.VMEM((blocks, dims, tile), BF16), pltpu.VMEM((blocks, extra, tile), F32)]

    def stage(g, bufs, state, hand=False):
        args = [held(lists), held(counts)] + [near(v) for v in shared + bufs]
        outs, aliases = [state_shape], {}
        if state is not None:
            args.append(near(state))
            aliases[len(args) - 1] = 0
        if hand:
            outs += half_shapes
            for k, v in enumerate(shared + bufs):
                aliases[2 + k] = len(outs)
                outs.append(pltpu.VMEM(v.shape, v.dtype))
        return call(
            functools.partial(stage_kernel, g, groups, state is None, g >= steps, len(bufs)),
            outs,
            args,
            in_specs=[SMEM, SMEM] + [VMEM] * (len(args) - 2),
            out_specs=[VMEM] * len(outs),
            scratch=[
                pltpu.VMEM((2 * blocks, extra, tile), F32),
                pltpu.VMEM((sum(v.shape[0] for v in bufs), 2 * dims + extra, tile), BF16),
                *[pltpu.VMEM((WIDE, heads, tile, tile), F32)] * 2,
                *[pltpu.VMEM((WIDE, pad8(heads), tile), F32)] * 2,
            ],
            aliases=aliases,
            flops=8000000000,
        )

    state = None
    for g, bufs in enumerate(arrivals[:-1]):
        (state,) = stage(g, bufs, state)
    state, sums, levels, *rest = stage(steps + 1, arrivals[-1], state, True)
    back = lax.ppermute(sums, "dp", swap), lax.ppermute(levels, "dp", swap)
    shared = rest[: len(shared)]
    (state,) = stage(steps + 2, rest[len(shared) :], state)
    return call(
        merge_kernel,
        jax.ShapeDtypeStruct((dims, nodes), BF16),
        (near(state), *[near(v) for v in back], near(node_feats), near(near_bias)),
        out_specs=anywhere,
        scratch=[pltpu.VMEM((dims, nodes), BF16), pltpu.SemaphoreType.DMA((math.gcd(blocks, 8),))],
    )


def solution(mesh):
    return jax.shard_map(
        local,
        mesh=mesh,
        in_specs=(
            P("mp", "dp"),
            P("mp", None),
            P("mp"),
            P("mp"),
            P("mp"),
            P("dp"),
            P("dp"),
            P("dp", None, None),
        ),
        out_specs=P("mp", "dp"),
        check_vma=False,
    )
```
